256 devices in a mesh: dp: 32 (over z, y), mp: 8 (over x, core).
Axes of the slice: x: 4, y: 4, z: 8, core: 2. Of those that a mesh axis runs over, the one named last changes fastest.
Arguments:
- queries: bfloat16 [256, 64, 128], P('dp', 'mp'), may hold values from -140 to 140
- resident_cache: bfloat16 [256, 256, 8, 128], P('dp', None, 'mp'), may hold values from -6 to 6
- overflow_cache: bfloat16 [32, 32, 2, 128, 8, 128], P('dp', None, None, None, 'mp'), may hold values from -6 to 6
- key_up_weight: bfloat16 [8, 64, 128], P('mp'), may hold values from -0.75 to 0.75
- value_up_weight: bfloat16 [8, 64, 128], P('mp'), may hold values from -0.75 to 0.75
- lengths: int32 [256], replicated, may hold values from 257 to 1024
- routes: int32 [256, 6, 1], replicated, may hold values from 0 to 31; in each aligned block of 48 rows (0 to 47, 48 to 95, ..., all dimensions but the last counted through in order) at most 2 rows name the same one
- out_weight: bfloat16 [8192, 8192], P('mp', 'dp'), may hold values from -0.0625 to 0.0625
Outputs:
- mixed_out: bfloat16 [256, 8192], P('mp', 'dp')
The draws below stay inside these ranges and needn't reach their ends.
Inputs may be any that keep to these rules, and one draw needn't show every extreme that they name: Among the 48 entries of one sequence group (sequences s with the same s // 8) no group is named more than 2 times; the page named by routes[s, j, 0] lies in the slots of that holding group kept for the group s // 8, at the slot given by ranking. Slots that no entry names hold data that no output reads.
All inputs are finite; a program needn't handle non-finite values.
Results may differ from the reference program's by a relative error of at most 0.0049.
Values may be sent and summed in bfloat16 or wider, within the bound.
A program may use at most 64 MiB of HBM per device.

```python
import math
import jax
import jax.numpy as jnp
import numpy as np
from jax import lax

D = 8192
QUERY_HEADS = 64
KEY_VALUE_HEADS = 8
HEAD_DIMENSION = 128
KEY_LATENT_RANK = 64
VALUE_LATENT_RANK = 64
PAGE_TOKENS = 128
RESIDENT_PAGES = 2
REMOTE_PAGES = 6
SEQ_DEV = 8
SEQUENCE_TOTAL = 256
SPILL_CAPACITY = 2
N_DP = 32


def draw_queries(key, part):
    shape = (SEQUENCE_TOTAL, QUERY_HEADS, HEAD_DIMENSION)
    first_key = jax.random.fold_in(key, 0)
    values = jnp.clip(jax.random.normal(first_key, shape, jnp.float32), -4.0, 4.0)
    return values.astype(jnp.bfloat16)


def with_ends(entries, stream_key, smallest, largest):
    place = [jax.random.randint(jax.random.fold_in(stream_key, axis), (), 0, length) for axis, length in enumerate(entries.shape)]
    main_axis = entries.shape.index(max(entries.shape))
    beside = place[:main_axis] + [(place[main_axis] + 1) % entries.shape[main_axis]] + place[main_axis + 1:]
    return entries.at[tuple(place)].set(smallest).at[tuple(beside)].set(largest)


def block_scale(stream_key, dims, cuts, low, top_value):
    loudness = 1.0
    for dim, shards_of in cuts:
        steps = jax.random.uniform(jax.random.fold_in(jax.random.fold_in(stream_key, 6), dim), (shards_of,), jnp.float32, low / len(cuts), top_value / len(cuts))
        loudness = loudness * jnp.repeat(jnp.exp(steps), dims[dim] // shards_of).reshape((-1,) + (1,) * (len(dims) - 1 - dim))
    return loudness


def shared_out(rng, own, number, rows, number_of, top, bound, slope):
    order = jax.random.permutation(rng, number_of)
    crowded, ordinary = load_shares(number_of, rows * top, bound, slope, True), load_shares(number_of, rows * top, bound, slope, False)
    places = jnp.arange(number_of)

    def named(sizes, offset_by):
        used = int((sizes > 0).sum())
        fixed = max(1, used // 4)
        moved = fixed + (places - fixed + offset_by * (used - fixed)) % max(1, number_of - fixed)
        return jnp.zeros((number_of,), jnp.int32).at[order[jnp.where(places < fixed, places, moved)]].set(jnp.asarray(sizes, jnp.int32))

    sizes = jnp.where(number % 4 == 0, named(crowded, number // 4), named(ordinary, number - number // 4 - 1))
    mixed = jax.random.permutation(jax.random.fold_in(own, 3), number_of)
    source_of, sink = mixed[0:number_of // 2 * 2:2], mixed[1:number_of // 2 * 2:2]
    slack = jnp.minimum(sizes[source_of] - 1, bound - sizes[sink]) // 2
    slack = jnp.where((source_of == order[0]) | (sink == order[0]) | (sizes[sink] == 0), 0, jnp.maximum(slack, 0))
    moved = jax.random.randint(jax.random.fold_in(own, 4), (number_of // 2,), 0, 1 << 20) % (slack + 1)
    sizes = sizes.at[source_of].add(-moved).at[sink].add(moved)
    members = jnp.searchsorted(jnp.cumsum(sizes), jnp.arange(rows * top), side="right").astype(jnp.int32)
    listing = members.reshape(top, rows).T
    listing = listing[jax.random.permutation(jax.random.fold_in(own, 1), rows)]
    offset_by = jax.random.randint(jax.random.fold_in(own, 2), (rows, 1), 0, top)
    return jnp.take_along_axis(listing, (jnp.arange(top)[None, :] + offset_by) % top, axis=1)


def load_shares(number_of, total, reach, lean, full):
    weights = [(1 << 20) // math.isqrt(standing ** lean) + 1 for standing in range(1, number_of + 1)]
    largest = reach if full else min(reach, max(-(-total // number_of), total * weights[0] // sum(weights)))
    least = 1 if total - largest >= number_of - 1 else 0
    given, surplus = [largest] + [least] * (number_of - 1), total - largest - least * (number_of - 1)
    while surplus > 0:
        free = [i for i in range(1, number_of) if given[i] < largest] or [i for i in range(1, number_of) if given[i] < reach]
        pool, left = sum([weights[i] for i in free]), surplus
        for i in free:
            addition = min(reach - given[i], max(1, left * weights[i] // pool), surplus)
            given[i] = given[i] + addition
            surplus = surplus - addition
    return np.array(given)


def scatter_about(key, dims, deviation, limit, cuts=(), kind=jnp.bfloat16):
    drawn = jax.random.normal(key, dims, jnp.float32) * deviation
    if len(cuts) > 0:
        drawn = block_scale(key, dims, cuts, -0.22, 0.18) * drawn
    return jnp.clip(drawn, min=-limit, max=limit).astype(kind)


def setup_inputs(seed: int = 0) -> dict:
    arg_keys = jax.random.split(jax.random.key(seed), 9)
    queries = draw_queries(jax.random.fold_in(arg_keys[8], 71), 0)
    resident_cache = scatter_about(arg_keys[1], (SEQUENCE_TOTAL, RESIDENT_PAGES * PAGE_TOKENS, KEY_VALUE_HEADS, KEY_LATENT_RANK + VALUE_LATENT_RANK), 1.0, 6.0, ((0, 32), (2, 8)))
    overflow_cache = scatter_about(arg_keys[2], (N_DP, N_DP, SPILL_CAPACITY, PAGE_TOKENS, KEY_VALUE_HEADS, KEY_LATENT_RANK + VALUE_LATENT_RANK), 1.0, 6.0, ((0, 32), (4, 8)))
    key_up_weight = scatter_about(arg_keys[3], (KEY_VALUE_HEADS, KEY_LATENT_RANK, HEAD_DIMENSION), KEY_LATENT_RANK ** -0.5, 0.75, ((0, 8),))
    value_up_weight = scatter_about(arg_keys[4], (KEY_VALUE_HEADS, VALUE_LATENT_RANK, HEAD_DIMENSION), VALUE_LATENT_RANK ** -0.5, 0.75, ((0, 8),))
    lengths = with_ends(jax.random.randint(arg_keys[5], (SEQUENCE_TOTAL,), RESIDENT_PAGES * PAGE_TOKENS + 1, (RESIDENT_PAGES + REMOTE_PAGES) * PAGE_TOKENS + 1), jax.random.fold_in(arg_keys[5], 1), RESIDENT_PAGES * PAGE_TOKENS + 1, (RESIDENT_PAGES + REMOTE_PAGES) * PAGE_TOKENS).astype(jnp.int32)
    routes_keys = jax.random.split(jax.random.fold_in(arg_keys[6], 1), SEQUENCE_TOTAL * REMOTE_PAGES // (SEQ_DEV * REMOTE_PAGES))
    routes_turns = jax.random.permutation(jax.random.fold_in(arg_keys[6], 3), SEQUENCE_TOTAL * REMOTE_PAGES // (SEQ_DEV * REMOTE_PAGES))
    routes = jax.vmap(lambda own, number: shared_out(jax.random.fold_in(arg_keys[6], 2), own, number, SEQ_DEV * REMOTE_PAGES, N_DP, 1, SPILL_CAPACITY, 2))(routes_keys, routes_turns).reshape((SEQUENCE_TOTAL, REMOTE_PAGES, 1))
    out_weight = scatter_about(arg_keys[7], (QUERY_HEADS * HEAD_DIMENSION, D), (QUERY_HEADS * HEAD_DIMENSION) ** -0.5, 0.0625, ((0, 8), (1, 32)))
    return {"queries": queries, "resident_cache": resident_cache, "overflow_cache": overflow_cache, "key_up_weight": key_up_weight, "value_up_weight": value_up_weight, "lengths": lengths, "routes": routes, "out_weight": out_weight}


def spill_ranks(targets):
    entry_count = targets.shape[-1]
    position = jnp.arange(entry_count, dtype=jnp.int32)
    same_target = targets[..., :, None] == targets[..., None, :]
    earlier = position[None, :] < position[:, None]
    return lax.optimization_barrier(jnp.sum((same_target & earlier).astype(jnp.int32), axis=-1)).astype(jnp.int32)

def reference(queries, resident_cache, overflow_cache, key_up_weight, value_up_weight, lengths, routes, out_weight):
    targets = routes[:, :, 0].reshape(N_DP, SEQ_DEV * REMOTE_PAGES)
    ranking = spill_ranks(targets).reshape(N_DP * SEQ_DEV, REMOTE_PAGES)
    targets = targets.reshape(N_DP * SEQ_DEV, REMOTE_PAGES)
    key_table = key_up_weight.astype(jnp.float32)
    value_table = value_up_weight.astype(jnp.float32)
    head_cluster = QUERY_HEADS // KEY_VALUE_HEADS
    token_total = (RESIDENT_PAGES + REMOTE_PAGES) * PAGE_TOKENS
    score_scale = 1.0 / math.sqrt(HEAD_DIMENSION)

    def one_sequence(packed):
        sequence, single_query, resident_rows, length, target_row, rank_row = packed
        owner_group = (sequence // SEQ_DEV).astype(jnp.int32)
        remote_rows = overflow_cache[target_row, owner_group, rank_row]
        latent_vector = jnp.concatenate([resident_rows, remote_rows.reshape(REMOTE_PAGES * PAGE_TOKENS, KEY_VALUE_HEADS, KEY_LATENT_RANK + VALUE_LATENT_RANK)], axis=0).astype(jnp.float32)
        rebuilt_keys = jnp.einsum('thr,hrd->thd', latent_vector[..., :KEY_LATENT_RANK], key_table)
        rebuilt_values = jnp.einsum('thr,hrd->thd', latent_vector[..., KEY_LATENT_RANK:], value_table)
        group_sorted = single_query.astype(jnp.float32).reshape(KEY_VALUE_HEADS, head_cluster, HEAD_DIMENSION)
        scores = jnp.einsum('hgd,thd->hgt', group_sorted, rebuilt_keys, precision=lax.Precision.HIGHEST) * score_scale
        token_mask = jnp.arange(token_total, dtype=jnp.int32) < length
        scores = jnp.where(token_mask[None, None, :], scores, -jnp.inf)
        probs = jax.nn.softmax(scores, axis=-1)
        weighted = jnp.einsum('hgt,thd->hgd', probs, rebuilt_values, precision=lax.Precision.HIGHEST)
        return weighted.reshape(QUERY_HEADS * HEAD_DIMENSION).astype(jnp.bfloat16)
    sequences = jnp.arange(N_DP * SEQ_DEV, dtype=jnp.int32)
    attended = lax.map(one_sequence, (sequences, queries, resident_cache, lengths, targets, ranking))
    return jnp.dot(attended, out_weight, preferred_element_type=jnp.float32).astype(jnp.bfloat16)
```

```python
import functools
import math

import jax
import jax.numpy as jnp
from jax import lax
from jax.experimental import pallas as pl
from jax.experimental.pallas import tpu as pltpu
from jax.sharding import PartitionSpec as P

MESH = pl.DeviceIdType.MESH
very_low = -1e30
f32, bf16, i32 = jnp.float32, jnp.bfloat16, jnp.int32

SEQS = 8
HEADS = 8
SLOTS = 2
PAGE = 128
LANES = 128
RANK = 64


def iota(shape, dim):
    return lax.broadcasted_iota(i32, shape, dim)


def ones_where(condition, kind=bf16):
    return jnp.where(condition, 1.0, 0.0).astype(kind)


def dot(a, b):
    return jnp.dot(a, b, preferred_element_type=f32)


def dot_last(a, b):
    return lax.dot_general(a, b, (((1,), (1,)), ((), ())), preferred_element_type=f32)


def dot_first(a, b):
    return lax.dot_general(a, b, (((0,), (0,)), ((), ())), preferred_element_type=f32)


def rounded(x):
    return x.astype(bf16).astype(f32)


def three_pieces(x):
    top = rounded(x)
    middle = rounded(x - top)
    return top, middle, (x - top) - middle


def distance_order(nz):
    return sorted(range(nz), key=lambda dz: (min(dz, nz - dz), dz))


def kernel(
    nz,
    ny,
    nm,
    scale,
    q_ref,
    res_ref,
    ovf_ref,
    wk_ref,
    wv_ref,
    len_ref,
    rt_ref,
    w_ref,
    out_ref,
    pages,
    resident,
    wbuf,
    w_top,
    w_low,
    chosen,
    counts,
    q_send,
    q_recv,
    p_send,
    p_recv,
    own_lat,
    all_lat,
    own_part,
    r_send,
    r_recv,
    page_sem,
    local_sem,
    qs_sem,
    qr_sem,
    ps_sem,
    pr_sem,
    as_sem,
    ar_sem,
    rs_sem,
    rr_sem,
):
    me, mp = lax.axis_index("dp"), lax.axis_index("mp")
    z, y = lax.div(me, ny), lax.rem(me, ny)
    groups = nz * ny
    items = groups * SLOTS
    rows = items * HEADS
    tail = rt_ref.shape[0]
    total = groups * SEQS
    home_tokens = resident.shape[1]

    def group_at(dz, dy):
        return lax.rem(z + dz, nz) * ny + lax.rem(y + dy, ny)

    def holder_at(dz, ya):
        return lax.rem(z + dz, nz) * ny + ya

    def source_at(dz, ya):
        return lax.rem(z + nz - dz, nz) * ny + ya

    def others_in_plane(dz):
        return [lax.rem(y + dy, ny) for dy in range(1 if dz == 0 else 0, ny)]

    barrier = pltpu.get_barrier_semaphore()

    def greet_group(step, carry):
        peer = group_at(lax.div(step, ny), lax.rem(step, ny))
        pl.semaphore_signal(barrier, inc=1, device_id=(peer, mp), device_id_type=MESH)
        return carry

    def greet_member(step, carry):
        peer = lax.rem(mp + step, nm)
        pl.semaphore_signal(barrier, inc=1, device_id=(me, peer), device_id_type=MESH)
        return carry

    lax.fori_loop(1, groups, greet_group, 0)
    lax.fori_loop(1, nm, greet_member, 0)

    near_first = distance_order(nz)
    far_first = near_first[::-1]

    resident_copy = pltpu.make_async_copy(res_ref, resident, local_sem.at[0])
    resident_copy.start()
    page_copies = {}
    for dz in near_first:
        first = lax.rem(z + nz - dz, nz) * ny
        page_copies[dz] = pltpu.make_async_copy(
            ovf_ref.at[pl.ds(first, ny)], pages.at[pl.ds(dz * ny, ny)], page_sem.at[dz]
        )
        page_copies[dz].start()
    weight_copy = pltpu.make_async_copy(w_ref, wbuf, local_sem.at[1])
    weight_copy.start()

    routes = jnp.concatenate([rt_ref[p] for p in range(tail)], axis=0).astype(f32)
    lens = len_ref[...].astype(f32)

    entry = iota((items, LANES), 0)
    lane = iota((items, LANES), 1)
    entry_dz, entry_y, entry_c = entry // (ny * SLOTS), (entry // SLOTS) % ny, entry % SLOTS
    holder = (((z + entry_dz) % nz) * ny + entry_y).astype(f32)
    own_columns = ones_where(
        iota((total, LANES), 0) == me * SEQS + iota((total, LANES), 1) % SEQS
    )
    own_routes = dot(routes.astype(bf16), own_columns)
    named = [jnp.where(own_routes[p : p + 1] == holder, 1.0, 0.0) for p in range(tail)]
    row_l, column_l = iota((LANES, LANES), 0), iota((LANES, LANES), 1)
    earlier = ones_where(
        (row_l // SEQS == column_l // SEQS) & (row_l % SEQS < column_l % SEQS)
    )
    before = dot(functools.reduce(jnp.add, named).astype(bf16), earlier)
    picked = jnp.zeros((items, LANES), f32)
    wanted = entry_c.astype(f32)
    for match in named:
        picked = picked + jnp.where(before == wanted, match, 0.0)
        before = before + match
    expand = ones_where(iota((rows, items), 0) // HEADS == iota((rows, items), 1))
    row = iota((rows, LANES), 0)
    row_lane = iota((rows, LANES), 1)
    same_head = row_lane // SEQS == row % HEADS
    picks = jnp.where(same_head, dot(expand, picked.astype(bf16)), 0.0).astype(bf16)
    chosen[pl.ds(0, rows), :] = picks

    home_row, home_lane = iota((64, LANES), 0), iota((64, LANES), 1)
    turned = ones_where(
        (home_lane // SEQS == home_row % HEADS) & (home_lane % SEQS == home_row // HEADS)
    )
    chosen[pl.ds(rows, 64), :] = turned
    chosen[pl.ds(rows + 64, 64), :] = turned
    queries = q_ref[...]
    by_head = dot_first(turned, queries).astype(bf16)
    q_send[...] = dot(picks, by_head).astype(bf16).reshape(groups, SLOTS * HEADS, LANES)

    sequence = iota((total, total), 0)
    later = iota((total, total), 1)
    held_before = ones_where((sequence // SEQS == later // SEQS) & (sequence < later))
    here = jnp.where(routes == me.astype(f32), 1.0, 0.0)
    rank = dot(jnp.sum(here, axis=0, keepdims=True).astype(bf16), held_before)
    room = [jnp.zeros((1, total), f32) for _ in range(SLOTS)]
    for p in range(tail):
        match = here[p : p + 1]
        valid = jnp.clip(lens - (home_tokens + p * PAGE), 0.0, float(PAGE)) * match
        for c in range(SLOTS):
            room[c] = room[c] + jnp.where(rank == float(c), valid, 0.0)
        rank = rank + match
    entry_s = iota((items, total), 0)
    column_s = iota((items, total), 1)
    source = ((z + nz - entry_s // (ny * SLOTS)) % nz) * ny + (entry_s // SLOTS) % ny
    sized = jnp.where(entry_s % SLOTS == 0, room[0], room[1])
    sized = jnp.where(column_s // SEQS == source, sized, 0.0).astype(bf16)
    all_ones = jnp.ones((total, LANES), bf16)
    per_item = dot(sized, all_ones).astype(bf16)
    counts[...] = dot(expand, per_item)

    home_s = iota((64, total), 1) == me * SEQS + iota((64, total), 0) // HEADS
    home_count = dot(
        jnp.where(home_s, jnp.minimum(lens, float(home_tokens)), 0.0).astype(bf16), all_ones
    )

    pl.semaphore_wait(barrier, groups - 1 + nm - 1)

    def query_copy(dz, ya_source_slot, ya_target_slot, peer):
        return pltpu.make_async_remote_copy(
            src_ref=q_send.at[dz * ny + ya_source_slot],
            dst_ref=q_recv.at[dz * ny + ya_target_slot],
            send_sem=qs_sem.at[dz * ny + ya_source_slot],
            recv_sem=qr_sem.at[dz * ny + ya_target_slot],
            device_id=(peer, mp),
            device_id_type=MESH,
        )

    def part_copy(dz, ya_source_slot, ya_target_slot, peer):
        return pltpu.make_async_remote_copy(
            src_ref=p_send.at[dz * ny + ya_source_slot],
            dst_ref=p_recv.at[dz * ny + ya_target_slot],
            send_sem=ps_sem.at[dz * ny + ya_source_slot],
            recv_sem=pr_sem.at[dz * ny + ya_target_slot],
            device_id=(peer, mp),
            device_id_type=MESH,
        )

    for dz in far_first:
        for ya in others_in_plane(dz):
            query_copy(dz, ya, y, holder_at(dz, ya)).start()
    q_recv[y] = q_send[y]

    wk_wide = jnp.concatenate([wk_ref[...], jnp.zeros((RANK, LANES), bf16)], axis=0)

    def message(best, sums, mixed):
        at = iota(mixed.shape, 1)
        best_pieces, sum_pieces = three_pieces(best), three_pieces(sums)
        packed = mixed
        for i in range(3):
            packed = jnp.where(at == i, best_pieces[i], packed)
            packed = jnp.where(at == 3 + i, sum_pieces[i], packed)
        return packed, at

    def partials(query_rows, latents, token_count):
        folded = three_pieces(dot_last(query_rows, wk_wide))
        scores = []
        for i, latent in enumerate(latents):
            stacked = jnp.concatenate([f[8 * i : 8 * i + 8] for f in folded], axis=0)
            s = dot_last(stacked.astype(bf16), latent)
            scores.append(s[0:8] + s[8:16] + s[16:24])
        scores = jnp.concatenate(scores, axis=0) * scale
        mask = iota(scores.shape, 1).astype(f32) < token_count
        scores = jnp.where(mask, scores, very_low)
        best = jnp.max(scores, axis=1, keepdims=True)
        weights = jnp.where(mask, jnp.exp(scores - best), 0.0)
        sums = jnp.sum(weights, axis=1, keepdims=True)
        top = rounded(weights)
        low = weights - top
        mixed = []
        for i, latent in enumerate(latents):
            stacked = jnp.concatenate([top[8 * i : 8 * i + 8], low[8 * i : 8 * i + 8]], axis=0)
            o = dot(stacked.astype(bf16), latent)
            mixed.append(o[0:8] + o[8:16])
        return best, sums, jnp.concatenate(mixed, axis=0)

    resident_copy.wait()
    wide_count = jnp.concatenate([home_count] * (home_tokens // LANES), axis=1)
    best, sums, mixed = partials(queries, [resident[k] for k in range(SEQS)], wide_count)
    packed, at = message(best, sums, mixed)
    p_recv[pl.ds(groups, 4)] = packed.astype(bf16).reshape(4, 16, LANES)
    remainder = jnp.where((at >= 3) & (at < RANK), 0.0, packed - rounded(packed))
    remainder = jnp.where(at < 3, packed, remainder)
    p_recv[pl.ds(groups + 4, 4)] = remainder.astype(bf16).reshape(4, 16, LANES)

    weight_copy.wait()
    for h in range(HEADS):
        joined = dot(wv_ref[...], wbuf[pl.ds(h * LANES, LANES), :])
        w_top[pl.ds(h * RANK, RANK), :] = joined.astype(bf16)
        w_low[pl.ds(h * RANK, RANK), :] = (joined - rounded(joined)).astype(bf16)

    for dz in near_first:
        page_copies[dz].wait()
        for ya in others_in_plane(dz):
            query_copy(dz, ya, ya, holder_at(dz, ya)).wait_recv()
        block = q_recv[pl.ds(dz * ny, ny)].reshape(ny * SLOTS * HEADS, LANES)
        latents = [
            pages[dz * ny + i // SLOTS, pl.ds((i % SLOTS) * PAGE, PAGE), :]
            for i in range(ny * SLOTS)
        ]
        chunk = ny * SLOTS * HEADS
        best, sums, mixed = partials(block, latents, counts[pl.ds(dz * chunk, chunk), :])
        packed, _ = message(best, sums, mixed)
        p_send[pl.ds(dz * ny, ny)] = packed.astype(bf16).reshape(ny, SLOTS * HEADS, LANES)
        for ya in others_in_plane(dz):
            part_copy(dz, ya, y, source_at(dz, ya)).start()
        if dz == 0:
            p_recv[y] = p_send[y]

    for dz in near_first:
        for ya in others_in_plane(dz):
            part_copy(dz, ya, ya, source_at(dz, ya)).wait_recv()
    parts = p_recv[...].reshape(rows + 128, LANES)
    peaks = dot(parts, ones_where(iota((LANES, LANES), 0) < 3))
    member = chosen[...].astype(f32) > 0.5
    peak = jnp.max(jnp.where(member, peaks, very_low), axis=0, keepdims=True)
    factor = jnp.where(member, jnp.exp(peaks - peak), 0.0)
    factor_top = factor.astype(bf16)
    factor_low = (factor - factor_top.astype(f32)).astype(bf16)
    merged = (dot_first(factor_top, parts) + dot_first(factor_low, parts))[0:64]
    merged_sum = merged[:, 3:4] + merged[:, 4:5] + merged[:, 5:6]
    latent = merged / merged_sum
    low_lane = iota((SEQS, LANES), 1) < RANK
    for v in range(HEADS // 2):
        even = latent[16 * v : 16 * v + 8]
        odd = latent[16 * v + 8 : 16 * v + 16]
        own_lat[:, pl.ds(v * LANES, LANES)] = jnp.where(
            low_lane, pltpu.roll(even, RANK, 1), odd
        ).astype(bf16)

    def latent_copy(dz, ya, slot, peer):
        return pltpu.make_async_remote_copy(
            src_ref=own_lat,
            dst_ref=all_lat.at[slot],
            send_sem=as_sem.at[dz * ny + ya],
            recv_sem=ar_sem.at[slot],
            device_id=(peer, mp),
            device_id_type=MESH,
        )

    for dz in far_first:
        for ya in others_in_plane(dz):
            latent_copy(dz, ya, me, holder_at(dz, ya)).start()
    all_lat[me] = own_lat[...]

    def sum_copy(target):
        slot = lax.rem(mp + nm - target, nm)
        return pltpu.make_async_remote_copy(
            src_ref=r_send.at[target],
            dst_ref=r_recv.at[slot],
            send_sem=rs_sem.at[target],
            recv_sem=rr_sem.at[slot],
            device_id=(me, target),
            device_id_type=MESH,
        )

    for dz in near_first:
        target = lax.rem(z + nz - dz, nz)
        for ya in others_in_plane(dz):
            source_group = source_at(dz, ya)
            latent_copy(dz, ya, source_group, source_group).wait_recv()
        block = all_lat[pl.ds(target * ny, ny)].reshape(ny * SEQS, HEADS * RANK)
        part = dot(block, w_top[...]) + dot(block, w_low[...])

        @pl.when(target == mp)
        def _():
            own_part[...] = part

        @pl.when(target != mp)
        def _():
            r_send[target] = part.astype(bf16)
            sum_copy(target).start()

    summed = own_part[...]
    for step in range(1, nm):
        pltpu.make_async_remote_copy(
            src_ref=r_send.at[lax.rem(mp + step, nm)],
            dst_ref=r_recv.at[step],
            send_sem=rs_sem.at[lax.rem(mp + step, nm)],
            recv_sem=rr_sem.at[step],
            device_id=(me, lax.rem(mp + step, nm)),
            device_id_type=MESH,
        ).wait_recv()
        summed = summed + r_recv[step].astype(f32)
    out_ref[...] = summed.astype(bf16)

    for dz in range(nz):
        for ya in others_in_plane(dz):
            query_copy(dz, ya, y, holder_at(dz, ya)).wait_send()
            part_copy(dz, ya, y, source_at(dz, ya)).wait_send()
            latent_copy(dz, ya, me, holder_at(dz, ya)).wait_send()
    for step in range(1, nm):
        sum_copy(lax.rem(mp + step, nm)).wait_send()


def body(
    nz,
    ny,
    queries,
    resident_cache,
    overflow_cache,
    key_up_weight,
    value_up_weight,
    lengths,
    routes,
    out_weight,
):
    nm = lax.axis_size("mp")
    groups = nz * ny
    home_tokens = resident_cache.shape[1]
    out_columns = out_weight.shape[1]
    total = lengths.shape[0]
    tail = routes.shape[1]
    rows = groups * SLOTS * HEADS
    args = (
        queries.reshape(SEQS * HEADS, LANES),
        resident_cache.reshape(SEQS, home_tokens, LANES),
        overflow_cache.reshape(groups, SLOTS * PAGE, LANES),
        key_up_weight.reshape(RANK, LANES),
        value_up_weight.reshape(RANK, LANES),
        lengths.reshape(1, total),
        routes.transpose(1, 2, 0),
        out_weight,
    )
    in_vmem = pl.BlockSpec(memory_space=pltpu.VMEM)
    anywhere = pl.BlockSpec(memory_space=pl.ANY)
    dma = pltpu.SemaphoreType.DMA
    return pl.pallas_call(
        functools.partial(kernel, nz, ny, nm, 1.0 / math.sqrt(LANES)),
        out_shape=jax.ShapeDtypeStruct((ny * SEQS, out_columns), bf16),
        in_specs=[in_vmem, anywhere, anywhere, in_vmem, in_vmem, in_vmem, in_vmem, anywhere],
        out_specs=in_vmem,
        scratch_shapes=[
            pltpu.VMEM((groups, SLOTS * PAGE, LANES), bf16),
            pltpu.VMEM((SEQS, home_tokens, LANES), bf16),
            pltpu.VMEM(out_weight.shape, bf16),
            pltpu.VMEM((HEADS * RANK, out_columns), bf16),
            pltpu.VMEM((HEADS * RANK, out_columns), bf16),
            pltpu.VMEM((rows + 128, LANES), bf16),
            pltpu.VMEM((rows, LANES), f32),
            pltpu.VMEM((groups, SLOTS * HEADS, LANES), bf16),
            pltpu.VMEM((groups, SLOTS * HEADS, LANES), bf16),
            pltpu.VMEM((groups, SLOTS * HEADS, LANES), bf16),
            pltpu.VMEM((groups + 8, SLOTS * HEADS, LANES), bf16),
            pltpu.VMEM((SEQS, HEADS * RANK), bf16),
            pltpu.VMEM((groups, SEQS, HEADS * RANK), bf16),
            pltpu.VMEM((ny * SEQS, out_columns), f32),
            pltpu.VMEM((nm, ny * SEQS, out_columns), bf16),
            pltpu.VMEM((nm, ny * SEQS, out_columns), bf16),
            dma((nz,)),
            dma((2,)),
            dma((groups,)),
            dma((groups,)),
            dma((groups,)),
            dma((groups,)),
            dma((groups,)),
            dma((groups,)),
            dma((nm,)),
            dma((nm,)),
        ],
        compiler_params=pltpu.CompilerParams(collective_id=0, has_side_effects=True),
        name="spilled_attention",
    )(*args)


def solution(mesh):
    placed = (
        P("dp", "mp", None),
        P("dp", None, "mp", None),
        P("dp", None, None, None, "mp", None),
        P("mp", None, None),
        P("mp", None, None),
        P(),
        P(),
        P("mp", "dp"),
    )
    nz = mesh.shape["mp"]
    ny = mesh.shape["dp"] // nz
    return jax.shard_map(
        functools.partial(body, nz, ny),
        mesh=mesh,
        in_specs=placed,
        out_specs=P("mp", "dp"),
        check_vma=False,
    )
```

```python
import functools
import math

import jax
import jax.numpy as jnp
from jax import lax
from jax.experimental import pallas as pl
from jax.experimental.pallas import tpu as pltpu
from jax.sharding import PartitionSpec as P

MESH = pl.DeviceIdType.MESH
very_low = -1e30
f32, bf16, i32 = jnp.float32, jnp.bfloat16, jnp.int32

SEQS = 8
HEADS = 8
SLOTS = 2
PAGE = 128
LANES = 128
RANK = 64


def iota(shape, dim):
    return lax.broadcasted_iota(i32, shape, dim)


def ones_where(condition, kind=bf16):
    return jnp.where(condition, 1.0, 0.0).astype(kind)


def dot(a, b):
    return jnp.dot(a, b, preferred_element_type=f32)


def dot_last(a, b):
    return lax.dot_general(a, b, (((1,), (1,)), ((), ())), preferred_element_type=f32)


def dot_first(a, b):
    return lax.dot_general(a, b, (((0,), (0,)), ((), ())), preferred_element_type=f32)


def rounded(x):
    return x.astype(bf16).astype(f32)


def three_pieces(x):
    top = rounded(x)
    middle = rounded(x - top)
    return top, middle, (x - top) - middle


def distance_order(nz):
    return sorted(range(nz), key=lambda dz: (min(dz, nz - dz), dz))


def batches(order, sizes):
    cut, at = [], 0
    for size in sizes:
        if order[at : at + size]:
            cut.append(order[at : at + size])
        at += size
    return cut


def kernel(
    nz,
    ny,
    nm,
    scale,
    q_hbm,
    res_ref,
    ovf_ref,
    wk_hbm,
    wv_hbm,
    len_hbm,
    rt_hbm,
    w_ref,
    out_ref,
    q_ref,
    wk_ref,
    wv_ref,
    len_ref,
    rt_ref,
    pages,
    resident,
    wbuf,
    w_top,
    w_low,
    chosen,
    counts,
    q_send,
    q_recv,
    p_send,
    p_recv,
    own_lat,
    all_lat,
    own_part,
    r_send,
    r_recv,
    page_sem,
    local_sem,
    qs_sem,
    qr_sem,
    ps_sem,
    pr_sem,
    as_sem,
    ar_sem,
    rs_sem,
    rr_sem,
):
    me, mp = lax.axis_index("dp"), lax.axis_index("mp")
    z, y = lax.div(me, ny), lax.rem(me, ny)
    groups = nz * ny
    items = groups * SLOTS
    rows = items * HEADS
    tail = rt_ref.shape[0]
    total = groups * SEQS
    home_tokens = resident.shape[1]

    def group_at(dz, dy):
        return lax.rem(z + dz, nz) * ny + lax.rem(y + dy, ny)

    def holder_at(dz, ya):
        return lax.rem(z + dz, nz) * ny + ya

    def source_at(dz, ya):
        return lax.rem(z + nz - dz, nz) * ny + ya

    def others_in_plane(dz):
        return [lax.rem(y + dy, ny) for dy in range(1 if dz == 0 else 0, ny)]

    barrier = pltpu.get_barrier_semaphore()

    near_first = distance_order(nz)
    far_first = near_first[::-1]
    serve_batches = [[0]] + batches([dz for dz in far_first if dz], (2, 2, 3))
    project_batches = [[0]] + batches([dz for dz in near_first if dz], (3, 4))

    def batch_of(dz, cut):
        return next(i for i, batch in enumerate(cut) if dz in batch)

    def slots_in(batch):
        return sum(ny - (dz == 0) for dz in batch)

    for dz in far_first:
        for ya in others_in_plane(dz):
            pl.semaphore_signal(
                barrier, inc=1, device_id=(holder_at(dz, ya), mp), device_id_type=MESH
            )
    for step in range(1, nm):
        pl.semaphore_signal(
            barrier, inc=1, device_id=(me, lax.rem(mp + step, nm)), device_id_type=MESH
        )

    small = [
        pltpu.make_async_copy(source, target, local_sem.at[i])
        for i, (source, target) in enumerate(
            [
                (rt_hbm, rt_ref),
                (len_hbm, len_ref),
                (q_hbm, q_ref),
                (wk_hbm, wk_ref),
                (wv_hbm, wv_ref),
                (res_ref, resident),
                (w_ref, wbuf),
            ]
        )
    ]
    for copy in small:
        copy.start()
    for i, batch in enumerate(serve_batches):
        for dz in batch:
            first = lax.rem(z + nz - dz, nz) * ny
            pltpu.make_async_copy(
                ovf_ref.at[pl.ds(first, ny)], pages.at[pl.ds(dz * ny, ny)], page_sem.at[i]
            ).start()
    for copy in small[:5]:
        copy.wait()

    routes = jnp.concatenate([rt_ref[p] for p in range(tail)], axis=0).astype(f32)
    lens = len_ref[...].astype(f32)

    entry = iota((items, LANES), 0)
    lane = iota((items, LANES), 1)
    entry_dz, entry_y, entry_c = entry // (ny * SLOTS), (entry // SLOTS) % ny, entry % SLOTS
    holder = (((z + entry_dz) % nz) * ny + entry_y).astype(f32)
    own_columns = ones_where(
        iota((total, LANES), 0) == me * SEQS + iota((total, LANES), 1) % SEQS
    )
    own_routes = dot(routes.astype(bf16), own_columns)
    named = [jnp.where(own_routes[p : p + 1] == holder, 1.0, 0.0) for p in range(tail)]
    row_l, column_l = iota((LANES, LANES), 0), iota((LANES, LANES), 1)
    earlier = ones_where(
        (row_l // SEQS == column_l // SEQS) & (row_l % SEQS < column_l % SEQS)
    )
    before = dot(functools.reduce(jnp.add, named).astype(bf16), earlier)
    picked = jnp.zeros((items, LANES), f32)
    wanted = entry_c.astype(f32)
    for match in named:
        picked = picked + jnp.where(before == wanted, match, 0.0)
        before = before + match
    expand = ones_where(iota((rows, items), 0) // HEADS == iota((rows, items), 1))
    row = iota((rows, LANES), 0)
    row_lane = iota((rows, LANES), 1)
    same_head = row_lane // SEQS == row % HEADS
    picks = jnp.where(same_head, dot(expand, picked.astype(bf16)), 0.0).astype(bf16)
    chosen[pl.ds(0, rows), :] = picks

    home_row, home_lane = iota((64, LANES), 0), iota((64, LANES), 1)
    turned = ones_where(
        (home_lane // SEQS == home_row % HEADS) & (home_lane % SEQS == home_row // HEADS)
    )
    chosen[pl.ds(rows, 64), :] = turned
    chosen[pl.ds(rows + 64, 64), :] = turned
    queries = q_ref[...]
    by_head = dot_first(turned, queries).astype(bf16)
    q_send[...] = dot(picks, by_head).astype(bf16).reshape(groups, SLOTS * HEADS, LANES)

    sequence = iota((total, total), 0)
    later = iota((total, total), 1)
    held_before = ones_where((sequence // SEQS == later // SEQS) & (sequence < later))
    here = jnp.where(routes == me.astype(f32), 1.0, 0.0)
    rank = dot(jnp.sum(here, axis=0, keepdims=True).astype(bf16), held_before)
    room = [jnp.zeros((1, total), f32) for _ in range(SLOTS)]
    for p in range(tail):
        match = here[p : p + 1]
        valid = jnp.clip(lens - (home_tokens + p * PAGE), 0.0, float(PAGE)) * match
        for c in range(SLOTS):
            room[c] = room[c] + jnp.where(rank == float(c), valid, 0.0)
        rank = rank + match
    entry_s = iota((items, total), 0)
    column_s = iota((items, total), 1)
    source = ((z + nz - entry_s // (ny * SLOTS)) % nz) * ny + (entry_s // SLOTS) % ny
    sized = jnp.where(entry_s % SLOTS == 0, room[0], room[1])
    sized = jnp.where(column_s // SEQS == source, sized, 0.0).astype(bf16)
    all_ones = jnp.ones((total, LANES), bf16)
    per_item = dot(sized, all_ones).astype(bf16)
    counts[...] = dot(expand, per_item)

    home_s = iota((64, total), 1) == me * SEQS + iota((64, total), 0) // HEADS
    home_count = dot(
        jnp.where(home_s, jnp.minimum(lens, float(home_tokens)), 0.0).astype(bf16), all_ones
    )

    pl.semaphore_wait(barrier, groups - 1 + nm - 1)

    def query_copy(dz, ya, peer):
        return pltpu.make_async_remote_copy(
            src_ref=q_send.at[dz * ny + ya],
            dst_ref=q_recv.at[dz * ny + y],
            send_sem=qs_sem.at[0],
            recv_sem=qr_sem.at[batch_of(dz, serve_batches)],
            device_id=(peer, mp),
            device_id_type=MESH,
        )

    def part_copy(dz, ya, peer):
        return pltpu.make_async_remote_copy(
            src_ref=p_send.at[dz * ny + ya],
            dst_ref=p_recv.at[dz * ny + y],
            send_sem=ps_sem.at[0],
            recv_sem=pr_sem.at[0],
            device_id=(peer, mp),
            device_id_type=MESH,
        )

    def many(source, target, count, send_sem, recv_sem):
        return pltpu.make_async_remote_copy(
            src_ref=source.at[pl.ds(0, count)],
            dst_ref=target.at[pl.ds(0, count)],
            send_sem=send_sem,
            recv_sem=recv_sem,
            device_id=(me, mp),
            device_id_type=MESH,
        )

    for dz in far_first:
        for ya in others_in_plane(dz):
            query_copy(dz, ya, holder_at(dz, ya)).start()
    q_recv[y] = q_send[y]

    wk_wide = jnp.concatenate([wk_ref[...], jnp.zeros((RANK, LANES), bf16)], axis=0)

    def message(best, sums, mixed):
        at = iota(mixed.shape, 1)
        best_pieces, sum_pieces = three_pieces(best), three_pieces(sums)
        packed = mixed
        for i in range(3):
            packed = jnp.where(at == i, best_pieces[i], packed)
            packed = jnp.where(at == 3 + i, sum_pieces[i], packed)
        return packed, at

    def partials(query_rows, latents, token_count):
        folded = three_pieces(dot_last(query_rows, wk_wide))
        scores = []
        for i, latent in enumerate(latents):
            stacked = jnp.concatenate([f[8 * i : 8 * i + 8] for f in folded], axis=0)
            s = dot_last(stacked.astype(bf16), latent)
            scores.append(s[0:8] + s[8:16] + s[16:24])
        scores = jnp.concatenate(scores, axis=0) * scale
        mask = iota(scores.shape, 1).astype(f32) < token_count
        scores = jnp.where(mask, scores, very_low)
        best = jnp.max(scores, axis=1, keepdims=True)
        weights = jnp.where(mask, jnp.exp(scores - best), 0.0)
        sums = jnp.sum(weights, axis=1, keepdims=True)
        top = rounded(weights)
        low = weights - top
        mixed = []
        for i, latent in enumerate(latents):
            stacked = jnp.concatenate([top[8 * i : 8 * i + 8], low[8 * i : 8 * i + 8]], axis=0)
            o = dot(stacked.astype(bf16), latent)
            mixed.append(o[0:8] + o[8:16])
        return best, sums, jnp.concatenate(mixed, axis=0)

    small[5].wait()
    wide_count = jnp.concatenate([home_count] * (home_tokens // LANES), axis=1)
    best, sums, mixed = partials(queries, [resident[k] for k in range(SEQS)], wide_count)
    packed, at = message(best, sums, mixed)
    p_recv[pl.ds(groups, 4)] = packed.astype(bf16).reshape(4, 16, LANES)
    remainder = jnp.where((at >= 3) & (at < RANK), 0.0, packed - rounded(packed))
    remainder = jnp.where(at < 3, packed, remainder)
    p_recv[pl.ds(groups + 4, 4)] = remainder.astype(bf16).reshape(4, 16, LANES)

    small[6].wait()
    for h in range(HEADS):
        joined = dot(wv_ref[...], wbuf[pl.ds(h * LANES, LANES), :])
        w_top[pl.ds(h * RANK, RANK), :] = joined.astype(bf16)
        w_low[pl.ds(h * RANK, RANK), :] = (joined - rounded(joined)).astype(bf16)

    chunk = ny * SLOTS * HEADS
    for i, batch in enumerate(serve_batches):
        held = len(batch) * ny
        pltpu.make_async_copy(
            ovf_ref.at[pl.ds(0, held)], pages.at[pl.ds(0, held)], page_sem.at[i]
        ).wait()
        many(q_send, q_recv, slots_in(batch), qs_sem.at[0], qr_sem.at[i]).wait_recv()
        block = jnp.concatenate(
            [q_recv[pl.ds(dz * ny, ny)].reshape(chunk, LANES) for dz in batch], axis=0
        )
        token_count = jnp.concatenate(
            [counts[pl.ds(dz * chunk, chunk), :] for dz in batch], axis=0
        )
        latents = [
            pages[dz * ny + i // SLOTS, pl.ds((i % SLOTS) * PAGE, PAGE), :]
            for dz in batch
            for i in range(ny * SLOTS)
        ]
        best, sums, mixed = partials(block, latents, token_count)
        packed, _ = message(best, sums, mixed)
        packed = packed.astype(bf16).reshape(len(batch) * ny, SLOTS * HEADS, LANES)
        for n, dz in enumerate(batch):
            p_send[pl.ds(dz * ny, ny)] = packed[n * ny : (n + 1) * ny]
        for dz in batch:
            for ya in others_in_plane(dz):
                part_copy(dz, ya, source_at(dz, ya)).start()
            if dz == 0:
                p_recv[y] = p_send[y]

    many(p_send, p_recv, groups - 1, ps_sem.at[0], pr_sem.at[0]).wait_recv()
    parts = p_recv[...].reshape(rows + 128, LANES)
    peaks = dot(parts, ones_where(iota((LANES, LANES), 0) < 3))
    member = chosen[...].astype(f32) > 0.5
    peak = jnp.max(jnp.where(member, peaks, very_low), axis=0, keepdims=True)
    factor = jnp.where(member, jnp.exp(peaks - peak), 0.0)
    factor_top = factor.astype(bf16)
    factor_low = (factor - factor_top.astype(f32)).astype(bf16)
    merged = (dot_first(factor_top, parts) + dot_first(factor_low, parts))[0:64]
    merged_sum = merged[:, 3:4] + merged[:, 4:5] + merged[:, 5:6]
    latent = merged / merged_sum
    low_lane = iota((SEQS, LANES), 1) < RANK
    for v in range(HEADS // 2):
        even = latent[16 * v : 16 * v + 8]
        odd = latent[16 * v + 8 : 16 * v + 16]
        own_lat[:, pl.ds(v * LANES, LANES)] = jnp.where(
            low_lane, pltpu.roll(even, RANK, 1), odd
        ).astype(bf16)

    def latent_copy(dz, peer):
        return pltpu.make_async_remote_copy(
            src_ref=own_lat,
            dst_ref=all_lat.at[me],
            send_sem=as_sem.at[0],
            recv_sem=ar_sem.at[batch_of(dz, project_batches)],
            device_id=(peer, mp),
            device_id_type=MESH,
        )

    for dz in far_first:
        for ya in others_in_plane(dz):
            latent_copy(dz, holder_at(dz, ya)).start()
    all_lat[me] = own_lat[...]

    def sum_copy(target):
        return pltpu.make_async_remote_copy(
            src_ref=r_send.at[target],
            dst_ref=r_recv.at[lax.rem(mp + nm - target, nm)],
            send_sem=rs_sem.at[0],
            recv_sem=rr_sem.at[0],
            device_id=(me, target),
            device_id_type=MESH,
        )

    for i, batch in enumerate(project_batches):
        many(all_lat, all_lat, slots_in(batch), as_sem.at[0], ar_sem.at[i]).wait_recv()
        block = jnp.concatenate(
            [
                all_lat[pl.ds(lax.rem(z + nz - dz, nz) * ny, ny)].reshape(
                    ny * SEQS, HEADS * RANK
                )
                for dz in batch
            ],
            axis=0,
        )
        part = dot(block, w_top[...]) + dot(block, w_low[...])
        for n, dz in enumerate(batch):
            target = lax.rem(z + nz - dz, nz)
            piece = part[n * ny * SEQS : (n + 1) * ny * SEQS]

            @pl.when(target == mp)
            def _():
                own_part[...] = piece

            @pl.when(target != mp)
            def _():
                r_send[target] = piece.astype(bf16)
                sum_copy(target).start()

    many(r_send, r_recv, nm - 1, rs_sem.at[0], rr_sem.at[0]).wait_recv()
    summed = own_part[...]
    for step in range(1, nm):
        summed = summed + r_recv[step].astype(f32)
    out_ref[...] = summed.astype(bf16)
    many(q_send, q_recv, groups - 1, qs_sem.at[0], qr_sem.at[0]).wait_send()
    many(p_send, p_recv, groups - 1, ps_sem.at[0], pr_sem.at[0]).wait_send()
    many(all_lat, all_lat, groups - 1, as_sem.at[0], ar_sem.at[0]).wait_send()
    many(r_send, r_recv, nm - 1, rs_sem.at[0], rr_sem.at[0]).wait_send()


def body(
    nz,
    ny,
    queries,
    resident_cache,
    overflow_cache,
    key_up_weight,
    value_up_weight,
    lengths,
    routes,
    out_weight,
):
    nm = lax.axis_size("mp")
    groups = nz * ny
    home_tokens = resident_cache.shape[1]
    out_columns = out_weight.shape[1]
    total = lengths.shape[0]
    tail = routes.shape[1]
    rows = groups * SLOTS * HEADS
    args = (
        queries.reshape(SEQS * HEADS, LANES),
        resident_cache.reshape(SEQS, home_tokens, LANES),
        overflow_cache.reshape(groups, SLOTS * PAGE, LANES),
        key_up_weight.reshape(RANK, LANES),
        value_up_weight.reshape(RANK, LANES),
        lengths.reshape(1, total),
        routes.transpose(1, 2, 0),
        out_weight,
    )
    in_vmem = pl.BlockSpec(memory_space=pltpu.VMEM)
    anywhere = pl.BlockSpec(memory_space=pl.ANY)
    dma = pltpu.SemaphoreType.DMA
    return pl.pallas_call(
        functools.partial(kernel, nz, ny, nm, 1.0 / math.sqrt(LANES)),
        out_shape=jax.ShapeDtypeStruct((ny * SEQS, out_columns), bf16),
        in_specs=[anywhere] * 8,
        out_specs=in_vmem,
        scratch_shapes=[
            pltpu.VMEM((SEQS * HEADS, LANES), bf16),
            pltpu.VMEM((RANK, LANES), bf16),
            pltpu.VMEM((RANK, LANES), bf16),
            pltpu.VMEM((1, total), i32),
            pltpu.VMEM((tail, 1, total), i32),
            pltpu.VMEM((groups, SLOTS * PAGE, LANES), bf16),
            pltpu.VMEM((SEQS, home_tokens, LANES), bf16),
            pltpu.VMEM(out_weight.shape, bf16),
            pltpu.VMEM((HEADS * RANK, out_columns), bf16),
            pltpu.VMEM((HEADS * RANK, out_columns), bf16),
            pltpu.VMEM((rows + 128, LANES), bf16),
            pltpu.VMEM((rows, LANES), f32),
            pltpu.VMEM((groups, SLOTS * HEADS, LANES), bf16),
            pltpu.VMEM((groups, SLOTS * HEADS, LANES), bf16),
            pltpu.VMEM((groups, SLOTS * HEADS, LANES), bf16),
            pltpu.VMEM((groups + 8, SLOTS * HEADS, LANES), bf16),
            pltpu.VMEM((SEQS, HEADS * RANK), bf16),
            pltpu.VMEM((groups, SEQS, HEADS * RANK), bf16),
            pltpu.VMEM((ny * SEQS, out_columns), f32),
            pltpu.VMEM((nm, ny * SEQS, out_columns), bf16),
            pltpu.VMEM((nm, ny * SEQS, out_columns), bf16),
            dma((4,)),
            dma((7,)),
            dma((1,)),
            dma((4,)),
            dma((1,)),
            dma((1,)),
            dma((1,)),
            dma((3,)),
            dma((1,)),
            dma((1,)),
        ],
        compiler_params=pltpu.CompilerParams(collective_id=0, has_side_effects=True),
        name="spilled_attention",
    )(*args)


def solution(mesh):
    placed = (
        P("dp", "mp", None),
        P("dp", None, "mp", None),
        P("dp", None, None, None, "mp", None),
        P("mp", None, None),
        P("mp", None, None),
        P(),
        P(),
        P("mp", "dp"),
    )
    nz = mesh.shape["mp"]
    ny = mesh.shape["dp"] // nz
    return jax.shard_map(
        functools.partial(body, nz, ny),
        mesh=mesh,
        in_specs=placed,
        out_specs=P("mp", "dp"),
        check_vma=False,
    )
```

```python
import functools
import math

import jax
import jax.numpy as jnp
from jax import lax
from jax.experimental import pallas as pl
from jax.experimental.pallas import tpu as pltpu
from jax.sharding import PartitionSpec as P

MESH = pl.DeviceIdType.MESH
very_low = -1e30
f32, bf16, i32 = jnp.float32, jnp.bfloat16, jnp.int32

SEQS = 8
HEADS = 8
SLOTS = 2
PAGE = 128
LANES = 128
RANK = 64


def iota(shape, dim):
    return lax.broadcasted_iota(i32, shape, dim)


def ones_where(condition, kind=bf16):
    return jnp.where(condition, 1.0, 0.0).astype(kind)


def dot(a, b):
    return jnp.dot(a, b, preferred_element_type=f32)


def dot_last(a, b):
    return lax.dot_general(a, b, (((1,), (1,)), ((), ())), preferred_element_type=f32)


def dot_first(a, b):
    return lax.dot_general(a, b, (((0,), (0,)), ((), ())), preferred_element_type=f32)


def rounded(x):
    return x.astype(bf16).astype(f32)


def three_pieces(x):
    top = rounded(x)
    middle = rounded(x - top)
    return top, middle, (x - top) - middle


def distance_order(nz):
    return sorted(range(nz), key=lambda dz: (min(dz, nz - dz), dz))


def batches(order, sizes):
    cut, at = [], 0
    for size in sizes:
        if order[at : at + size]:
            cut.append(order[at : at + size])
        at += size
    return cut


def kernel(
    nz,
    ny,
    nm,
    scale,
    q_hbm,
    res_ref,
    ovf_ref,
    wk_hbm,
    wv_hbm,
    len_hbm,
    rt_hbm,
    w_ref,
    out_ref,
    q_ref,
    wk_ref,
    wv_ref,
    len_ref,
    rt_ref,
    pages,
    resident,
    wbuf,
    w_top,
    w_low,
    chosen,
    counts,
    q_send,
    q_recv,
    p_send,
    p_recv,
    own_lat,
    all_lat,
    own_part,
    r_send,
    r_recv,
    page_sem,
    local_sem,
    qs_sem,
    qr_sem,
    ps_sem,
    pr_sem,
    as_sem,
    ar_sem,
    rs_sem,
    rr_sem,
):
    me, mp = lax.axis_index("dp"), lax.axis_index("mp")
    z, y = lax.div(me, ny), lax.rem(me, ny)
    groups = nz * ny
    items = groups * SLOTS
    rows = items * HEADS
    tail = rt_ref.shape[0]
    total = groups * SEQS
    home_tokens = resident.shape[1]

    def group_at(dz, dy):
        return lax.rem(z + dz, nz) * ny + lax.rem(y + dy, ny)

    def holder_at(dz, ya):
        return lax.rem(z + dz, nz) * ny + ya

    def source_at(dz, ya):
        return lax.rem(z + nz - dz, nz) * ny + ya

    def others_in_plane(dz):
        return [lax.rem(y + dy, ny) for dy in range(1 if dz == 0 else 0, ny)]

    barrier = pltpu.get_barrier_semaphore()

    near_first = distance_order(nz)
    far_first = near_first[::-1]
    serve_batches = [[0]] + batches([dz for dz in far_first if dz], (1, 2, 2, 2))
    project_batches = [[0]] + batches([dz for dz in far_first if dz], (4, 3))

    def batch_of(dz, cut):
        return next(i for i, batch in enumerate(cut) if dz in batch)

    def slots_in(batch):
        return sum(ny - (dz == 0) for dz in batch)

    for dz in far_first:
        for ya in others_in_plane(dz):
            pl.semaphore_signal(
                barrier, inc=1, device_id=(holder_at(dz, ya), mp), device_id_type=MESH
            )
    for step in range(1, nm):
        pl.semaphore_signal(
            barrier, inc=1, device_id=(me, lax.rem(mp + step, nm)), device_id_type=MESH
        )

    small = [
        pltpu.make_async_copy(source, target, local_sem.at[i])
        for i, (source, target) in enumerate(
            [
                (rt_hbm, rt_ref),
                (len_hbm, len_ref),
                (q_hbm, q_ref),
                (wk_hbm, wk_ref),
                (wv_hbm, wv_ref),
                (res_ref, resident),
                (w_ref, wbuf),
            ]
        )
    ]
    for copy in small:
        copy.start()
    for i, batch in enumerate(serve_batches):
        for dz in batch:
            first = lax.rem(z + nz - dz, nz) * ny
            pltpu.make_async_copy(
                ovf_ref.at[pl.ds(first, ny)], pages.at[pl.ds(dz * ny, ny)], page_sem.at[i]
            ).start()
    for copy in small[:5]:
        copy.wait()

    routes = jnp.concatenate([rt_ref[p] for p in range(tail)], axis=0).astype(f32)
    lens = len_ref[...].astype(f32)

    entry = iota((items, LANES), 0)
    lane = iota((items, LANES), 1)
    entry_dz, entry_y, entry_c = entry // (ny * SLOTS), (entry // SLOTS) % ny, entry % SLOTS
    holder = (((z + entry_dz) % nz) * ny + entry_y).astype(f32)
    own_columns = ones_where(
        iota((total, LANES), 0) == me * SEQS + iota((total, LANES), 1) % SEQS
    )
    own_routes = dot(routes.astype(bf16), own_columns)
    named = [jnp.where(own_routes[p : p + 1] == holder, 1.0, 0.0) for p in range(tail)]
    row_l, column_l = iota((LANES, LANES), 0), iota((LANES, LANES), 1)
    earlier = ones_where(
        (row_l // SEQS == column_l // SEQS) & (row_l % SEQS < column_l % SEQS)
    )
    before = dot(functools.reduce(jnp.add, named).astype(bf16), earlier)
    picked = jnp.zeros((items, LANES), f32)
    wanted = entry_c.astype(f32)
    for match in named:
        picked = picked + jnp.where(before == wanted, match, 0.0)
        before = before + match
    expand = ones_where(iota((rows, items), 0) // HEADS == iota((rows, items), 1))
    row = iota((rows, LANES), 0)
    row_lane = iota((rows, LANES), 1)
    same_head = row_lane // SEQS == row % HEADS
    picks = jnp.where(same_head, dot(expand, picked.astype(bf16)), 0.0).astype(bf16)

    home_row, home_lane = iota((64, LANES), 0), iota((64, LANES), 1)
    turned = ones_where(
        (home_lane // SEQS == home_row % HEADS) & (home_lane % SEQS == home_row // HEADS)
    )
    queries = q_ref[...]
    by_head = dot_first(turned, queries).astype(bf16)
    q_send[...] = dot(picks, by_head).astype(bf16).reshape(groups, SLOTS * HEADS, LANES)

    sequence = iota((total, total), 0)
    later = iota((total, total), 1)
    held_before = ones_where((sequence // SEQS == later // SEQS) & (sequence < later))
    here = jnp.where(routes == me.astype(f32), 1.0, 0.0)
    rank = dot(jnp.sum(here, axis=0, keepdims=True).astype(bf16), held_before)
    room = [jnp.zeros((1, total), f32) for _ in range(SLOTS)]
    for p in range(tail):
        match = here[p : p + 1]
        valid = jnp.clip(lens - (home_tokens + p * PAGE), 0.0, float(PAGE)) * match
        for c in range(SLOTS):
            room[c] = room[c] + jnp.where(rank == float(c), valid, 0.0)
        rank = rank + match
    entry_s = iota((items, total), 0)
    column_s = iota((items, total), 1)
    source = ((z + nz - entry_s // (ny * SLOTS)) % nz) * ny + (entry_s // SLOTS) % ny
    sized = jnp.where(entry_s % SLOTS == 0, room[0], room[1])
    sized = jnp.where(column_s // SEQS == source, sized, 0.0).astype(bf16)
    all_ones = jnp.ones((total, LANES), bf16)
    per_item = dot(sized, all_ones).astype(bf16)
    counts[...] = dot(expand, per_item)

    home_s = iota((64, total), 1) == me * SEQS + iota((64, total), 0) // HEADS
    home_count = dot(
        jnp.where(home_s, jnp.minimum(lens, float(home_tokens)), 0.0).astype(bf16), all_ones
    )

    pl.semaphore_wait(barrier, groups - 1 + nm - 1)

    def query_copy(dz, ya, peer):
        return pltpu.make_async_remote_copy(
            src_ref=q_send.at[dz * ny + ya],
            dst_ref=q_recv.at[dz * ny + y],
            send_sem=qs_sem.at[0],
            recv_sem=qr_sem.at[batch_of(dz, serve_batches)],
            device_id=(peer, mp),
            device_id_type=MESH,
        )

    def part_copy(dz, ya, peer):
        return pltpu.make_async_remote_copy(
            src_ref=p_send.at[dz * ny + ya],
            dst_ref=p_recv.at[dz * ny + y],
            send_sem=ps_sem.at[0],
            recv_sem=pr_sem.at[0],
            device_id=(peer, mp),
            device_id_type=MESH,
        )

    def many(source, target, count, send_sem, recv_sem):
        return pltpu.make_async_remote_copy(
            src_ref=source.at[pl.ds(0, count)],
            dst_ref=target.at[pl.ds(0, count)],
            send_sem=send_sem,
            recv_sem=recv_sem,
            device_id=(me, mp),
            device_id_type=MESH,
        )

    for dz in far_first:
        for ya in others_in_plane(dz):
            query_copy(dz, ya, holder_at(dz, ya)).start()
    q_recv[y] = q_send[y]

    wk_wide = jnp.concatenate([wk_ref[...], jnp.zeros((RANK, LANES), bf16)], axis=0)

    def message(best, sums, mixed):
        at = iota(mixed.shape, 1)
        best_pieces, sum_pieces = three_pieces(best), three_pieces(sums)
        packed = mixed
        for i in range(3):
            packed = jnp.where(at == i, best_pieces[i], packed)
            packed = jnp.where(at == 3 + i, sum_pieces[i], packed)
        return packed, at

    def partials(query_rows, latents, token_count):
        folded = three_pieces(dot_last(query_rows, wk_wide))
        scores = []
        for i, latent in enumerate(latents):
            stacked = jnp.concatenate([f[8 * i : 8 * i + 8] for f in folded], axis=0)
            s = dot_last(stacked.astype(bf16), latent)
            scores.append(s[0:8] + s[8:16] + s[16:24])
        scores = jnp.concatenate(scores, axis=0) * scale
        mask = iota(scores.shape, 1).astype(f32) < token_count
        scores = jnp.where(mask, scores, very_low)
        best = jnp.max(scores, axis=1, keepdims=True)
        weights = jnp.where(mask, jnp.exp(scores - best), 0.0)
        sums = jnp.sum(weights, axis=1, keepdims=True)
        top = rounded(weights)
        low = weights - top
        mixed = []
        for i, latent in enumerate(latents):
            stacked = jnp.concatenate([top[8 * i : 8 * i + 8], low[8 * i : 8 * i + 8]], axis=0)
            o = dot(stacked.astype(bf16), latent)
            mixed.append(o[0:8] + o[8:16])
        return best, sums, jnp.concatenate(mixed, axis=0)

    square = ones_where(home_row == home_lane)
    chosen[:, pl.ds(0, rows)] = dot_last(square, picks)
    turned_back = dot_last(square, turned)
    chosen[:, pl.ds(rows, 128)] = jnp.concatenate([turned_back, turned_back], axis=1)
    small[5].wait()
    wide_count = jnp.concatenate([home_count] * (home_tokens // LANES), axis=1)
    best, sums, mixed = partials(queries, [resident[k] for k in range(SEQS)], wide_count)
    packed, at = message(best, sums, mixed)
    p_recv[pl.ds(groups, 4)] = packed.astype(bf16).reshape(4, 16, LANES)
    remainder = jnp.where((at >= 3) & (at < RANK), 0.0, packed - rounded(packed))
    remainder = jnp.where(at < 3, packed, remainder)
    p_recv[pl.ds(groups + 4, 4)] = remainder.astype(bf16).reshape(4, 16, LANES)

    small[6].wait()
    for h in range(HEADS):
        joined = dot(wv_ref[...], wbuf[pl.ds(h * LANES, LANES), :])
        w_top[pl.ds(h * RANK, RANK), :] = joined.astype(bf16)
        w_low[pl.ds(h * RANK, RANK), :] = (joined - rounded(joined)).astype(bf16)

    chunk = ny * SLOTS * HEADS
    for i, batch in enumerate(serve_batches):
        held = len(batch) * ny
        pltpu.make_async_copy(
            ovf_ref.at[pl.ds(0, held)], pages.at[pl.ds(0, held)], page_sem.at[i]
        ).wait()
        many(q_send, q_recv, slots_in(batch), qs_sem.at[0], qr_sem.at[i]).wait_recv()
        block = jnp.concatenate(
            [q_recv[pl.ds(dz * ny, ny)].reshape(chunk, LANES) for dz in batch], axis=0
        )
        token_count = jnp.concatenate(
            [counts[pl.ds(dz * chunk, chunk), :] for dz in batch], axis=0
        )
        latents = [
            pages[dz * ny + i // SLOTS, pl.ds((i % SLOTS) * PAGE, PAGE), :]
            for dz in batch
            for i in range(ny * SLOTS)
        ]
        best, sums, mixed = partials(block, latents, token_count)
        packed, _ = message(best, sums, mixed)
        packed = packed.astype(bf16).reshape(len(batch) * ny, SLOTS * HEADS, LANES)
        for n, dz in enumerate(batch):
            p_send[pl.ds(dz * ny, ny)] = packed[n * ny : (n + 1) * ny]
        for dz in batch:
            for ya in others_in_plane(dz):
                part_copy(dz, ya, source_at(dz, ya)).start()
            if dz == 0:
                p_recv[y] = p_send[y]

    many(p_send, p_recv, groups - 1, ps_sem.at[0], pr_sem.at[0]).wait_recv()
    parts = p_recv[...].reshape(rows + 128, LANES)
    peaks = dot_last(ones_where(iota((SEQS, LANES), 1) < 3), parts)
    peaks = jnp.broadcast_to(peaks[0:1], chosen.shape)
    member = chosen[...] > 0.5
    peak = jnp.max(jnp.where(member, peaks, very_low), axis=1, keepdims=True)
    factor = jnp.where(member, jnp.exp(peaks - peak), 0.0)
    factor_top = rounded(factor)
    merged = dot(
        jnp.concatenate([factor_top, factor - factor_top], axis=0).astype(bf16), parts
    )
    merged = merged[0:64] + merged[64:128]
    merged_sum = merged[:, 3:4] + merged[:, 4:5] + merged[:, 5:6]
    latent = merged / merged_sum
    low_lane = iota((SEQS, LANES), 1) < RANK
    for v in range(HEADS // 2):
        even = latent[16 * v : 16 * v + 8]
        odd = latent[16 * v + 8 : 16 * v + 16]
        own_lat[:, pl.ds(v * LANES, LANES)] = jnp.where(
            low_lane, pltpu.roll(even, RANK, 1), odd
        ).astype(bf16)

    def latent_copy(dz, peer):
        return pltpu.make_async_remote_copy(
            src_ref=own_lat,
            dst_ref=all_lat.at[me],
            send_sem=as_sem.at[0],
            recv_sem=ar_sem.at[batch_of(dz, project_batches)],
            device_id=(peer, mp),
            device_id_type=MESH,
        )

    for dz in far_first:
        for ya in others_in_plane(dz):
            latent_copy(dz, holder_at(dz, ya)).start()
    all_lat[me] = own_lat[...]

    def sum_copy(target):
        return pltpu.make_async_remote_copy(
            src_ref=r_send.at[target],
            dst_ref=r_recv.at[lax.rem(mp + nm - target, nm)],
            send_sem=rs_sem.at[0],
            recv_sem=rr_sem.at[0],
            device_id=(me, target),
            device_id_type=MESH,
        )

    for i, batch in enumerate(project_batches):
        many(all_lat, all_lat, slots_in(batch), as_sem.at[0], ar_sem.at[i]).wait_recv()
        block = jnp.concatenate(
            [
                all_lat[pl.ds(lax.rem(z + nz - dz, nz) * ny, ny)].reshape(
                    ny * SEQS, HEADS * RANK
                )
                for dz in batch
            ],
            axis=0,
        )
        part = dot(block, w_top[...]) + dot(block, w_low[...])
        for n, dz in enumerate(batch):
            target = lax.rem(z + nz - dz, nz)
            piece = part[n * ny * SEQS : (n + 1) * ny * SEQS]

            @pl.when(target == mp)
            def _():
                own_part[...] = piece

            @pl.when(target != mp)
            def _():
                r_send[target] = piece.astype(bf16)
                sum_copy(target).start()

    many(r_send, r_recv, nm - 1, rs_sem.at[0], rr_sem.at[0]).wait_recv()
    summed = own_part[...]
    for step in range(1, nm):
        summed = summed + r_recv[step].astype(f32)
    out_ref[...] = summed.astype(bf16)
    many(q_send, q_recv, groups - 1, qs_sem.at[0], qr_sem.at[0]).wait_send()
    many(p_send, p_recv, groups - 1, ps_sem.at[0], pr_sem.at[0]).wait_send()
    many(all_lat, all_lat, groups - 1, as_sem.at[0], ar_sem.at[0]).wait_send()
    many(r_send, r_recv, nm - 1, rs_sem.at[0], rr_sem.at[0]).wait_send()


def body(
    nz,
    ny,
    queries,
    resident_cache,
    overflow_cache,
    key_up_weight,
    value_up_weight,
    lengths,
    routes,
    out_weight,
):
    nm = lax.axis_size("mp")
    groups = nz * ny
    home_tokens = resident_cache.shape[1]
    out_columns = out_weight.shape[1]
    total = lengths.shape[0]
    tail = routes.shape[1]
    rows = groups * SLOTS * HEADS
    args = (
        queries.reshape(SEQS * HEADS, LANES),
        resident_cache.reshape(SEQS, home_tokens, LANES),
        overflow_cache.reshape(groups, SLOTS * PAGE, LANES),
        key_up_weight.reshape(RANK, LANES),
        value_up_weight.reshape(RANK, LANES),
        lengths.reshape(1, total),
        routes.transpose(1, 2, 0),
        out_weight,
    )
    in_vmem = pl.BlockSpec(memory_space=pltpu.VMEM)
    anywhere = pl.BlockSpec(memory_space=pl.ANY)
    dma = pltpu.SemaphoreType.DMA
    return pl.pallas_call(
        functools.partial(kernel, nz, ny, nm, 1.0 / math.sqrt(LANES)),
        out_shape=pltpu.VMEM((ny * SEQS, out_columns), bf16),
        in_specs=[anywhere] * 8,
        out_specs=in_vmem,
        scratch_shapes=[
            pltpu.VMEM((SEQS * HEADS, LANES), bf16),
            pltpu.VMEM((RANK, LANES), bf16),
            pltpu.VMEM((RANK, LANES), bf16),
            pltpu.VMEM((1, total), i32),
            pltpu.VMEM((tail, 1, total), i32),
            pltpu.VMEM((groups, SLOTS * PAGE, LANES), bf16),
            pltpu.VMEM((SEQS, home_tokens, LANES), bf16),
            pltpu.VMEM(out_weight.shape, bf16),
            pltpu.VMEM((HEADS * RANK, out_columns), bf16),
            pltpu.VMEM((HEADS * RANK, out_columns), bf16),
            pltpu.VMEM((SEQS * HEADS, rows + 128), f32),
            pltpu.VMEM((rows, LANES), f32),
            pltpu.VMEM((groups, SLOTS * HEADS, LANES), bf16),
            pltpu.VMEM((groups, SLOTS * HEADS, LANES), bf16),
            pltpu.VMEM((groups, SLOTS * HEADS, LANES), bf16),
            pltpu.VMEM((groups + 8, SLOTS * HEADS, LANES), bf16),
            pltpu.VMEM((SEQS, HEADS * RANK), bf16),
            pltpu.VMEM((groups, SEQS, HEADS * RANK), bf16),
            pltpu.VMEM((ny * SEQS, out_columns), f32),
            pltpu.VMEM((nm, ny * SEQS, out_columns), bf16),
            pltpu.VMEM((nm, ny * SEQS, out_columns), bf16),
            dma((5,)),
            dma((7,)),
            dma((1,)),
            dma((5,)),
            dma((1,)),
            dma((1,)),
            dma((1,)),
            dma((3,)),
            dma((1,)),
            dma((1,)),
        ],
        compiler_params=pltpu.CompilerParams(collective_id=0, has_side_effects=True),
        name="spilled_attention",
    )(*args)


def solution(mesh):
    placed = (
        P("dp", "mp", None),
        P("dp", None, "mp", None),
        P("dp", None, None, None, "mp", None),
        P("mp", None, None),
        P("mp", None, None),
        P(),
        P(),
        P("mp", "dp"),
    )
    nz = mesh.shape["mp"]
    ny = mesh.shape["dp"] // nz
    return jax.shard_map(
        functools.partial(body, nz, ny),
        mesh=mesh,
        in_specs=placed,
        out_specs=P("mp", "dp"),
        check_vma=False,
    )
```

```python
import functools
import math

import jax
import jax.numpy as jnp
from jax import lax
from jax.experimental import pallas as pl
from jax.experimental.pallas import tpu as pltpu
from jax.sharding import PartitionSpec as P

MESH = pl.DeviceIdType.MESH
very_low = -1e30
f32, bf16, i32 = jnp.float32, jnp.bfloat16, jnp.int32

SEQS = 8
HEADS = 8
SLOTS = 2
PAGE = 128
LANES = 128
RANK = 64


def iota(shape, dim):
    return lax.broadcasted_iota(i32, shape, dim)


def ones_where(condition, kind=bf16):
    return jnp.where(condition, 1.0, 0.0).astype(kind)


def dot(a, b):
    return jnp.dot(a, b, preferred_element_type=f32)


def dot_last(a, b):
    return lax.dot_general(a, b, (((1,), (1,)), ((), ())), preferred_element_type=f32)


def dot_first(a, b):
    return lax.dot_general(a, b, (((0,), (0,)), ((), ())), preferred_element_type=f32)


def rounded(x):
    return x.astype(bf16).astype(f32)


def three_pieces(x):
    top = rounded(x)
    middle = rounded(x - top)
    return top, middle, (x - top) - middle


def distance_order(nz):
    return sorted(range(nz), key=lambda dz: (min(dz, nz - dz), dz))


def batches(order, sizes):
    cut, at = [], 0
    for size in sizes:
        if order[at : at + size]:
            cut.append(order[at : at + size])
        at += size
    return cut


def kernel(
    nz,
    ny,
    nm,
    scale,
    q_hbm,
    res_ref,
    ovf_ref,
    wk_hbm,
    wv_hbm,
    len_hbm,
    rt_hbm,
    w_ref,
    out_ref,
    q_ref,
    wk_ref,
    wv_ref,
    len_ref,
    rt_ref,
    pages,
    resident,
    keys,
    values,
    wbuf,
    w_top,
    w_low,
    chosen,
    counts,
    q_send,
    q_recv,
    p_send,
    p_recv,
    own_lat,
    all_lat,
    own_part,
    r_send,
    r_recv,
    page_sem,
    local_sem,
    qs_sem,
    qr_sem,
    ps_sem,
    pr_sem,
    as_sem,
    ar_sem,
    rs_sem,
    rr_sem,
):
    me, mp = lax.axis_index("dp"), lax.axis_index("mp")
    z, y = lax.div(me, ny), lax.rem(me, ny)
    groups = nz * ny
    items = groups * SLOTS
    rows = items * HEADS
    tail = rt_ref.shape[0]
    total = groups * SEQS
    home_tokens = resident.shape[1]

    def group_at(dz, dy):
        return lax.rem(z + dz, nz) * ny + lax.rem(y + dy, ny)

    def holder_at(dz, ya):
        return lax.rem(z + dz, nz) * ny + ya

    def source_at(dz, ya):
        return lax.rem(z + nz - dz, nz) * ny + ya

    def others_in_plane(dz):
        return [lax.rem(y + dy, ny) for dy in range(1 if dz == 0 else 0, ny)]

    barrier = pltpu.get_barrier_semaphore()

    near_first = distance_order(nz)
    far_first = near_first[::-1]
    serve_batches = [[0]] + batches([dz for dz in far_first if dz], (4, 3))
    project_batches = [[0]] + batches([dz for dz in far_first if dz], (4, 3))

    def batch_of(dz, cut):
        return next(i for i, batch in enumerate(cut) if dz in batch)

    def slots_in(batch):
        return sum(ny - (dz == 0) for dz in batch)

    for dz in far_first:
        for ya in others_in_plane(dz):
            pl.semaphore_signal(
                barrier, inc=1, device_id=(holder_at(dz, ya), mp), device_id_type=MESH
            )
    for step in range(1, nm):
        pl.semaphore_signal(
            barrier, inc=1, device_id=(me, lax.rem(mp + step, nm)), device_id_type=MESH
        )

    small = [
        pltpu.make_async_copy(source, target, local_sem.at[i])
        for i, (source, target) in enumerate(
            [
                (rt_hbm, rt_ref),
                (len_hbm, len_ref),
                (q_hbm, q_ref),
                (wk_hbm, wk_ref),
                (wv_hbm, wv_ref),
                (res_ref, resident),
                (w_ref, wbuf),
            ]
        )
    ]
    for copy in small:
        copy.start()
    for i, batch in enumerate(serve_batches):
        for dz in batch:
            first = lax.rem(z + nz - dz, nz) * ny
            pltpu.make_async_copy(
                ovf_ref.at[pl.ds(first, ny)], pages.at[pl.ds(dz * ny, ny)], page_sem.at[i]
            ).start()
    for copy in small[:5]:
        copy.wait()

    routes = jnp.concatenate([rt_ref[p] for p in range(tail)], axis=0).astype(f32)
    lens = len_ref[...].astype(f32)

    entry = iota((items, LANES), 0)
    lane = iota((items, LANES), 1)
    entry_dz, entry_y, entry_c = entry // (ny * SLOTS), (entry // SLOTS) % ny, entry % SLOTS
    holder = (((z + entry_dz) % nz) * ny + entry_y).astype(f32)
    own_columns = ones_where(
        iota((total, LANES), 0) == me * SEQS + iota((total, LANES), 1) % SEQS
    )
    own_routes = dot(routes.astype(bf16), own_columns)
    named = [jnp.where(own_routes[p : p + 1] == holder, 1.0, 0.0) for p in range(tail)]
    row_l, column_l = iota((LANES, LANES), 0), iota((LANES, LANES), 1)
    earlier = ones_where(
        (row_l // SEQS == column_l // SEQS) & (row_l % SEQS < column_l % SEQS)
    )
    before = dot(functools.reduce(jnp.add, named).astype(bf16), earlier)
    picked = jnp.zeros((items, LANES), f32)
    wanted = entry_c.astype(f32)
    for match in named:
        picked = picked + jnp.where(before == wanted, match, 0.0)
        before = before + match
    expand = ones_where(iota((rows, items), 0) // HEADS == iota((rows, items), 1))
    row = iota((rows, LANES), 0)
    row_lane = iota((rows, LANES), 1)
    same_head = row_lane // SEQS == row % HEADS
    picks = jnp.where(same_head, dot(expand, picked.astype(bf16)), 0.0).astype(bf16)

    home_row, home_lane = iota((64, LANES), 0), iota((64, LANES), 1)
    turned = ones_where(
        (home_lane // SEQS == home_row % HEADS) & (home_lane % SEQS == home_row // HEADS)
    )
    queries = q_ref[...]
    by_head = dot_first(turned, queries).astype(bf16)
    q_send[...] = dot(picks, by_head).astype(bf16).reshape(groups, SLOTS * HEADS, LANES)

    sequence = iota((total, total), 0)
    later = iota((total, total), 1)
    held_before = ones_where((sequence // SEQS == later // SEQS) & (sequence < later))
    here = jnp.where(routes == me.astype(f32), 1.0, 0.0)
    rank = dot(jnp.sum(here, axis=0, keepdims=True).astype(bf16), held_before)
    room = [jnp.zeros((1, total), f32) for _ in range(SLOTS)]
    for p in range(tail):
        match = here[p : p + 1]
        valid = jnp.clip(lens - (home_tokens + p * PAGE), 0.0, float(PAGE)) * match
        for c in range(SLOTS):
            room[c] = room[c] + jnp.where(rank == float(c), valid, 0.0)
        rank = rank + match
    entry_s = iota((items, total), 0)
    column_s = iota((items, total), 1)
    source = ((z + nz - entry_s // (ny * SLOTS)) % nz) * ny + (entry_s // SLOTS) % ny
    sized = jnp.where(entry_s % SLOTS == 0, room[0], room[1])
    sized = jnp.where(column_s // SEQS == source, sized, 0.0).astype(bf16)
    all_ones = jnp.ones((total, LANES), bf16)
    per_item = dot(sized, all_ones).astype(bf16)
    counts[...] = dot(expand, per_item)

    home_s = iota((64, total), 1) == me * SEQS + iota((64, total), 0) // HEADS
    home_count = dot(
        jnp.where(home_s, jnp.minimum(lens, float(home_tokens)), 0.0).astype(bf16), all_ones
    )

    pl.semaphore_wait(barrier, groups - 1 + nm - 1)

    def query_copy(dz, ya, peer):
        return pltpu.make_async_remote_copy(
            src_ref=q_send.at[dz * ny + ya],
            dst_ref=q_recv.at[dz * ny + y],
            send_sem=qs_sem.at[0],
            recv_sem=qr_sem.at[batch_of(dz, serve_batches)],
            device_id=(peer, mp),
            device_id_type=MESH,
        )

    def part_copy(dz, ya, peer):
        return pltpu.make_async_remote_copy(
            src_ref=p_send.at[dz * ny + ya],
            dst_ref=p_recv.at[dz * ny + y],
            send_sem=ps_sem.at[0],
            recv_sem=pr_sem.at[0],
            device_id=(peer, mp),
            device_id_type=MESH,
        )

    def many(source, target, count, send_sem, recv_sem):
        return pltpu.make_async_remote_copy(
            src_ref=source.at[pl.ds(0, count)],
            dst_ref=target.at[pl.ds(0, count)],
            send_sem=send_sem,
            recv_sem=recv_sem,
            device_id=(me, mp),
            device_id_type=MESH,
        )

    for dz in far_first:
        for ya in others_in_plane(dz):
            query_copy(dz, ya, holder_at(dz, ya)).start()
    q_recv[y] = q_send[y]

    wk_wide = jnp.concatenate([wk_ref[...], jnp.zeros((RANK, LANES), bf16)], axis=0)

    def message(best, sums, mixed):
        at = iota(mixed.shape, 1)
        best_pieces, sum_pieces = three_pieces(best), three_pieces(sums)
        packed = mixed
        for i in range(3):
            packed = jnp.where(at == i, best_pieces[i], packed)
            packed = jnp.where(at == 3 + i, sum_pieces[i], packed)
        return packed, at

    def partials(query_rows, latents, token_count):
        folded = three_pieces(dot_last(query_rows, wk_wide))
        scores = []
        for i, latent in enumerate(latents):
            stacked = jnp.concatenate([f[8 * i : 8 * i + 8] for f in folded], axis=0)
            s = dot_last(stacked.astype(bf16), latent)
            scores.append(s[0:8] + s[8:16] + s[16:24])
        scores = jnp.concatenate(scores, axis=0) * scale
        mask = iota(scores.shape, 1).astype(f32) < token_count
        scores = jnp.where(mask, scores, very_low)
        best = jnp.max(scores, axis=1, keepdims=True)
        weights = jnp.where(mask, jnp.exp(scores - best), 0.0)
        sums = jnp.sum(weights, axis=1, keepdims=True)
        top = rounded(weights)
        low = weights - top
        mixed = []
        for i, latent in enumerate(latents):
            stacked = jnp.concatenate([top[8 * i : 8 * i + 8], low[8 * i : 8 * i + 8]], axis=0)
            o = dot(stacked.astype(bf16), latent)
            mixed.append(o[0:8] + o[8:16])
        return best, sums, jnp.concatenate(mixed, axis=0)

    square = ones_where(home_row == home_lane)
    chosen[:, pl.ds(0, rows)] = dot_last(square, picks)
    turned_back = dot_last(square, turned)
    chosen[:, pl.ds(rows, 128)] = jnp.concatenate([turned_back, turned_back], axis=1)
    small[5].wait()
    wide_count = jnp.concatenate([home_count] * (home_tokens // LANES), axis=1)
    best, sums, mixed = partials(queries, [resident[k] for k in range(SEQS)], wide_count)
    packed, at = message(best, sums, mixed)
    p_recv[pl.ds(groups, 4)] = packed.astype(bf16).reshape(4, 16, LANES)
    remainder = jnp.where((at >= 3) & (at < RANK), 0.0, packed - rounded(packed))
    remainder = jnp.where(at < 3, packed, remainder)
    p_recv[pl.ds(groups + 4, 4)] = remainder.astype(bf16).reshape(4, 16, LANES)

    small[6].wait()
    for h in range(HEADS):
        joined = dot(wv_ref[...], wbuf[pl.ds(h * LANES, LANES), :])
        w_top[pl.ds(h * RANK, RANK), :] = joined.astype(bf16)
        w_low[pl.ds(h * RANK, RANK), :] = (joined - rounded(joined)).astype(bf16)

    pick_keys = ones_where(iota((RANK, LANES), 0) == iota((RANK, LANES), 1))
    for i, batch in enumerate(serve_batches):
        held = len(batch) * ny
        pltpu.make_async_copy(
            ovf_ref.at[pl.ds(0, held)], pages.at[pl.ds(0, held)], page_sem.at[i]
        ).wait()
        for slot in [dz * ny + ya for dz in batch for ya in range(ny)]:
            page_pair = pages[slot]
            turned_keys = dot_last(pick_keys, page_pair).astype(bf16)
            keys[slot, pl.ds(0, RANK), :] = turned_keys[:, 0:PAGE]
            keys[slot, pl.ds(RANK, RANK), :] = turned_keys[:, PAGE : 2 * PAGE]
            values[slot] = jnp.concatenate(
                [page_pair[PAGE : 2 * PAGE, RANK:], page_pair[0:PAGE, RANK:]], axis=1
            )

    wk_twice = jnp.concatenate([wk_ref[...], wk_ref[...]], axis=0)

    def served(query_rows, slots, token_count):
        at, row_at = iota(query_rows.shape, 1), iota(query_rows.shape, 0)
        second = (row_at // HEADS) % SLOTS == 1
        folded = dot_last(query_rows, wk_twice)
        folded = jnp.where((at >= RANK) == second, folded, 0.0)
        top = folded.astype(bf16)
        rest = folded - top.astype(f32)
        middle = rest.astype(bf16)
        low = (rest - middle.astype(f32)).astype(bf16)
        scores = []
        for i, slot in enumerate(slots):
            part = slice(16 * i, 16 * i + 16)
            s = dot(jnp.concatenate([top[part], middle[part], low[part]], axis=0), keys[slot])
            scores.append(s[0:16] + s[16:32] + s[32:48])
        scores = jnp.concatenate(scores, axis=0) * scale
        mask = at.astype(f32) < token_count
        scores = jnp.where(mask, scores, very_low)
        best = jnp.max(scores, axis=1, keepdims=True)
        weights = jnp.where(mask, jnp.exp(scores - best), 0.0)
        sums = jnp.sum(weights, axis=1, keepdims=True)
        top = weights.astype(bf16)
        low = (weights - top.astype(f32)).astype(bf16)
        mixed = []
        for i, slot in enumerate(slots):
            part = slice(16 * i, 16 * i + 16)
            o = dot(jnp.concatenate([top[part], low[part]], axis=0), values[slot])
            mixed.append(o[0:16] + o[16:32])
        mixed = jnp.concatenate(mixed, axis=0)
        return best, sums, jnp.where(second, pltpu.roll(mixed, RANK, 1), mixed)

    chunk = ny * SLOTS * HEADS
    for i, batch in enumerate(serve_batches):
        many(q_send, q_recv, slots_in(batch), qs_sem.at[0], qr_sem.at[i]).wait_recv()
        block = jnp.concatenate(
            [q_recv[pl.ds(dz * ny, ny)].reshape(chunk, LANES) for dz in batch], axis=0
        )
        token_count = jnp.concatenate(
            [counts[pl.ds(dz * chunk, chunk), :] for dz in batch], axis=0
        )
        slots = [dz * ny + ya for dz in batch for ya in range(ny)]
        best, sums, mixed = served(block, slots, token_count)
        packed, _ = message(best, sums, mixed)
        packed = packed.astype(bf16).reshape(len(batch) * ny, SLOTS * HEADS, LANES)
        for n, dz in enumerate(batch):
            p_send[pl.ds(dz * ny, ny)] = packed[n * ny : (n + 1) * ny]
        for dz in batch:
            for ya in others_in_plane(dz):
                part_copy(dz, ya, source_at(dz, ya)).start()
            if dz == 0:
                p_recv[y] = p_send[y]

    many(p_send, p_recv, groups - 1, ps_sem.at[0], pr_sem.at[0]).wait_recv()
    parts = p_recv[...].reshape(rows + 128, LANES)
    peaks = dot_last(ones_where(iota((SEQS, LANES), 1) < 3), parts)
    peaks = jnp.broadcast_to(peaks[0:1], chosen.shape)
    member = chosen[...] > 0.5
    peak = jnp.max(jnp.where(member, peaks, very_low), axis=1, keepdims=True)
    factor = jnp.where(member, jnp.exp(peaks - peak), 0.0)
    factor_top = rounded(factor)
    merged = dot(
        jnp.concatenate([factor_top, factor - factor_top], axis=0).astype(bf16), parts
    )
    merged = merged[0:64] + merged[64:128]
    merged_sum = merged[:, 3:4] + merged[:, 4:5] + merged[:, 5:6]
    latent = merged / merged_sum
    low_lane = iota((SEQS, LANES), 1) < RANK
    for v in range(HEADS // 2):
        even = latent[16 * v : 16 * v + 8]
        odd = latent[16 * v + 8 : 16 * v + 16]
        own_lat[:, pl.ds(v * LANES, LANES)] = jnp.where(
            low_lane, pltpu.roll(even, RANK, 1), odd
        ).astype(bf16)

    def latent_copy(dz, peer):
        return pltpu.make_async_remote_copy(
            src_ref=own_lat,
            dst_ref=all_lat.at[me],
            send_sem=as_sem.at[0],
            recv_sem=ar_sem.at[batch_of(dz, project_batches)],
            device_id=(peer, mp),
            device_id_type=MESH,
        )

    for dz in far_first:
        for ya in others_in_plane(dz):
            latent_copy(dz, holder_at(dz, ya)).start()
    all_lat[me] = own_lat[...]

    def sum_copy(target):
        return pltpu.make_async_remote_copy(
            src_ref=r_send.at[target],
            dst_ref=r_recv.at[lax.rem(mp + nm - target, nm)],
            send_sem=rs_sem.at[0],
            recv_sem=rr_sem.at[0],
            device_id=(me, target),
            device_id_type=MESH,
        )

    for i, batch in enumerate(project_batches):
        many(all_lat, all_lat, slots_in(batch), as_sem.at[0], ar_sem.at[i]).wait_recv()
        block = jnp.concatenate(
            [
                all_lat[pl.ds(lax.rem(z + nz - dz, nz) * ny, ny)].reshape(
                    ny * SEQS, HEADS * RANK
                )
                for dz in batch
            ],
            axis=0,
        )
        part = dot(block, w_top[...]) + dot(block, w_low[...])
        for n, dz in enumerate(batch):
            target = lax.rem(z + nz - dz, nz)
            piece = part[n * ny * SEQS : (n + 1) * ny * SEQS]

            @pl.when(target == mp)
            def _():
                own_part[...] = piece

            @pl.when(target != mp)
            def _():
                r_send[target] = piece.astype(bf16)
                sum_copy(target).start()

    many(r_send, r_recv, nm - 1, rs_sem.at[0], rr_sem.at[0]).wait_recv()
    summed = own_part[...]
    for step in range(1, nm):
        summed = summed + r_recv[step].astype(f32)
    out_ref[...] = summed.astype(bf16)
    many(q_send, q_recv, groups - 1, qs_sem.at[0], qr_sem.at[0]).wait_send()
    many(p_send, p_recv, groups - 1, ps_sem.at[0], pr_sem.at[0]).wait_send()
    many(all_lat, all_lat, groups - 1, as_sem.at[0], ar_sem.at[0]).wait_send()
    many(r_send, r_recv, nm - 1, rs_sem.at[0], rr_sem.at[0]).wait_send()


def body(
    nz,
    ny,
    queries,
    resident_cache,
    overflow_cache,
    key_up_weight,
    value_up_weight,
    lengths,
    routes,
    out_weight,
):
    nm = lax.axis_size("mp")
    groups = nz * ny
    home_tokens = resident_cache.shape[1]
    out_columns = out_weight.shape[1]
    total = lengths.shape[0]
    tail = routes.shape[1]
    rows = groups * SLOTS * HEADS
    args = (
        queries.reshape(SEQS * HEADS, LANES),
        resident_cache.reshape(SEQS, home_tokens, LANES),
        overflow_cache.reshape(groups, SLOTS * PAGE, LANES),
        key_up_weight.reshape(RANK, LANES),
        value_up_weight.reshape(RANK, LANES),
        lengths.reshape(1, total),
        routes.transpose(1, 2, 0),
        out_weight,
    )
    in_vmem = pl.BlockSpec(memory_space=pltpu.VMEM)
    anywhere = pl.BlockSpec(memory_space=pl.ANY)
    dma = pltpu.SemaphoreType.DMA
    return pl.pallas_call(
        functools.partial(kernel, nz, ny, nm, 1.0 / math.sqrt(LANES)),
        out_shape=pltpu.VMEM((ny * SEQS, out_columns), bf16),
        in_specs=[anywhere] * 8,
        out_specs=in_vmem,
        scratch_shapes=[
            pltpu.VMEM((SEQS * HEADS, LANES), bf16),
            pltpu.VMEM((RANK, LANES), bf16),
            pltpu.VMEM((RANK, LANES), bf16),
            pltpu.VMEM((1, total), i32),
            pltpu.VMEM((tail, 1, total), i32),
            pltpu.VMEM((groups, SLOTS * PAGE, LANES), bf16),
            pltpu.VMEM((SEQS, home_tokens, LANES), bf16),
            pltpu.VMEM((groups, SLOTS * RANK, PAGE), bf16),
            pltpu.VMEM((groups, PAGE, SLOTS * RANK), bf16),
            pltpu.VMEM(out_weight.shape, bf16),
            pltpu.VMEM((HEADS * RANK, out_columns), bf16),
            pltpu.VMEM((HEADS * RANK, out_columns), bf16),
            pltpu.VMEM((SEQS * HEADS, rows + 128), f32),
            pltpu.VMEM((rows, LANES), f32),
            pltpu.VMEM((groups, SLOTS * HEADS, LANES), bf16),
            pltpu.VMEM((groups, SLOTS * HEADS, LANES), bf16),
            pltpu.VMEM((groups, SLOTS * HEADS, LANES), bf16),
            pltpu.VMEM((groups + 8, SLOTS * HEADS, LANES), bf16),
            pltpu.VMEM((SEQS, HEADS * RANK), bf16),
            pltpu.VMEM((groups, SEQS, HEADS * RANK), bf16),
            pltpu.VMEM((ny * SEQS, out_columns), f32),
            pltpu.VMEM((nm, ny * SEQS, out_columns), bf16),
            pltpu.VMEM((nm, ny * SEQS, out_columns), bf16),
            dma((5,)),
            dma((7,)),
            dma((1,)),
            dma((5,)),
            dma((1,)),
            dma((1,)),
            dma((1,)),
            dma((3,)),
            dma((1,)),
            dma((1,)),
        ],
        compiler_params=pltpu.CompilerParams(collective_id=0, has_side_effects=True),
        name="spilled_attention",
    )(*args)


def solution(mesh):
    placed = (
        P("dp", "mp", None),
        P("dp", None, "mp", None),
        P("dp", None, None, None, "mp", None),
        P("mp", None, None),
        P("mp", None, None),
        P(),
        P(),
        P("mp", "dp"),
    )
    nz = mesh.shape["mp"]
    ny = mesh.shape["dp"] // nz
    return jax.shard_map(
        functools.partial(body, nz, ny),
        mesh=mesh,
        in_specs=placed,
        out_specs=P("mp", "dp"),
        check_vma=False,
    )
```

```python
import functools
import math

import jax
import jax.numpy as jnp
from jax import lax
from jax.experimental import pallas as pl
from jax.experimental.pallas import tpu as pltpu
from jax.sharding import PartitionSpec as P

MESH = pl.DeviceIdType.MESH
very_low = -1e30
f32, bf16, i32 = jnp.float32, jnp.bfloat16, jnp.int32

SEQS = 8
HEADS = 8
SLOTS = 2
PAGE = 128
LANES = 128
RANK = 64


def iota(shape, dim):
    return lax.broadcasted_iota(i32, shape, dim)


def ones_where(condition, kind=bf16):
    return jnp.where(condition, 1.0, 0.0).astype(kind)


def dot(a, b):
    return jnp.dot(a, b, preferred_element_type=f32)


def dot_last(a, b):
    return lax.dot_general(a, b, (((1,), (1,)), ((), ())), preferred_element_type=f32)


def dot_first(a, b):
    return lax.dot_general(a, b, (((0,), (0,)), ((), ())), preferred_element_type=f32)


def rounded(x):
    return x.astype(bf16).astype(f32)


def three_pieces(x):
    top = rounded(x)
    middle = rounded(x - top)
    return top, middle, (x - top) - middle


def distance_order(nz):
    return sorted(range(nz), key=lambda dz: (min(dz, nz - dz), dz))


def batches(order, sizes):
    cut, at = [], 0
    for size in sizes:
        if order[at : at + size]:
            cut.append(order[at : at + size])
        at += size
    return cut


def kernel(
    nz,
    ny,
    nm,
    scale,
    q_hbm,
    res_ref,
    ovf_ref,
    wk_hbm,
    wv_hbm,
    len_hbm,
    rt_hbm,
    w_ref,
    out_ref,
    q_ref,
    wk_ref,
    wv_ref,
    len_ref,
    rt_ref,
    pages,
    resident,
    keys,
    values,
    wbuf,
    w_top,
    w_low,
    chosen,
    counts,
    q_send,
    q_recv,
    p_send,
    p_recv,
    own_lat,
    all_lat,
    own_part,
    r_send,
    r_recv,
    page_sem,
    local_sem,
    qs_sem,
    qr_sem,
    ps_sem,
    pr_sem,
    as_sem,
    ar_sem,
    rs_sem,
    rr_sem,
    ws_sem,
    wr_sem,
):
    me, mp = lax.axis_index("dp"), lax.axis_index("mp")
    z, y = lax.div(me, ny), lax.rem(me, ny)
    groups = nz * ny
    core, partner = lax.rem(mp, 2), mp + 1
    half = nm // 2
    items = groups * SLOTS
    rows = items * HEADS
    tail = rt_ref.shape[0]
    total = groups * SEQS
    home_tokens = resident.shape[1]

    def group_at(dz, dy):
        return lax.rem(z + dz, nz) * ny + lax.rem(y + dy, ny)

    def holder_at(dz, ya):
        return lax.rem(z + dz, nz) * ny + ya

    def source_at(dz, ya):
        return lax.rem(z + nz - dz, nz) * ny + ya

    def others_in_plane(dz):
        return [lax.rem(y + dy, ny) for dy in range(1 if dz == 0 else 0, ny)]

    barrier = pltpu.get_barrier_semaphore()

    near_first = distance_order(nz)
    far_first = near_first[::-1]
    serve_batches = [[0]] + batches([dz for dz in far_first if dz], (4, 3))
    project_batches = [[0]] + batches([dz for dz in far_first if dz], (4, 3))

    def batch_of(dz, cut):
        return next(i for i, batch in enumerate(cut) if dz in batch)

    def slots_in(batch):
        return sum(ny - (dz == 0) for dz in batch)

    for dz in far_first:
        for ya in others_in_plane(dz):
            pl.semaphore_signal(
                barrier, inc=1, device_id=(holder_at(dz, ya), mp), device_id_type=MESH
            )
    for step in range(1, nm):
        pl.semaphore_signal(
            barrier, inc=1, device_id=(me, lax.rem(mp + step, nm)), device_id_type=MESH
        )

    small = [
        pltpu.make_async_copy(source, target, local_sem.at[i])
        for i, (source, target) in enumerate(
            [
                (rt_hbm, rt_ref),
                (len_hbm, len_ref),
                (q_hbm, q_ref),
                (wk_hbm, wk_ref),
                (wv_hbm, wv_ref),
                (res_ref, resident),
                (w_ref, wbuf),
            ]
        )
    ]
    for copy in small:
        copy.start()
    for i, batch in enumerate(serve_batches):
        for dz in batch:
            first = lax.rem(z + nz - dz, nz) * ny
            pltpu.make_async_copy(
                ovf_ref.at[pl.ds(first, ny)], pages.at[pl.ds(dz * ny, ny)], page_sem.at[i]
            ).start()
    for copy in small[:5]:
        copy.wait()

    routes = jnp.concatenate([rt_ref[p] for p in range(tail)], axis=0).astype(f32)
    lens = len_ref[...].astype(f32)

    entry = iota((items, LANES), 0)
    lane = iota((items, LANES), 1)
    entry_dz, entry_y, entry_c = entry // (ny * SLOTS), (entry // SLOTS) % ny, entry % SLOTS
    holder = (((z + entry_dz) % nz) * ny + entry_y).astype(f32)
    own_columns = ones_where(
        iota((total, LANES), 0) == me * SEQS + iota((total, LANES), 1) % SEQS
    )
    own_routes = dot(routes.astype(bf16), own_columns)
    named = [jnp.where(own_routes[p : p + 1] == holder, 1.0, 0.0) for p in range(tail)]
    row_l, column_l = iota((LANES, LANES), 0), iota((LANES, LANES), 1)
    earlier = ones_where(
        (row_l // SEQS == column_l // SEQS) & (row_l % SEQS < column_l % SEQS)
    )
    before = dot(functools.reduce(jnp.add, named).astype(bf16), earlier)
    picked = jnp.zeros((items, LANES), f32)
    wanted = entry_c.astype(f32)
    for match in named:
        picked = picked + jnp.where(before == wanted, match, 0.0)
        before = before + match
    expand = ones_where(iota((rows, items), 0) // HEADS == iota((rows, items), 1))
    row = iota((rows, LANES), 0)
    row_lane = iota((rows, LANES), 1)
    same_head = row_lane // SEQS == row % HEADS
    picks = jnp.where(same_head, dot(expand, picked.astype(bf16)), 0.0).astype(bf16)

    home_row, home_lane = iota((64, LANES), 0), iota((64, LANES), 1)
    turned = ones_where(
        (home_lane // SEQS == home_row % HEADS) & (home_lane % SEQS == home_row // HEADS)
    )
    queries = q_ref[...]
    by_head = dot_first(turned, queries).astype(bf16)
    q_send[...] = dot(picks, by_head).astype(bf16).reshape(groups, SLOTS * HEADS, LANES)

    sequence = iota((total, total), 0)
    later = iota((total, total), 1)
    held_before = ones_where((sequence // SEQS == later // SEQS) & (sequence < later))
    here = jnp.where(routes == me.astype(f32), 1.0, 0.0)
    rank = dot(jnp.sum(here, axis=0, keepdims=True).astype(bf16), held_before)
    room = [jnp.zeros((1, total), f32) for _ in range(SLOTS)]
    for p in range(tail):
        match = here[p : p + 1]
        valid = jnp.clip(lens - (home_tokens + p * PAGE), 0.0, float(PAGE)) * match
        for c in range(SLOTS):
            room[c] = room[c] + jnp.where(rank == float(c), valid, 0.0)
        rank = rank + match
    entry_s = iota((items, total), 0)
    column_s = iota((items, total), 1)
    source = ((z + nz - entry_s // (ny * SLOTS)) % nz) * ny + (entry_s // SLOTS) % ny
    sized = jnp.where(entry_s % SLOTS == 0, room[0], room[1])
    sized = jnp.where(column_s // SEQS == source, sized, 0.0).astype(bf16)
    all_ones = jnp.ones((total, LANES), bf16)
    per_item = dot(sized, all_ones).astype(bf16)
    counts[...] = dot(expand, per_item)

    home_s = iota((64, total), 1) == me * SEQS + iota((64, total), 0) // HEADS
    home_count = dot(
        jnp.where(home_s, jnp.minimum(lens, float(home_tokens)), 0.0).astype(bf16), all_ones
    )

    pl.semaphore_wait(barrier, groups - 1 + nm - 1)

    def query_copy(dz, ya, peer):
        return pltpu.make_async_remote_copy(
            src_ref=q_send.at[dz * ny + ya],
            dst_ref=q_recv.at[dz * ny + y],
            send_sem=qs_sem.at[0],
            recv_sem=qr_sem.at[batch_of(dz, serve_batches)],
            device_id=(peer, mp),
            device_id_type=MESH,
        )

    def part_copy(dz, ya, peer):
        return pltpu.make_async_remote_copy(
            src_ref=p_send.at[dz * ny + ya],
            dst_ref=p_recv.at[dz * ny + y],
            send_sem=ps_sem.at[0],
            recv_sem=pr_sem.at[0],
            device_id=(peer, mp),
            device_id_type=MESH,
        )

    def many(source, target, count, send_sem, recv_sem):
        return pltpu.make_async_remote_copy(
            src_ref=source.at[pl.ds(0, count)],
            dst_ref=target.at[pl.ds(0, count)],
            send_sem=send_sem,
            recv_sem=recv_sem,
            device_id=(me, mp),
            device_id_type=MESH,
        )

    for dz in far_first:
        for ya in others_in_plane(dz):
            query_copy(dz, ya, holder_at(dz, ya)).start()
    q_recv[y] = q_send[y]

    wk_wide = jnp.concatenate([wk_ref[...], jnp.zeros((RANK, LANES), bf16)], axis=0)

    def message(best, sums, mixed):
        at = iota(mixed.shape, 1)
        best_pieces, sum_pieces = three_pieces(best), three_pieces(sums)
        packed = mixed
        for i in range(3):
            packed = jnp.where(at == i, best_pieces[i], packed)
            packed = jnp.where(at == 3 + i, sum_pieces[i], packed)
        return packed, at

    def partials(query_rows, latents, token_count):
        folded = three_pieces(dot_last(query_rows, wk_wide))
        scores = []
        for i, latent in enumerate(latents):
            stacked = jnp.concatenate([f[8 * i : 8 * i + 8] for f in folded], axis=0)
            s = dot_last(stacked.astype(bf16), latent)
            scores.append(s[0:8] + s[8:16] + s[16:24])
        scores = jnp.concatenate(scores, axis=0) * scale
        mask = iota(scores.shape, 1).astype(f32) < token_count
        scores = jnp.where(mask, scores, very_low)
        best = jnp.max(scores, axis=1, keepdims=True)
        weights = jnp.where(mask, jnp.exp(scores - best), 0.0)
        sums = jnp.sum(weights, axis=1, keepdims=True)
        top = rounded(weights)
        low = weights - top
        mixed = []
        for i, latent in enumerate(latents):
            stacked = jnp.concatenate([top[8 * i : 8 * i + 8], low[8 * i : 8 * i + 8]], axis=0)
            o = dot(stacked.astype(bf16), latent)
            mixed.append(o[0:8] + o[8:16])
        return best, sums, jnp.concatenate(mixed, axis=0)

    square = ones_where(home_row == home_lane)
    chosen[:, pl.ds(0, rows)] = dot_last(square, picks)
    turned_back = dot_last(square, turned)
    chosen[:, pl.ds(rows, 128)] = jnp.concatenate([turned_back, turned_back], axis=1)
    small[5].wait()
    wide_count = jnp.concatenate([home_count] * (home_tokens // LANES), axis=1)
    best, sums, mixed = partials(queries, [resident[k] for k in range(SEQS)], wide_count)
    packed, at = message(best, sums, mixed)
    p_recv[pl.ds(groups, 4)] = packed.astype(bf16).reshape(4, 16, LANES)
    remainder = jnp.where((at >= 3) & (at < RANK), 0.0, packed - rounded(packed))
    remainder = jnp.where(at < 3, packed, remainder)
    p_recv[pl.ds(groups + 4, 4)] = remainder.astype(bf16).reshape(4, 16, LANES)

    small[6].wait()
    for h in range(HEADS):
        joined = dot(wv_ref[...], wbuf[pl.ds(h * LANES, LANES), :])
        w_top[core, pl.ds(h * RANK, RANK), :] = joined.astype(bf16)
        w_low[core, pl.ds(h * RANK, RANK), :] = (joined - rounded(joined)).astype(bf16)

    def weight_handover(which, array):
        return pltpu.make_async_remote_copy(
            src_ref=array.at[0],
            dst_ref=array.at[0],
            send_sem=ws_sem.at[which],
            recv_sem=wr_sem.at[which],
            device_id=(me, partner),
            device_id_type=MESH,
        )

    @pl.when(core == 0)
    def _():
        weight_handover(0, w_top).start()
        weight_handover(1, w_low).start()

    pick_keys = ones_where(iota((RANK, LANES), 0) == iota((RANK, LANES), 1))
    for i, batch in enumerate(serve_batches):
        held = len(batch) * ny
        pltpu.make_async_copy(
            ovf_ref.at[pl.ds(0, held)], pages.at[pl.ds(0, held)], page_sem.at[i]
        ).wait()
        for slot in [dz * ny + ya for dz in batch for ya in range(ny)]:
            page_pair = pages[slot]
            turned_keys = dot_last(pick_keys, page_pair).astype(bf16)
            keys[slot, pl.ds(0, RANK), :] = turned_keys[:, 0:PAGE]
            keys[slot, pl.ds(RANK, RANK), :] = turned_keys[:, PAGE : 2 * PAGE]
            values[slot] = jnp.concatenate(
                [page_pair[PAGE : 2 * PAGE, RANK:], page_pair[0:PAGE, RANK:]], axis=1
            )

    wk_twice = jnp.concatenate([wk_ref[...], wk_ref[...]], axis=0)

    def served(query_rows, slots, token_count):
        at, row_at = iota(query_rows.shape, 1), iota(query_rows.shape, 0)
        second = (row_at // HEADS) % SLOTS == 1
        folded = dot_last(query_rows, wk_twice)
        folded = jnp.where((at >= RANK) == second, folded, 0.0)
        top = folded.astype(bf16)
        rest = folded - top.astype(f32)
        middle = rest.astype(bf16)
        low = (rest - middle.astype(f32)).astype(bf16)
        scores = []
        for i, slot in enumerate(slots):
            part = slice(16 * i, 16 * i + 16)
            s = dot(jnp.concatenate([top[part], middle[part], low[part]], axis=0), keys[slot])
            scores.append(s[0:16] + s[16:32] + s[32:48])
        scores = jnp.concatenate(scores, axis=0) * scale
        mask = at.astype(f32) < token_count
        scores = jnp.where(mask, scores, very_low)
        best = jnp.max(scores, axis=1, keepdims=True)
        weights = jnp.where(mask, jnp.exp(scores - best), 0.0)
        sums = jnp.sum(weights, axis=1, keepdims=True)
        top = weights.astype(bf16)
        low = (weights - top.astype(f32)).astype(bf16)
        mixed = []
        for i, slot in enumerate(slots):
            part = slice(16 * i, 16 * i + 16)
            o = dot(jnp.concatenate([top[part], low[part]], axis=0), values[slot])
            mixed.append(o[0:16] + o[16:32])
        mixed = jnp.concatenate(mixed, axis=0)
        return best, sums, jnp.where(second, pltpu.roll(mixed, RANK, 1), mixed)

    chunk = ny * SLOTS * HEADS
    for i, batch in enumerate(serve_batches):
        many(q_send, q_recv, slots_in(batch), qs_sem.at[0], qr_sem.at[i]).wait_recv()
        block = jnp.concatenate(
            [q_recv[pl.ds(dz * ny, ny)].reshape(chunk, LANES) for dz in batch], axis=0
        )
        token_count = jnp.concatenate(
            [counts[pl.ds(dz * chunk, chunk), :] for dz in batch], axis=0
        )
        slots = [dz * ny + ya for dz in batch for ya in range(ny)]
        best, sums, mixed = served(block, slots, token_count)
        packed, _ = message(best, sums, mixed)
        packed = packed.astype(bf16).reshape(len(batch) * ny, SLOTS * HEADS, LANES)
        for n, dz in enumerate(batch):
            p_send[pl.ds(dz * ny, ny)] = packed[n * ny : (n + 1) * ny]
        for dz in batch:
            for ya in others_in_plane(dz):
                part_copy(dz, ya, source_at(dz, ya)).start()
            if dz == 0:
                p_recv[y] = p_send[y]

    many(p_send, p_recv, groups - 1, ps_sem.at[0], pr_sem.at[0]).wait_recv()
    parts = p_recv[...].reshape(rows + 128, LANES)
    peaks = dot_last(ones_where(iota((SEQS, LANES), 1) < 3), parts)
    peaks = jnp.broadcast_to(peaks[0:1], chosen.shape)
    member = chosen[...] > 0.5
    peak = jnp.max(jnp.where(member, peaks, very_low), axis=1, keepdims=True)
    factor = jnp.where(member, jnp.exp(peaks - peak), 0.0)
    factor_top = rounded(factor)
    merged = dot(
        jnp.concatenate([factor_top, factor - factor_top], axis=0).astype(bf16), parts
    )
    merged = merged[0:64] + merged[64:128]
    merged_sum = merged[:, 3:4] + merged[:, 4:5] + merged[:, 5:6]
    latent = merged / merged_sum
    low_lane = iota((SEQS, LANES), 1) < RANK
    for v in range(HEADS // 2):
        even = latent[16 * v : 16 * v + 8]
        odd = latent[16 * v + 8 : 16 * v + 16]
        own_lat[:, pl.ds(v * LANES, LANES)] = jnp.where(
            low_lane, pltpu.roll(even, RANK, 1), odd
        ).astype(bf16)

    def latent_copy(dz, peer):
        return pltpu.make_async_remote_copy(
            src_ref=own_lat,
            dst_ref=all_lat.at[core * groups + me],
            send_sem=as_sem.at[0],
            recv_sem=ar_sem.at[batch_of(dz, project_batches)],
            device_id=(peer, lax.div(mp, 2) * 2 + 1),
            device_id_type=MESH,
        )

    for dz in far_first:
        for ya in others_in_plane(dz):
            latent_copy(dz, holder_at(dz, ya)).start()

    @pl.when(core == 0)
    def _():
        latent_copy(0, me).start()

    @pl.when(core == 1)
    def _():
        all_lat[groups + me] = own_lat[...]

    def sum_copy(target):
        place = lax.rem(lax.div(mp, 2) + half - lax.div(target, 2), half)
        return pltpu.make_async_remote_copy(
            src_ref=r_send.at[target],
            dst_ref=r_recv.at[place],
            send_sem=rs_sem.at[0],
            recv_sem=rr_sem.at[0],
            device_id=(me, target),
            device_id_type=MESH,
        )

    def project(batch):
        part = None
        for c in range(2):
            block = jnp.concatenate(
                [
                    all_lat[
                        pl.ds(c * groups + lax.rem(z + nz - dz, nz) * ny, ny)
                    ].reshape(ny * SEQS, HEADS * RANK)
                    for dz in batch
                ],
                axis=0,
            )
            added = dot(block, w_top[c]) + dot(block, w_low[c])
            part = added if part is None else part + added
        for n, dz in enumerate(batch):
            target = lax.rem(z + nz - dz, nz)
            piece = part[n * ny * SEQS : (n + 1) * ny * SEQS]

            @pl.when(target == mp)
            def _():
                own_part[...] = piece

            @pl.when(target != mp)
            def _():
                r_send[target] = piece.astype(bf16)
                sum_copy(target).start()

    @pl.when(core == 1)
    def _():
        weight_handover(0, w_top).wait_recv()
        weight_handover(1, w_low).wait_recv()
        for i, batch in enumerate(project_batches):
            landed = slots_in(batch) + len(batch) * ny
            many(all_lat, all_lat, landed, as_sem.at[0], ar_sem.at[i]).wait_recv()
            project(batch)
        many(r_send, r_recv, half - 1, rs_sem.at[0], rr_sem.at[0]).wait_recv()

    @pl.when(core == 0)
    def _():
        many(r_send, r_recv, half, rs_sem.at[0], rr_sem.at[0]).wait_recv()
        own_part[...] = r_recv[0].astype(f32)

    summed = own_part[...]
    for place in range(1, half):
        summed = summed + r_recv[place].astype(f32)
    out_ref[...] = summed.astype(bf16)
    many(q_send, q_recv, groups - 1, qs_sem.at[0], qr_sem.at[0]).wait_send()
    many(p_send, p_recv, groups - 1, ps_sem.at[0], pr_sem.at[0]).wait_send()

    @pl.when(core == 0)
    def _():
        weight_handover(0, w_top).wait_send()
        weight_handover(1, w_low).wait_send()
        many(all_lat, all_lat, groups, as_sem.at[0], ar_sem.at[0]).wait_send()

    @pl.when(core == 1)
    def _():
        many(all_lat, all_lat, groups - 1, as_sem.at[0], ar_sem.at[0]).wait_send()
        many(r_send, r_send, nm - 1, rs_sem.at[0], rr_sem.at[0]).wait_send()


def body(
    nz,
    ny,
    queries,
    resident_cache,
    overflow_cache,
    key_up_weight,
    value_up_weight,
    lengths,
    routes,
    out_weight,
):
    nm = lax.axis_size("mp")
    groups = nz * ny
    home_tokens = resident_cache.shape[1]
    out_columns = out_weight.shape[1]
    total = lengths.shape[0]
    tail = routes.shape[1]
    rows = groups * SLOTS * HEADS
    args = (
        queries.reshape(SEQS * HEADS, LANES),
        resident_cache.reshape(SEQS, home_tokens, LANES),
        overflow_cache.reshape(groups, SLOTS * PAGE, LANES),
        key_up_weight.reshape(RANK, LANES),
        value_up_weight.reshape(RANK, LANES),
        lengths.reshape(1, total),
        routes.transpose(1, 2, 0),
        out_weight,
    )
    in_vmem = pl.BlockSpec(memory_space=pltpu.VMEM)
    anywhere = pl.BlockSpec(memory_space=pl.ANY)
    dma = pltpu.SemaphoreType.DMA
    return pl.pallas_call(
        functools.partial(kernel, nz, ny, nm, 1.0 / math.sqrt(LANES)),
        out_shape=pltpu.VMEM((ny * SEQS, out_columns), bf16),
        in_specs=[anywhere] * 8,
        out_specs=in_vmem,
        scratch_shapes=[
            pltpu.VMEM((SEQS * HEADS, LANES), bf16),
            pltpu.VMEM((RANK, LANES), bf16),
            pltpu.VMEM((RANK, LANES), bf16),
            pltpu.VMEM((1, total), i32),
            pltpu.VMEM((tail, 1, total), i32),
            pltpu.VMEM((groups, SLOTS * PAGE, LANES), bf16),
            pltpu.VMEM((SEQS, home_tokens, LANES), bf16),
            pltpu.VMEM((groups, SLOTS * RANK, PAGE), bf16),
            pltpu.VMEM((groups, PAGE, SLOTS * RANK), bf16),
            pltpu.VMEM(out_weight.shape, bf16),
            pltpu.VMEM((2, HEADS * RANK, out_columns), bf16),
            pltpu.VMEM((2, HEADS * RANK, out_columns), bf16),
            pltpu.VMEM((SEQS * HEADS, rows + 128), f32),
            pltpu.VMEM((rows, LANES), f32),
            pltpu.VMEM((groups, SLOTS * HEADS, LANES), bf16),
            pltpu.VMEM((groups, SLOTS * HEADS, LANES), bf16),
            pltpu.VMEM((groups, SLOTS * HEADS, LANES), bf16),
            pltpu.VMEM((groups + 8, SLOTS * HEADS, LANES), bf16),
            pltpu.VMEM((SEQS, HEADS * RANK), bf16),
            pltpu.VMEM((2 * groups, SEQS, HEADS * RANK), bf16),
            pltpu.VMEM((ny * SEQS, out_columns), f32),
            pltpu.VMEM((nm, ny * SEQS, out_columns), bf16),
            pltpu.VMEM((nm // 2, ny * SEQS, out_columns), bf16),
            dma((5,)),
            dma((7,)),
            dma((1,)),
            dma((5,)),
            dma((1,)),
            dma((1,)),
            dma((1,)),
            dma((3,)),
            dma((1,)),
            dma((1,)),
            dma((2,)),
            dma((2,)),
        ],
        compiler_params=pltpu.CompilerParams(collective_id=0, has_side_effects=True),
        name="spilled_attention",
    )(*args)


def solution(mesh):
    placed = (
        P("dp", "mp", None),
        P("dp", None, "mp", None),
        P("dp", None, None, None, "mp", None),
        P("mp", None, None),
        P("mp", None, None),
        P(),
        P(),
        P("mp", "dp"),
    )
    nz = mesh.shape["mp"]
    ny = mesh.shape["dp"] // nz
    return jax.shard_map(
        functools.partial(body, nz, ny),
        mesh=mesh,
        in_specs=placed,
        out_specs=P("mp", "dp"),
        check_vma=False,
    )
```

```python
import functools
import math

import jax
import jax.numpy as jnp
from jax import lax
from jax.experimental import pallas as pl
from jax.experimental.pallas import tpu as pltpu
from jax.sharding import PartitionSpec as P

MESH = pl.DeviceIdType.MESH
very_low = -1e30
f32, bf16, i32 = jnp.float32, jnp.bfloat16, jnp.int32

SEQS = 8
HEADS = 8
SLOTS = 2
PAGE = 128
LANES = 128
RANK = 64


def iota(shape, dim):
    return lax.broadcasted_iota(i32, shape, dim)


def ones_where(condition, kind=bf16):
    return jnp.where(condition, 1.0, 0.0).astype(kind)


def dot(a, b):
    return jnp.dot(a, b, preferred_element_type=f32)


def dot_last(a, b):
    return lax.dot_general(a, b, (((1,), (1,)), ((), ())), preferred_element_type=f32)


def dot_first(a, b):
    return lax.dot_general(a, b, (((0,), (0,)), ((), ())), preferred_element_type=f32)


def rounded(x):
    return x.astype(bf16).astype(f32)


def three_pieces(x):
    top = rounded(x)
    middle = rounded(x - top)
    return top, middle, (x - top) - middle


def distance_order(nz):
    return sorted(range(nz), key=lambda dz: (min(dz, nz - dz), -dz))


def batches(order, sizes):
    cut, at = [], 0
    for size in sizes:
        if order[at : at + size]:
            cut.append(order[at : at + size])
        at += size
    return cut


def kernel(
    nz,
    ny,
    nm,
    scale,
    q_hbm,
    res_ref,
    ovf_ref,
    wk_hbm,
    wv_hbm,
    len_hbm,
    rt_hbm,
    w_ref,
    out_ref,
    q_ref,
    wk_ref,
    wv_ref,
    len_ref,
    rt_ref,
    pages,
    resident,
    keys,
    values,
    wbuf,
    w_top,
    w_low,
    chosen,
    counts,
    q_send,
    q_recv,
    p_send,
    p_recv,
    own_lat,
    all_lat,
    own_part,
    r_send,
    r_recv,
    page_sem,
    local_sem,
    qs_sem,
    qr_sem,
    ps_sem,
    pr_sem,
    as_sem,
    ar_sem,
    rs_sem,
    rr_sem,
    ws_sem,
    wr_sem,
):
    me, mp = lax.axis_index("dp"), lax.axis_index("mp")
    z, y = lax.div(me, ny), lax.rem(me, ny)
    groups = nz * ny
    core, partner = lax.rem(mp, 2), mp + 1
    half = nm // 2
    items = groups * SLOTS
    rows = items * HEADS
    tail = rt_ref.shape[0]
    total = groups * SEQS
    home_tokens = resident.shape[1]

    def group_at(dz, dy):
        return lax.rem(z + dz, nz) * ny + lax.rem(y + dy, ny)

    def holder_at(dz, ya):
        return lax.rem(z + dz, nz) * ny + ya

    def source_at(dz, ya):
        return lax.rem(z + nz - dz, nz) * ny + ya

    def others_in_plane(dz):
        return [lax.rem(y + dy, ny) for dy in range(1 if dz == 0 else 0, ny)]

    barrier = pltpu.get_barrier_semaphore()

    near_first = distance_order(nz)
    far_first = near_first[::-1]
    serve_batches = [[0]] + batches([dz for dz in far_first if dz], (4, 3))
    project_batches = batches(near_first, (1, 1, 2, 2, 2))

    def batch_of(dz, cut):
        return next(i for i, batch in enumerate(cut) if dz in batch)

    def slots_in(batch):
        return sum(ny - (dz == 0) for dz in batch)

    for dz in far_first:
        for ya in others_in_plane(dz):
            pl.semaphore_signal(
                barrier, inc=1, device_id=(holder_at(dz, ya), mp), device_id_type=MESH
            )
    for step in range(1, nm):
        pl.semaphore_signal(
            barrier, inc=1, device_id=(me, lax.rem(mp + step, nm)), device_id_type=MESH
        )

    small = [
        pltpu.make_async_copy(source, target, local_sem.at[i])
        for i, (source, target) in enumerate(
            [
                (rt_hbm, rt_ref),
                (len_hbm, len_ref),
                (q_hbm, q_ref),
                (wk_hbm, wk_ref),
                (wv_hbm, wv_ref),
                (res_ref, resident),
                (w_ref, wbuf),
            ]
        )
    ]
    for copy in small:
        copy.start()
    for i, batch in enumerate(serve_batches):
        for dz in batch:
            first = lax.rem(z + nz - dz, nz) * ny
            pltpu.make_async_copy(
                ovf_ref.at[pl.ds(first, ny)], pages.at[pl.ds(dz * ny, ny)], page_sem.at[i]
            ).start()
    for copy in small[:5]:
        copy.wait()

    routes = jnp.concatenate([rt_ref[p] for p in range(tail)], axis=0).astype(f32)
    lens = len_ref[...].astype(f32)

    entry = iota((items, LANES), 0)
    lane = iota((items, LANES), 1)
    entry_dz, entry_y, entry_c = entry // (ny * SLOTS), (entry // SLOTS) % ny, entry % SLOTS
    holder = (((z + entry_dz) % nz) * ny + entry_y).astype(f32)
    own_columns = ones_where(
        iota((total, LANES), 0) == me * SEQS + iota((total, LANES), 1) % SEQS
    )
    own_routes = dot(routes.astype(bf16), own_columns)
    named = [jnp.where(own_routes[p : p + 1] == holder, 1.0, 0.0) for p in range(tail)]
    row_l, column_l = iota((LANES, LANES), 0), iota((LANES, LANES), 1)
    earlier = ones_where(
        (row_l // SEQS == column_l // SEQS) & (row_l % SEQS < column_l % SEQS)
    )
    before = dot(functools.reduce(jnp.add, named).astype(bf16), earlier)
    picked = jnp.zeros((items, LANES), f32)
    wanted = entry_c.astype(f32)
    for match in named:
        picked = picked + jnp.where(before == wanted, match, 0.0)
        before = before + match
    expand = ones_where(iota((rows, items), 0) // HEADS == iota((rows, items), 1))
    row = iota((rows, LANES), 0)
    row_lane = iota((rows, LANES), 1)
    same_head = row_lane // SEQS == row % HEADS
    picks = jnp.where(same_head, dot(expand, picked.astype(bf16)), 0.0).astype(bf16)

    home_row, home_lane = iota((64, LANES), 0), iota((64, LANES), 1)
    turned = ones_where(
        (home_lane // SEQS == home_row % HEADS) & (home_lane % SEQS == home_row // HEADS)
    )
    queries = q_ref[...]
    by_head = dot_first(turned, queries).astype(bf16)
    q_send[...] = dot(picks, by_head).astype(bf16).reshape(groups, SLOTS * HEADS, LANES)

    sequence = iota((total, total), 0)
    later = iota((total, total), 1)
    held_before = ones_where((sequence // SEQS == later // SEQS) & (sequence < later))
    here = jnp.where(routes == me.astype(f32), 1.0, 0.0)
    rank = dot(jnp.sum(here, axis=0, keepdims=True).astype(bf16), held_before)
    room = [jnp.zeros((1, total), f32) for _ in range(SLOTS)]
    for p in range(tail):
        match = here[p : p + 1]
        valid = jnp.clip(lens - (home_tokens + p * PAGE), 0.0, float(PAGE)) * match
        for c in range(SLOTS):
            room[c] = room[c] + jnp.where(rank == float(c), valid, 0.0)
        rank = rank + match
    entry_s = iota((items, total), 0)
    column_s = iota((items, total), 1)
    source = ((z + nz - entry_s // (ny * SLOTS)) % nz) * ny + (entry_s // SLOTS) % ny
    sized = jnp.where(entry_s % SLOTS == 0, room[0], room[1])
    sized = jnp.where(column_s // SEQS == source, sized, 0.0).astype(bf16)
    all_ones = jnp.ones((total, LANES), bf16)
    per_item = dot(sized, all_ones).astype(bf16)
    counts[...] = dot(expand, per_item)

    home_s = iota((64, total), 1) == me * SEQS + iota((64, total), 0) // HEADS
    home_count = dot(
        jnp.where(home_s, jnp.minimum(lens, float(home_tokens)), 0.0).astype(bf16), all_ones
    )

    pl.semaphore_wait(barrier, groups - 1 + nm - 1)

    def query_copy(dz, ya, peer):
        return pltpu.make_async_remote_copy(
            src_ref=q_send.at[dz * ny + ya],
            dst_ref=q_recv.at[dz * ny + y],
            send_sem=qs_sem.at[0],
            recv_sem=qr_sem.at[batch_of(dz, serve_batches)],
            device_id=(peer, mp),
            device_id_type=MESH,
        )

    def part_copy(dz, ya, peer):
        return pltpu.make_async_remote_copy(
            src_ref=p_send.at[dz * ny + ya],
            dst_ref=p_recv.at[dz * ny + y],
            send_sem=ps_sem.at[0],
            recv_sem=pr_sem.at[0],
            device_id=(peer, mp),
            device_id_type=MESH,
        )

    def many(source, target, count, send_sem, recv_sem):
        return pltpu.make_async_remote_copy(
            src_ref=source.at[pl.ds(0, count)],
            dst_ref=target.at[pl.ds(0, count)],
            send_sem=send_sem,
            recv_sem=recv_sem,
            device_id=(me, mp),
            device_id_type=MESH,
        )

    for dz in far_first:
        for ya in others_in_plane(dz):
            query_copy(dz, ya, holder_at(dz, ya)).start()
    q_recv[y] = q_send[y]

    wk_wide = jnp.concatenate([wk_ref[...], jnp.zeros((RANK, LANES), bf16)], axis=0)

    def message(best, sums, mixed):
        at = iota(mixed.shape, 1)
        best_pieces, sum_pieces = three_pieces(best), three_pieces(sums)
        packed = mixed
        for i in range(3):
            packed = jnp.where(at == i, best_pieces[i], packed)
            packed = jnp.where(at == 3 + i, sum_pieces[i], packed)
        return packed, at

    def partials(query_rows, latents, token_count):
        folded = three_pieces(dot_last(query_rows, wk_wide))
        scores = []
        for i, latent in enumerate(latents):
            stacked = jnp.concatenate([f[8 * i : 8 * i + 8] for f in folded], axis=0)
            s = dot_last(stacked.astype(bf16), latent)
            scores.append(s[0:8] + s[8:16] + s[16:24])
        scores = jnp.concatenate(scores, axis=0) * scale
        mask = iota(scores.shape, 1).astype(f32) < token_count
        scores = jnp.where(mask, scores, very_low)
        best = jnp.max(scores, axis=1, keepdims=True)
        weights = jnp.where(mask, jnp.exp(scores - best), 0.0)
        sums = jnp.sum(weights, axis=1, keepdims=True)
        top = rounded(weights)
        low = weights - top
        mixed = []
        for i, latent in enumerate(latents):
            stacked = jnp.concatenate([top[8 * i : 8 * i + 8], low[8 * i : 8 * i + 8]], axis=0)
            o = dot(stacked.astype(bf16), latent)
            mixed.append(o[0:8] + o[8:16])
        return best, sums, jnp.concatenate(mixed, axis=0)

    square = ones_where(home_row == home_lane)
    chosen[:, pl.ds(0, rows)] = dot_last(square, picks)
    turned_back = dot_last(square, turned)
    chosen[:, pl.ds(rows, 128)] = jnp.concatenate([turned_back, turned_back], axis=1)
    small[5].wait()
    wide_count = jnp.concatenate([home_count] * (home_tokens // LANES), axis=1)
    best, sums, mixed = partials(queries, [resident[k] for k in range(SEQS)], wide_count)
    packed, at = message(best, sums, mixed)
    p_recv[pl.ds(groups, 4)] = packed.astype(bf16).reshape(4, 16, LANES)
    remainder = jnp.where((at >= 3) & (at < RANK), 0.0, packed - rounded(packed))
    remainder = jnp.where(at < 3, packed, remainder)
    p_recv[pl.ds(groups + 4, 4)] = remainder.astype(bf16).reshape(4, 16, LANES)

    small[6].wait()
    for h in range(HEADS):
        joined = dot(wv_ref[...], wbuf[pl.ds(h * LANES, LANES), :])
        w_top[core, pl.ds(h * RANK, RANK), :] = joined.astype(bf16)
        w_low[core, pl.ds(h * RANK, RANK), :] = (joined - rounded(joined)).astype(bf16)

    def weight_handover(which, array):
        return pltpu.make_async_remote_copy(
            src_ref=array.at[0],
            dst_ref=array.at[0],
            send_sem=ws_sem.at[which],
            recv_sem=wr_sem.at[which],
            device_id=(me, partner),
            device_id_type=MESH,
        )

    @pl.when(core == 0)
    def _():
        weight_handover(0, w_top).start()
        weight_handover(1, w_low).start()

    pick_keys = ones_where(iota((RANK, LANES), 0) == iota((RANK, LANES), 1))
    for i, batch in enumerate(serve_batches):
        held = len(batch) * ny
        pltpu.make_async_copy(
            ovf_ref.at[pl.ds(0, held)], pages.at[pl.ds(0, held)], page_sem.at[i]
        ).wait()
        for slot in [dz * ny + ya for dz in batch for ya in range(ny)]:
            page_pair = pages[slot]
            turned_keys = dot_last(pick_keys, page_pair).astype(bf16)
            keys[slot, pl.ds(0, RANK), :] = turned_keys[:, 0:PAGE]
            keys[slot, pl.ds(RANK, RANK), :] = turned_keys[:, PAGE : 2 * PAGE]
            values[slot] = jnp.concatenate(
                [page_pair[PAGE : 2 * PAGE, RANK:], page_pair[0:PAGE, RANK:]], axis=1
            )

    wk_twice = jnp.concatenate([wk_ref[...], wk_ref[...]], axis=0)

    def served(query_rows, slots, token_count):
        at, row_at = iota(query_rows.shape, 1), iota(query_rows.shape, 0)
        second = (row_at // HEADS) % SLOTS == 1
        folded = dot_last(query_rows, wk_twice)
        folded = jnp.where((at >= RANK) == second, folded, 0.0)
        top = folded.astype(bf16)
        rest = folded - top.astype(f32)
        middle = rest.astype(bf16)
        low = (rest - middle.astype(f32)).astype(bf16)
        scores = []
        for i, slot in enumerate(slots):
            part = slice(16 * i, 16 * i + 16)
            s = dot(jnp.concatenate([top[part], middle[part], low[part]], axis=0), keys[slot])
            scores.append(s[0:16] + s[16:32] + s[32:48])
        scores = jnp.concatenate(scores, axis=0) * scale
        mask = at.astype(f32) < token_count
        scores = jnp.where(mask, scores, very_low)
        best = jnp.max(scores, axis=1, keepdims=True)
        weights = jnp.where(mask, jnp.exp(scores - best), 0.0)
        sums = jnp.sum(weights, axis=1, keepdims=True)
        top = weights.astype(bf16)
        low = (weights - top.astype(f32)).astype(bf16)
        mixed = []
        for i, slot in enumerate(slots):
            part = slice(16 * i, 16 * i + 16)
            o = dot(jnp.concatenate([top[part], low[part]], axis=0), values[slot])
            mixed.append(o[0:16] + o[16:32])
        mixed = jnp.concatenate(mixed, axis=0)
        return best, sums, jnp.where(second, pltpu.roll(mixed, RANK, 1), mixed)

    chunk = ny * SLOTS * HEADS
    for i, batch in enumerate(serve_batches):
        many(q_send, q_recv, slots_in(batch), qs_sem.at[0], qr_sem.at[i]).wait_recv()
        block = jnp.concatenate(
            [q_recv[pl.ds(dz * ny, ny)].reshape(chunk, LANES) for dz in batch], axis=0
        )
        token_count = jnp.concatenate(
            [counts[pl.ds(dz * chunk, chunk), :] for dz in batch], axis=0
        )
        slots = [dz * ny + ya for dz in batch for ya in range(ny)]
        best, sums, mixed = served(block, slots, token_count)
        packed, _ = message(best, sums, mixed)
        packed = packed.astype(bf16).reshape(len(batch) * ny, SLOTS * HEADS, LANES)
        for n, dz in enumerate(batch):
            p_send[pl.ds(dz * ny, ny)] = packed[n * ny : (n + 1) * ny]
        for dz in batch:
            for ya in others_in_plane(dz):
                part_copy(dz, ya, source_at(dz, ya)).start()
            if dz == 0:
                p_recv[y] = p_send[y]

    many(p_send, p_recv, groups - 1, ps_sem.at[0], pr_sem.at[0]).wait_recv()
    parts = p_recv[...].reshape(rows + 128, LANES)
    peaks = dot_last(ones_where(iota((SEQS, LANES), 1) < 3), parts)
    peaks = jnp.broadcast_to(peaks[0:1], chosen.shape)
    member = chosen[...] > 0.5
    peak = jnp.max(jnp.where(member, peaks, very_low), axis=1, keepdims=True)
    factor = jnp.where(member, jnp.exp(peaks - peak), 0.0)
    factor_top = rounded(factor)
    merged = dot(
        jnp.concatenate([factor_top, factor - factor_top], axis=0).astype(bf16), parts
    )
    merged = merged[0:64] + merged[64:128]
    merged_sum = merged[:, 3:4] + merged[:, 4:5] + merged[:, 5:6]
    latent = merged / merged_sum
    low_lane = iota((SEQS, LANES), 1) < RANK
    for v in range(HEADS // 2):
        even = latent[16 * v : 16 * v + 8]
        odd = latent[16 * v + 8 : 16 * v + 16]
        own_lat[:, pl.ds(v * LANES, LANES)] = jnp.where(
            low_lane, pltpu.roll(even, RANK, 1), odd
        ).astype(bf16)

    def latent_copy(dz, peer):
        return pltpu.make_async_remote_copy(
            src_ref=own_lat,
            dst_ref=all_lat.at[core * groups + me],
            send_sem=as_sem.at[0],
            recv_sem=ar_sem.at[dz],
            device_id=(peer, lax.div(mp, 2) * 2 + 1),
            device_id_type=MESH,
        )

    to_first = lax.rem(nz - z, nz)

    @pl.when(core == 0)
    def _():
        latent_copy(0, me).start()

    @pl.when(z != 0)
    def _():
        for ya in range(ny):
            latent_copy(to_first, ya).start()

    for dz in near_first:

        @pl.when((to_first != dz) | (dz == 0))
        def _():
            for ya in others_in_plane(dz):
                latent_copy(dz, holder_at(dz, ya)).start()

    @pl.when(core == 1)
    def _():
        all_lat[groups + me] = own_lat[...]

    def sum_copy(target):
        place = lax.rem(lax.div(mp, 2) + half - lax.div(target, 2), half)
        return pltpu.make_async_remote_copy(
            src_ref=r_send.at[target],
            dst_ref=r_recv.at[place],
            send_sem=rs_sem.at[0],
            recv_sem=rr_sem.at[0],
            device_id=(me, target),
            device_id_type=MESH,
        )

    def project(batch):
        part = None
        for c in range(2):
            block = jnp.concatenate(
                [
                    all_lat[
                        pl.ds(c * groups + lax.rem(z + nz - dz, nz) * ny, ny)
                    ].reshape(ny * SEQS, HEADS * RANK)
                    for dz in batch
                ],
                axis=0,
            )
            added = dot(block, w_top[c]) + dot(block, w_low[c])
            part = added if part is None else part + added
        for n, dz in enumerate(batch):
            target = lax.rem(z + nz - dz, nz)
            piece = part[n * ny * SEQS : (n + 1) * ny * SEQS]

            @pl.when(target == mp)
            def _():
                own_part[...] = piece

            @pl.when(target != mp)
            def _():
                r_send[target] = piece.astype(bf16)
                sum_copy(target).start()

    @pl.when(core == 1)
    def _():
        weight_handover(0, w_top).wait_recv()
        weight_handover(1, w_low).wait_recv()
        for batch in project_batches:
            for dz in batch:
                landed = slots_in([dz]) + ny
                many(all_lat, all_lat, landed, as_sem.at[0], ar_sem.at[dz]).wait_recv()
            project(batch)
        many(r_send, r_recv, half - 1, rs_sem.at[0], rr_sem.at[0]).wait_recv()

    @pl.when(core == 0)
    def _():
        many(r_send, r_recv, half, rs_sem.at[0], rr_sem.at[0]).wait_recv()
        own_part[...] = r_recv[0].astype(f32)

    summed = own_part[...]
    for place in range(1, half):
        summed = summed + r_recv[place].astype(f32)
    out_ref[...] = summed.astype(bf16)
    many(q_send, q_recv, groups - 1, qs_sem.at[0], qr_sem.at[0]).wait_send()
    many(p_send, p_recv, groups - 1, ps_sem.at[0], pr_sem.at[0]).wait_send()

    @pl.when(core == 0)
    def _():
        weight_handover(0, w_top).wait_send()
        weight_handover(1, w_low).wait_send()
        many(all_lat, all_lat, groups, as_sem.at[0], ar_sem.at[0]).wait_send()

    @pl.when(core == 1)
    def _():
        many(all_lat, all_lat, groups - 1, as_sem.at[0], ar_sem.at[0]).wait_send()
        many(r_send, r_send, nm - 1, rs_sem.at[0], rr_sem.at[0]).wait_send()


def body(
    nz,
    ny,
    queries,
    resident_cache,
    overflow_cache,
    key_up_weight,
    value_up_weight,
    lengths,
    routes,
    out_weight,
):
    nm = lax.axis_size("mp")
    groups = nz * ny
    home_tokens = resident_cache.shape[1]
    out_columns = out_weight.shape[1]
    total = lengths.shape[0]
    tail = routes.shape[1]
    rows = groups * SLOTS * HEADS
    args = (
        queries.reshape(SEQS * HEADS, LANES),
        resident_cache.reshape(SEQS, home_tokens, LANES),
        overflow_cache.reshape(groups, SLOTS * PAGE, LANES),
        key_up_weight.reshape(RANK, LANES),
        value_up_weight.reshape(RANK, LANES),
        lengths.reshape(1, total),
        routes.transpose(1, 2, 0),
        out_weight,
    )
    in_vmem = pl.BlockSpec(memory_space=pltpu.VMEM)
    anywhere = pl.BlockSpec(memory_space=pl.ANY)
    dma = pltpu.SemaphoreType.DMA
    return pl.pallas_call(
        functools.partial(kernel, nz, ny, nm, 1.0 / math.sqrt(LANES)),
        out_shape=pltpu.VMEM((ny * SEQS, out_columns), bf16),
        in_specs=[anywhere] * 8,
        out_specs=in_vmem,
        scratch_shapes=[
            pltpu.VMEM((SEQS * HEADS, LANES), bf16),
            pltpu.VMEM((RANK, LANES), bf16),
            pltpu.VMEM((RANK, LANES), bf16),
            pltpu.VMEM((1, total), i32),
            pltpu.VMEM((tail, 1, total), i32),
            pltpu.VMEM((groups, SLOTS * PAGE, LANES), bf16),
            pltpu.VMEM((SEQS, home_tokens, LANES), bf16),
            pltpu.VMEM((groups, SLOTS * RANK, PAGE), bf16),
            pltpu.VMEM((groups, PAGE, SLOTS * RANK), bf16),
            pltpu.VMEM(out_weight.shape, bf16),
            pltpu.VMEM((2, HEADS * RANK, out_columns), bf16),
            pltpu.VMEM((2, HEADS * RANK, out_columns), bf16),
            pltpu.VMEM((SEQS * HEADS, rows + 128), f32),
            pltpu.VMEM((rows, LANES), f32),
            pltpu.VMEM((groups, SLOTS * HEADS, LANES), bf16),
            pltpu.VMEM((groups, SLOTS * HEADS, LANES), bf16),
            pltpu.VMEM((groups, SLOTS * HEADS, LANES), bf16),
            pltpu.VMEM((groups + 8, SLOTS * HEADS, LANES), bf16),
            pltpu.VMEM((SEQS, HEADS * RANK), bf16),
            pltpu.VMEM((2 * groups, SEQS, HEADS * RANK), bf16),
            pltpu.VMEM((ny * SEQS, out_columns), f32),
            pltpu.VMEM((nm, ny * SEQS, out_columns), bf16),
            pltpu.VMEM((nm // 2, ny * SEQS, out_columns), bf16),
            dma((5,)),
            dma((7,)),
            dma((1,)),
            dma((5,)),
            dma((1,)),
            dma((1,)),
            dma((1,)),
            dma((nz,)),
            dma((1,)),
            dma((1,)),
            dma((2,)),
            dma((2,)),
        ],
        compiler_params=pltpu.CompilerParams(collective_id=0, has_side_effects=True),
        name="spilled_attention",
    )(*args)


def solution(mesh):
    placed = (
        P("dp", "mp", None),
        P("dp", None, "mp", None),
        P("dp", None, None, None, "mp", None),
        P("mp", None, None),
        P("mp", None, None),
        P(),
        P(),
        P("mp", "dp"),
    )
    nz = mesh.shape["mp"]
    ny = mesh.shape["dp"] // nz
    return jax.shard_map(
        functools.partial(body, nz, ny),
        mesh=mesh,
        in_specs=placed,
        out_specs=P("mp", "dp"),
        check_vma=False,
    )
```

```python
import functools
import math

import jax
import jax.numpy as jnp
from jax import lax
from jax.experimental import pallas as pl
from jax.experimental.pallas import tpu as pltpu
from jax.sharding import PartitionSpec as P

MESH = pl.DeviceIdType.MESH
very_low = -1e30
f32, bf16, i32 = jnp.float32, jnp.bfloat16, jnp.int32

SEQS = 8
HEADS = 8
SLOTS = 2
PAGE = 128
LANES = 128
RANK = 64


def iota(shape, dim):
    return lax.broadcasted_iota(i32, shape, dim)


def ones_where(condition, kind=bf16):
    return jnp.where(condition, 1.0, 0.0).astype(kind)


def dot(a, b):
    return jnp.dot(a, b, preferred_element_type=f32)


def dot_last(a, b):
    return lax.dot_general(a, b, (((1,), (1,)), ((), ())), preferred_element_type=f32)


def dot_first(a, b):
    return lax.dot_general(a, b, (((0,), (0,)), ((), ())), preferred_element_type=f32)


def rounded(x):
    return x.astype(bf16).astype(f32)


def three_pieces(x):
    top = rounded(x)
    middle = rounded(x - top)
    return top, middle, (x - top) - middle


def distance_order(nz):
    return sorted(range(nz), key=lambda dz: (min(dz, nz - dz), -dz))


def batches(order, sizes):
    cut, at = [], 0
    for size in sizes:
        if order[at : at + size]:
            cut.append(order[at : at + size])
        at += size
    return cut


def kernel(
    nz,
    ny,
    nm,
    scale,
    q_hbm,
    res_ref,
    ovf_ref,
    wk_hbm,
    wv_hbm,
    len_hbm,
    rt_hbm,
    w_ref,
    out_ref,
    q_ref,
    wk_ref,
    wv_ref,
    len_ref,
    rt_ref,
    pages,
    resident,
    keys,
    values,
    wbuf,
    w_top,
    w_low,
    chosen,
    counts,
    q_send,
    q_recv,
    p_send,
    p_recv,
    own_lat,
    all_lat,
    own_part,
    r_send,
    r_recv,
    page_sem,
    local_sem,
    qs_sem,
    qr_sem,
    ps_sem,
    pr_sem,
    as_sem,
    ar_sem,
    rs_sem,
    rr_sem,
    ws_sem,
    wr_sem,
):
    me, mp = lax.axis_index("dp"), lax.axis_index("mp")
    z, y = lax.div(me, ny), lax.rem(me, ny)
    groups = nz * ny
    core, partner = lax.rem(mp, 2), mp + 1
    half = nm // 2
    items = groups * SLOTS
    rows = items * HEADS
    tail = rt_ref.shape[0]
    total = groups * SEQS
    home_tokens = resident.shape[1]

    def group_at(dz, dy):
        return lax.rem(z + dz, nz) * ny + lax.rem(y + dy, ny)

    def holder_at(dz, ya):
        return lax.rem(z + dz, nz) * ny + ya

    def source_at(dz, ya):
        return lax.rem(z + nz - dz, nz) * ny + ya

    def others_in_plane(dz):
        return [lax.rem(y + dy, ny) for dy in range(1 if dz == 0 else 0, ny)]

    barrier = pltpu.get_barrier_semaphore()

    near_first = distance_order(nz)
    far_first = near_first[::-1]
    serve_batches = [[0]] + batches([dz for dz in far_first if dz], (4, 3))
    project_batches = batches(near_first, (1, 1, 2, 2, 2))

    def batch_of(dz, cut):
        return next(i for i, batch in enumerate(cut) if dz in batch)

    def slots_in(batch):
        return sum(ny - (dz == 0) for dz in batch)

    for dz in far_first:
        for ya in others_in_plane(dz):
            pl.semaphore_signal(
                barrier, inc=1, device_id=(holder_at(dz, ya), mp), device_id_type=MESH
            )
    for step in range(1, nm):
        pl.semaphore_signal(
            barrier, inc=1, device_id=(me, lax.rem(mp + step, nm)), device_id_type=MESH
        )

    small = [
        pltpu.make_async_copy(source, target, local_sem.at[i])
        for i, (source, target) in enumerate(
            [
                (rt_hbm, rt_ref),
                (len_hbm, len_ref),
                (q_hbm, q_ref),
                (wk_hbm, wk_ref),
                (wv_hbm, wv_ref),
                (res_ref, resident),
                (w_ref, wbuf),
            ]
        )
    ]
    for copy in small:
        copy.start()
    for i, batch in enumerate(serve_batches):
        for dz in batch:
            first = lax.rem(z + nz - dz, nz) * ny
            pltpu.make_async_copy(
                ovf_ref.at[pl.ds(first, ny)], pages.at[pl.ds(dz * ny, ny)], page_sem.at[i]
            ).start()
    for copy in small[:5]:
        copy.wait()

    routes = jnp.concatenate([rt_ref[p] for p in range(tail)], axis=0).astype(f32)
    lens = len_ref[...].astype(f32)

    entry = iota((items, LANES), 0)
    lane = iota((items, LANES), 1)
    entry_dz, entry_y, entry_c = entry // (ny * SLOTS), (entry // SLOTS) % ny, entry % SLOTS
    holder = (((z + entry_dz) % nz) * ny + entry_y).astype(f32)
    own_columns = ones_where(
        iota((total, LANES), 0) == me * SEQS + iota((total, LANES), 1) % SEQS
    )
    own_routes = dot(routes.astype(bf16), own_columns)
    named = [jnp.where(own_routes[p : p + 1] == holder, 1.0, 0.0) for p in range(tail)]
    row_l, column_l = iota((LANES, LANES), 0), iota((LANES, LANES), 1)
    earlier = ones_where(
        (row_l // SEQS == column_l // SEQS) & (row_l % SEQS < column_l % SEQS)
    )
    before = dot(functools.reduce(jnp.add, named).astype(bf16), earlier)
    picked = jnp.zeros((items, LANES), f32)
    wanted = entry_c.astype(f32)
    for match in named:
        picked = picked + jnp.where(before == wanted, match, 0.0)
        before = before + match
    expand = ones_where(iota((rows, items), 0) // HEADS == iota((rows, items), 1))
    row = iota((rows, LANES), 0)
    row_lane = iota((rows, LANES), 1)
    same_head = row_lane // SEQS == row % HEADS
    picks = jnp.where(same_head, dot(expand, picked.astype(bf16)), 0.0).astype(bf16)

    home_row, home_lane = iota((64, LANES), 0), iota((64, LANES), 1)
    turned = ones_where(
        (home_lane // SEQS == home_row % HEADS) & (home_lane % SEQS == home_row // HEADS)
    )
    queries = q_ref[...]
    by_head = dot_first(turned, queries).astype(bf16)
    q_send[...] = dot(picks, by_head).astype(bf16).reshape(groups, SLOTS * HEADS, LANES)

    sequence = iota((total, total), 0)
    later = iota((total, total), 1)
    held_before = ones_where((sequence // SEQS == later // SEQS) & (sequence < later))
    here = jnp.where(routes == me.astype(f32), 1.0, 0.0)
    rank = dot(jnp.sum(here, axis=0, keepdims=True).astype(bf16), held_before)
    room = [jnp.zeros((1, total), f32) for _ in range(SLOTS)]
    for p in range(tail):
        match = here[p : p + 1]
        valid = jnp.clip(lens - (home_tokens + p * PAGE), 0.0, float(PAGE)) * match
        for c in range(SLOTS):
            room[c] = room[c] + jnp.where(rank == float(c), valid, 0.0)
        rank = rank + match
    entry_s = iota((items, total), 0)
    column_s = iota((items, total), 1)
    source = ((z + nz - entry_s // (ny * SLOTS)) % nz) * ny + (entry_s // SLOTS) % ny
    sized = jnp.where(entry_s % SLOTS == 0, room[0], room[1])
    sized = jnp.where(column_s // SEQS == source, sized, 0.0).astype(bf16)
    all_ones = jnp.ones((total, LANES), bf16)
    per_item = dot(sized, all_ones).astype(bf16)
    counts[...] = dot(expand, per_item)

    home_s = iota((64, total), 1) == me * SEQS + iota((64, total), 0) // HEADS
    home_count = dot(
        jnp.where(home_s, jnp.minimum(lens, float(home_tokens)), 0.0).astype(bf16), all_ones
    )

    pl.semaphore_wait(barrier, groups - 1 + nm - 1)

    def query_copy(dz, ya, peer):
        return pltpu.make_async_remote_copy(
            src_ref=q_send.at[dz * ny + ya],
            dst_ref=q_recv.at[dz * ny + y],
            send_sem=qs_sem.at[0],
            recv_sem=qr_sem.at[batch_of(dz, serve_batches)],
            device_id=(peer, mp),
            device_id_type=MESH,
        )

    def part_copy(dz, ya, peer):
        return pltpu.make_async_remote_copy(
            src_ref=p_send.at[dz * ny + ya],
            dst_ref=p_recv.at[dz * ny + y],
            send_sem=ps_sem.at[0],
            recv_sem=pr_sem.at[0],
            device_id=(peer, mp),
            device_id_type=MESH,
        )

    def many(source, target, count, send_sem, recv_sem):
        return pltpu.make_async_remote_copy(
            src_ref=source.at[pl.ds(0, count)],
            dst_ref=target.at[pl.ds(0, count)],
            send_sem=send_sem,
            recv_sem=recv_sem,
            device_id=(me, mp),
            device_id_type=MESH,
        )

    for dz in far_first:
        for ya in others_in_plane(dz):
            query_copy(dz, ya, holder_at(dz, ya)).start()
    q_recv[y] = q_send[y]

    wk_wide = jnp.concatenate([wk_ref[...], jnp.zeros((RANK, LANES), bf16)], axis=0)

    def message(best, sums, mixed):
        at = iota(mixed.shape, 1)
        best_pieces, sum_pieces = three_pieces(best), three_pieces(sums)
        packed = mixed
        for i in range(3):
            packed = jnp.where(at == i, best_pieces[i], packed)
            packed = jnp.where(at == 3 + i, sum_pieces[i], packed)
        return packed, at

    def partials(query_rows, latents, token_count):
        folded = three_pieces(dot_last(query_rows, wk_wide))
        scores = []
        for i, latent in enumerate(latents):
            stacked = jnp.concatenate([f[8 * i : 8 * i + 8] for f in folded], axis=0)
            s = dot_last(stacked.astype(bf16), latent)
            scores.append(s[0:8] + s[8:16] + s[16:24])
        scores = jnp.concatenate(scores, axis=0) * scale
        mask = iota(scores.shape, 1).astype(f32) < token_count
        scores = jnp.where(mask, scores, very_low)
        best = jnp.max(scores, axis=1, keepdims=True)
        weights = jnp.where(mask, jnp.exp(scores - best), 0.0)
        sums = jnp.sum(weights, axis=1, keepdims=True)
        top = rounded(weights)
        low = weights - top
        mixed = []
        for i, latent in enumerate(latents):
            stacked = jnp.concatenate([top[8 * i : 8 * i + 8], low[8 * i : 8 * i + 8]], axis=0)
            o = dot(stacked.astype(bf16), latent)
            mixed.append(o[0:8] + o[8:16])
        return best, sums, jnp.concatenate(mixed, axis=0)

    square = ones_where(home_row == home_lane)
    chosen[:, pl.ds(0, rows)] = dot_last(square, picks)
    turned_back = dot_last(square, turned)
    chosen[:, pl.ds(rows, 128)] = jnp.concatenate([turned_back, turned_back], axis=1)
    small[5].wait()
    wide_count = jnp.concatenate([home_count] * (home_tokens // LANES), axis=1)
    best, sums, mixed = partials(queries, [resident[k] for k in range(SEQS)], wide_count)
    packed, at = message(best, sums, mixed)
    p_recv[pl.ds(groups, 4)] = packed.astype(bf16).reshape(4, 16, LANES)
    remainder = jnp.where((at >= 3) & (at < RANK), 0.0, packed - rounded(packed))
    remainder = jnp.where(at < 3, packed, remainder)
    p_recv[pl.ds(groups + 4, 4)] = remainder.astype(bf16).reshape(4, 16, LANES)

    small[6].wait()
    for h in range(HEADS):
        joined = dot(wv_ref[...], wbuf[pl.ds(h * LANES, LANES), :])
        w_top[core, pl.ds(h * RANK, RANK), :] = joined.astype(bf16)
        w_low[core, pl.ds(h * RANK, RANK), :] = (joined - rounded(joined)).astype(bf16)

    def weight_handover(which, array):
        return pltpu.make_async_remote_copy(
            src_ref=array.at[0],
            dst_ref=array.at[0],
            send_sem=ws_sem.at[which],
            recv_sem=wr_sem.at[which],
            device_id=(me, partner),
            device_id_type=MESH,
        )

    @pl.when(core == 0)
    def _():
        weight_handover(0, w_top).start()
        weight_handover(1, w_low).start()

    pick_keys = ones_where(iota((RANK, LANES), 0) == iota((RANK, LANES), 1))
    for i, batch in enumerate(serve_batches):
        held = len(batch) * ny
        pltpu.make_async_copy(
            ovf_ref.at[pl.ds(0, held)], pages.at[pl.ds(0, held)], page_sem.at[i]
        ).wait()
        for slot in [dz * ny + ya for dz in batch for ya in range(ny)]:
            page_pair = pages[slot]
            turned_keys = dot_last(pick_keys, page_pair).astype(bf16)
            keys[slot, pl.ds(0, RANK), :] = turned_keys[:, 0:PAGE]
            keys[slot, pl.ds(RANK, RANK), :] = turned_keys[:, PAGE : 2 * PAGE]
            values[slot] = jnp.concatenate(
                [page_pair[PAGE : 2 * PAGE, RANK:], page_pair[0:PAGE, RANK:]], axis=1
            )

    wk_twice = jnp.concatenate([wk_ref[...], wk_ref[...]], axis=0)

    def served(query_rows, slots, token_count):
        at, row_at = iota(query_rows.shape, 1), iota(query_rows.shape, 0)
        second = (row_at // HEADS) % SLOTS == 1
        folded = dot_last(query_rows, wk_twice)
        folded = jnp.where((at >= RANK) == second, folded, 0.0)
        top = folded.astype(bf16)
        rest = folded - top.astype(f32)
        middle = rest.astype(bf16)
        low = (rest - middle.astype(f32)).astype(bf16)
        scores = []
        for i, slot in enumerate(slots):
            part = slice(16 * i, 16 * i + 16)
            s = dot(jnp.concatenate([top[part], middle[part], low[part]], axis=0), keys[slot])
            scores.append(s[0:16] + s[16:32] + s[32:48])
        scores = jnp.concatenate(scores, axis=0) * scale
        mask = at.astype(f32) < token_count
        scores = jnp.where(mask, scores, very_low)
        best = jnp.max(scores, axis=1, keepdims=True)
        weights = jnp.where(mask, jnp.exp(scores - best), 0.0)
        sums = jnp.sum(weights, axis=1, keepdims=True)
        top = weights.astype(bf16)
        low = (weights - top.astype(f32)).astype(bf16)
        mixed = []
        for i, slot in enumerate(slots):
            part = slice(16 * i, 16 * i + 16)
            o = dot(jnp.concatenate([top[part], low[part]], axis=0), values[slot])
            mixed.append(o[0:16] + o[16:32])
        mixed = jnp.concatenate(mixed, axis=0)
        return best, sums, jnp.where(second, pltpu.roll(mixed, RANK, 1), mixed)

    chunk = ny * SLOTS * HEADS
    for i, batch in enumerate(serve_batches):
        many(q_send, q_recv, slots_in(batch), qs_sem.at[0], qr_sem.at[i]).wait_recv()
        block = jnp.concatenate(
            [q_recv[pl.ds(dz * ny, ny)].reshape(chunk, LANES) for dz in batch], axis=0
        )
        token_count = jnp.concatenate(
            [counts[pl.ds(dz * chunk, chunk), :] for dz in batch], axis=0
        )
        slots = [dz * ny + ya for dz in batch for ya in range(ny)]
        best, sums, mixed = served(block, slots, token_count)
        packed, _ = message(best, sums, mixed)
        packed = packed.astype(bf16).reshape(len(batch) * ny, SLOTS * HEADS, LANES)
        for n, dz in enumerate(batch):
            p_send[pl.ds(dz * ny, ny)] = packed[n * ny : (n + 1) * ny]
        for dz in batch:
            for ya in others_in_plane(dz):
                part_copy(dz, ya, source_at(dz, ya)).start()
            if dz == 0:
                p_recv[y] = p_send[y]

    many(p_send, p_recv, groups - 1, ps_sem.at[0], pr_sem.at[0]).wait_recv()
    parts = p_recv[...].reshape(rows + 128, LANES)
    peaks = dot_last(ones_where(iota((SEQS, LANES), 1) < 3), parts)
    peaks = jnp.broadcast_to(peaks[0:1], chosen.shape)
    member = chosen[...] > 0.5
    peak = jnp.max(jnp.where(member, peaks, very_low), axis=1, keepdims=True)
    factor = jnp.where(member, jnp.exp(peaks - peak), 0.0)
    factor_top = rounded(factor)
    merged = dot(
        jnp.concatenate([factor_top, factor - factor_top], axis=0).astype(bf16), parts
    )
    merged = merged[0:64] + merged[64:128]
    merged_sum = merged[:, 3:4] + merged[:, 4:5] + merged[:, 5:6]
    latent = merged / merged_sum
    low_lane = iota((SEQS, LANES), 1) < RANK
    for v in range(HEADS // 2):
        even = latent[16 * v : 16 * v + 8]
        odd = latent[16 * v + 8 : 16 * v + 16]
        own_lat[:, pl.ds(v * LANES, LANES)] = jnp.where(
            low_lane, pltpu.roll(even, RANK, 1), odd
        ).astype(bf16)

    def latent_copy(dz, peer):
        return pltpu.make_async_remote_copy(
            src_ref=own_lat,
            dst_ref=all_lat.at[core * groups + me],
            send_sem=as_sem.at[0],
            recv_sem=ar_sem.at[dz],
            device_id=(peer, lax.div(mp, 2) * 2 + 1),
            device_id_type=MESH,
        )

    early = [lax.rem(nz + plane - z, nz) for plane in range(min(3, nz))]

    @pl.when(core == 0)
    def _():
        latent_copy(0, me).start()

    for plane, to_plane in enumerate(early):

        @pl.when(z != plane)
        def _():
            for ya in range(ny):
                latent_copy(to_plane, plane * ny + ya).start()

    for dz in near_first:
        later = functools.reduce(jnp.logical_and, [to_plane != dz for to_plane in early])

        @pl.when(later | (dz == 0))
        def _():
            for ya in others_in_plane(dz):
                latent_copy(dz, holder_at(dz, ya)).start()

    @pl.when(core == 1)
    def _():
        all_lat[groups + me] = own_lat[...]

    def sum_copy(target):
        place = lax.rem(lax.div(mp, 2) + half - lax.div(target, 2), half)
        return pltpu.make_async_remote_copy(
            src_ref=r_send.at[target],
            dst_ref=r_recv.at[place],
            send_sem=rs_sem.at[0],
            recv_sem=rr_sem.at[0],
            device_id=(me, target),
            device_id_type=MESH,
        )

    def project(batch):
        part = None
        for c in range(2):
            block = jnp.concatenate(
                [
                    all_lat[
                        pl.ds(c * groups + lax.rem(z + nz - dz, nz) * ny, ny)
                    ].reshape(ny * SEQS, HEADS * RANK)
                    for dz in batch
                ],
                axis=0,
            )
            added = dot(block, w_top[c]) + dot(block, w_low[c])
            part = added if part is None else part + added
        for n, dz in enumerate(batch):
            target = lax.rem(z + nz - dz, nz)
            piece = part[n * ny * SEQS : (n + 1) * ny * SEQS]

            @pl.when(target == mp)
            def _():
                own_part[...] = piece

            @pl.when(target != mp)
            def _():
                r_send[target] = piece.astype(bf16)
                sum_copy(target).start()

    @pl.when(core == 1)
    def _():
        weight_handover(0, w_top).wait_recv()
        weight_handover(1, w_low).wait_recv()
        for batch in project_batches:
            for dz in batch:
                landed = slots_in([dz]) + ny
                many(all_lat, all_lat, landed, as_sem.at[0], ar_sem.at[dz]).wait_recv()
            project(batch)
        many(r_send, r_recv, half - 1, rs_sem.at[0], rr_sem.at[0]).wait_recv()

    @pl.when(core == 0)
    def _():
        many(r_send, r_recv, half, rs_sem.at[0], rr_sem.at[0]).wait_recv()
        own_part[...] = r_recv[0].astype(f32)

    summed = own_part[...]
    for place in range(1, half):
        summed = summed + r_recv[place].astype(f32)
    out_ref[...] = summed.astype(bf16)
    many(q_send, q_recv, groups - 1, qs_sem.at[0], qr_sem.at[0]).wait_send()
    many(p_send, p_recv, groups - 1, ps_sem.at[0], pr_sem.at[0]).wait_send()

    @pl.when(core == 0)
    def _():
        weight_handover(0, w_top).wait_send()
        weight_handover(1, w_low).wait_send()
        many(all_lat, all_lat, groups, as_sem.at[0], ar_sem.at[0]).wait_send()

    @pl.when(core == 1)
    def _():
        many(all_lat, all_lat, groups - 1, as_sem.at[0], ar_sem.at[0]).wait_send()
        many(r_send, r_send, nm - 1, rs_sem.at[0], rr_sem.at[0]).wait_send()


def body(
    nz,
    ny,
    queries,
    resident_cache,
    overflow_cache,
    key_up_weight,
    value_up_weight,
    lengths,
    routes,
    out_weight,
):
    nm = lax.axis_size("mp")
    groups = nz * ny
    home_tokens = resident_cache.shape[1]
    out_columns = out_weight.shape[1]
    total = lengths.shape[0]
    tail = routes.shape[1]
    rows = groups * SLOTS * HEADS
    args = (
        queries.reshape(SEQS * HEADS, LANES),
        resident_cache.reshape(SEQS, home_tokens, LANES),
        overflow_cache.reshape(groups, SLOTS * PAGE, LANES),
        key_up_weight.reshape(RANK, LANES),
        value_up_weight.reshape(RANK, LANES),
        lengths.reshape(1, total),
        routes.transpose(1, 2, 0),
        out_weight,
    )
    in_vmem = pl.BlockSpec(memory_space=pltpu.VMEM)
    anywhere = pl.BlockSpec(memory_space=pl.ANY)
    dma = pltpu.SemaphoreType.DMA
    return pl.pallas_call(
        functools.partial(kernel, nz, ny, nm, 1.0 / math.sqrt(LANES)),
        out_shape=pltpu.VMEM((ny * SEQS, out_columns), bf16),
        in_specs=[anywhere] * 8,
        out_specs=in_vmem,
        scratch_shapes=[
            pltpu.VMEM((SEQS * HEADS, LANES), bf16),
            pltpu.VMEM((RANK, LANES), bf16),
            pltpu.VMEM((RANK, LANES), bf16),
            pltpu.VMEM((1, total), i32),
            pltpu.VMEM((tail, 1, total), i32),
            pltpu.VMEM((groups, SLOTS * PAGE, LANES), bf16),
            pltpu.VMEM((SEQS, home_tokens, LANES), bf16),
            pltpu.VMEM((groups, SLOTS * RANK, PAGE), bf16),
            pltpu.VMEM((groups, PAGE, SLOTS * RANK), bf16),
            pltpu.VMEM(out_weight.shape, bf16),
            pltpu.VMEM((2, HEADS * RANK, out_columns), bf16),
            pltpu.VMEM((2, HEADS * RANK, out_columns), bf16),
            pltpu.VMEM((SEQS * HEADS, rows + 128), f32),
            pltpu.VMEM((rows, LANES), f32),
            pltpu.VMEM((groups, SLOTS * HEADS, LANES), bf16),
            pltpu.VMEM((groups, SLOTS * HEADS, LANES), bf16),
            pltpu.VMEM((groups, SLOTS * HEADS, LANES), bf16),
            pltpu.VMEM((groups + 8, SLOTS * HEADS, LANES), bf16),
            pltpu.VMEM((SEQS, HEADS * RANK), bf16),
            pltpu.VMEM((2 * groups, SEQS, HEADS * RANK), bf16),
            pltpu.VMEM((ny * SEQS, out_columns), f32),
            pltpu.VMEM((nm, ny * SEQS, out_columns), bf16),
            pltpu.VMEM((nm // 2, ny * SEQS, out_columns), bf16),
            dma((5,)),
            dma((7,)),
            dma((1,)),
            dma((5,)),
            dma((1,)),
            dma((1,)),
            dma((1,)),
            dma((nz,)),
            dma((1,)),
            dma((1,)),
            dma((2,)),
            dma((2,)),
        ],
        compiler_params=pltpu.CompilerParams(collective_id=0, has_side_effects=True),
        name="spilled_attention",
    )(*args)


def solution(mesh):
    placed = (
        P("dp", "mp", None),
        P("dp", None, "mp", None),
        P("dp", None, None, None, "mp", None),
        P("mp", None, None),
        P("mp", None, None),
        P(),
        P(),
        P("mp", "dp"),
    )
    nz = mesh.shape["mp"]
    ny = mesh.shape["dp"] // nz
    return jax.shard_map(
        functools.partial(body, nz, ny),
        mesh=mesh,
        in_specs=placed,
        out_specs=P("mp", "dp"),
        check_vma=False,
    )
```

```python
import functools
import math

import jax
import jax.numpy as jnp
from jax import lax
from jax.experimental import pallas as pl
from jax.experimental.pallas import tpu as pltpu
from jax.sharding import PartitionSpec as P

MESH = pl.DeviceIdType.MESH
very_low = -1e30
f32, bf16, i32 = jnp.float32, jnp.bfloat16, jnp.int32

SEQS = 8
HEADS = 8
SLOTS = 2
PAGE = 128
LANES = 128
RANK = 64


def iota(shape, dim):
    return lax.broadcasted_iota(i32, shape, dim)


def ones_where(condition, kind=bf16):
    return jnp.where(condition, 1.0, 0.0).astype(kind)


def dot(a, b):
    return jnp.dot(a, b, preferred_element_type=f32)


def dot_last(a, b):
    return lax.dot_general(a, b, (((1,), (1,)), ((), ())), preferred_element_type=f32)


def dot_first(a, b):
    return lax.dot_general(a, b, (((0,), (0,)), ((), ())), preferred_element_type=f32)


def rounded(x):
    return x.astype(bf16).astype(f32)


def three_pieces(x):
    top = rounded(x)
    middle = rounded(x - top)
    return top, middle, (x - top) - middle


def distance_order(nz):
    return sorted(range(nz), key=lambda dz: (min(dz, nz - dz), -dz))


def batches(order, sizes):
    cut, at = [], 0
    for size in sizes:
        if order[at : at + size]:
            cut.append(order[at : at + size])
        at += size
    return cut


def kernel(
    nz,
    ny,
    nm,
    scale,
    q_hbm,
    res_ref,
    ovf_ref,
    wk_hbm,
    wv_hbm,
    len_hbm,
    rt_hbm,
    w_ref,
    out_ref,
    q_ref,
    wk_ref,
    wv_ref,
    len_ref,
    rt_ref,
    pages,
    resident,
    keys,
    values,
    wbuf,
    w_top,
    w_low,
    chosen,
    counts,
    q_send,
    q_recv,
    p_send,
    p_recv,
    own_lat,
    all_lat,
    own_part,
    r_send,
    r_recv,
    page_sem,
    local_sem,
    qs_sem,
    qr_sem,
    ps_sem,
    pr_sem,
    as_sem,
    ar_sem,
    rs_sem,
    rr_sem,
    ws_sem,
    wr_sem,
):
    me, mp = lax.axis_index("dp"), lax.axis_index("mp")
    z, y = lax.div(me, ny), lax.rem(me, ny)
    groups = nz * ny
    core, partner = lax.rem(mp, 2), mp + 1
    half = nm // 2
    items = groups * SLOTS
    rows = items * HEADS
    tail = rt_ref.shape[0]
    total = groups * SEQS
    home_tokens = resident.shape[1]

    def group_at(dz, dy):
        return lax.rem(z + dz, nz) * ny + lax.rem(y + dy, ny)

    def holder_at(dz, ya):
        return lax.rem(z + dz, nz) * ny + ya

    def source_at(dz, ya):
        return lax.rem(z + nz - dz, nz) * ny + ya

    def others_in_plane(dz):
        return [lax.rem(y + dy, ny) for dy in range(1 if dz == 0 else 0, ny)]

    barrier = pltpu.get_barrier_semaphore()

    near_first = distance_order(nz)
    far_first = near_first[::-1]
    serve_batches = [[0]] + batches([dz for dz in far_first if dz], (4, 3))
    project_batches = batches(near_first, (1, 1, 2, 2, 1, 1))

    def batch_of(dz, cut):
        return next(i for i, batch in enumerate(cut) if dz in batch)

    def slots_in(batch):
        return sum(ny - (dz == 0) for dz in batch)

    for dz in far_first:
        for ya in others_in_plane(dz):
            pl.semaphore_signal(
                barrier, inc=1, device_id=(holder_at(dz, ya), mp), device_id_type=MESH
            )
    for step in range(1, nm):
        pl.semaphore_signal(
            barrier, inc=1, device_id=(me, lax.rem(mp + step, nm)), device_id_type=MESH
        )

    small = [
        pltpu.make_async_copy(source, target, local_sem.at[i])
        for i, (source, target) in enumerate(
            [
                (rt_hbm, rt_ref),
                (len_hbm, len_ref),
                (q_hbm, q_ref),
                (wk_hbm, wk_ref),
                (wv_hbm, wv_ref),
                (res_ref, resident),
                (w_ref, wbuf),
            ]
        )
    ]
    for copy in small:
        copy.start()
    for i, batch in enumerate(serve_batches):
        for dz in batch:
            first = lax.rem(z + nz - dz, nz) * ny
            pltpu.make_async_copy(
                ovf_ref.at[pl.ds(first, ny)], pages.at[pl.ds(dz * ny, ny)], page_sem.at[i]
            ).start()
    for copy in small[:5]:
        copy.wait()

    routes = jnp.concatenate([rt_ref[p] for p in range(tail)], axis=0).astype(f32)
    lens = len_ref[...].astype(f32)

    entry = iota((items, LANES), 0)
    lane = iota((items, LANES), 1)
    entry_dz, entry_y, entry_c = entry // (ny * SLOTS), (entry // SLOTS) % ny, entry % SLOTS
    holder = (((z + entry_dz) % nz) * ny + entry_y).astype(f32)
    own_columns = ones_where(
        iota((total, LANES), 0) == me * SEQS + iota((total, LANES), 1) % SEQS
    )
    own_routes = dot(routes.astype(bf16), own_columns)
    named = [jnp.where(own_routes[p : p + 1] == holder, 1.0, 0.0) for p in range(tail)]
    row_l, column_l = iota((LANES, LANES), 0), iota((LANES, LANES), 1)
    earlier = ones_where(
        (row_l // SEQS == column_l // SEQS) & (row_l % SEQS < column_l % SEQS)
    )
    before = dot(functools.reduce(jnp.add, named).astype(bf16), earlier)
    picked = jnp.zeros((items, LANES), f32)
    wanted = entry_c.astype(f32)
    for match in named:
        picked = picked + jnp.where(before == wanted, match, 0.0)
        before = before + match
    expand = ones_where(iota((rows, items), 0) // HEADS == iota((rows, items), 1))
    row = iota((rows, LANES), 0)
    row_lane = iota((rows, LANES), 1)
    same_head = row_lane // SEQS == row % HEADS
    picks = jnp.where(same_head, dot(expand, picked.astype(bf16)), 0.0).astype(bf16)

    home_row, home_lane = iota((64, LANES), 0), iota((64, LANES), 1)
    turned = ones_where(
        (home_lane // SEQS == home_row % HEADS) & (home_lane % SEQS == home_row // HEADS)
    )
    queries = q_ref[...]
    by_head = dot_first(turned, queries).astype(bf16)
    q_send[...] = dot(picks, by_head).astype(bf16).reshape(groups, SLOTS * HEADS, LANES)

    sequence = iota((total, total), 0)
    later = iota((total, total), 1)
    held_before = ones_where((sequence // SEQS == later // SEQS) & (sequence < later))
    here = jnp.where(routes == me.astype(f32), 1.0, 0.0)
    rank = dot(jnp.sum(here, axis=0, keepdims=True).astype(bf16), held_before)
    room = [jnp.zeros((1, total), f32) for _ in range(SLOTS)]
    for p in range(tail):
        match = here[p : p + 1]
        valid = jnp.clip(lens - (home_tokens + p * PAGE), 0.0, float(PAGE)) * match
        for c in range(SLOTS):
            room[c] = room[c] + jnp.where(rank == float(c), valid, 0.0)
        rank = rank + match
    entry_s = iota((items, total), 0)
    column_s = iota((items, total), 1)
    source = ((z + nz - entry_s // (ny * SLOTS)) % nz) * ny + (entry_s // SLOTS) % ny
    sized = jnp.where(entry_s % SLOTS == 0, room[0], room[1])
    sized = jnp.where(column_s // SEQS == source, sized, 0.0).astype(bf16)
    all_ones = jnp.ones((total, LANES), bf16)
    per_item = dot(sized, all_ones).astype(bf16)
    counts[...] = dot(expand, per_item)

    home_s = iota((64, total), 1) == me * SEQS + iota((64, total), 0) // HEADS
    home_count = dot(
        jnp.where(home_s, jnp.minimum(lens, float(home_tokens)), 0.0).astype(bf16), all_ones
    )

    pl.semaphore_wait(barrier, groups - 1 + nm - 1)

    def query_copy(dz, ya, peer):
        return pltpu.make_async_remote_copy(
            src_ref=q_send.at[dz * ny + ya],
            dst_ref=q_recv.at[dz * ny + y],
            send_sem=qs_sem.at[0],
            recv_sem=qr_sem.at[batch_of(dz, serve_batches)],
            device_id=(peer, mp),
            device_id_type=MESH,
        )

    def part_copy(dz, ya, peer):
        return pltpu.make_async_remote_copy(
            src_ref=p_send.at[dz * ny + ya],
            dst_ref=p_recv.at[dz * ny + y],
            send_sem=ps_sem.at[0],
            recv_sem=pr_sem.at[0],
            device_id=(peer, mp),
            device_id_type=MESH,
        )

    def many(source, target, count, send_sem, recv_sem):
        return pltpu.make_async_remote_copy(
            src_ref=source.at[pl.ds(0, count)],
            dst_ref=target.at[pl.ds(0, count)],
            send_sem=send_sem,
            recv_sem=recv_sem,
            device_id=(me, mp),
            device_id_type=MESH,
        )

    for dz in far_first:
        for ya in others_in_plane(dz):
            query_copy(dz, ya, holder_at(dz, ya)).start()
    q_recv[y] = q_send[y]

    wk_wide = jnp.concatenate([wk_ref[...], jnp.zeros((RANK, LANES), bf16)], axis=0)

    def message(best, sums, mixed):
        at = iota(mixed.shape, 1)
        best_pieces, sum_pieces = three_pieces(best), three_pieces(sums)
        packed = mixed
        for i in range(3):
            packed = jnp.where(at == i, best_pieces[i], packed)
            packed = jnp.where(at == 3 + i, sum_pieces[i], packed)
        return packed, at

    def partials(query_rows, latents, token_count):
        folded = three_pieces(dot_last(query_rows, wk_wide))
        scores = []
        for i, latent in enumerate(latents):
            stacked = jnp.concatenate([f[8 * i : 8 * i + 8] for f in folded], axis=0)
            s = dot_last(stacked.astype(bf16), latent)
            scores.append(s[0:8] + s[8:16] + s[16:24])
        scores = jnp.concatenate(scores, axis=0) * scale
        mask = iota(scores.shape, 1).astype(f32) < token_count
        scores = jnp.where(mask, scores, very_low)
        best = jnp.max(scores, axis=1, keepdims=True)
        weights = jnp.where(mask, jnp.exp(scores - best), 0.0)
        sums = jnp.sum(weights, axis=1, keepdims=True)
        top = rounded(weights)
        low = weights - top
        mixed = []
        for i, latent in enumerate(latents):
            stacked = jnp.concatenate([top[8 * i : 8 * i + 8], low[8 * i : 8 * i + 8]], axis=0)
            o = dot(stacked.astype(bf16), latent)
            mixed.append(o[0:8] + o[8:16])
        return best, sums, jnp.concatenate(mixed, axis=0)

    square = ones_where(home_row == home_lane)
    chosen[:, pl.ds(0, rows)] = dot_last(square, picks)
    turned_back = dot_last(square, turned)
    chosen[:, pl.ds(rows, 128)] = jnp.concatenate([turned_back, turned_back], axis=1)
    small[5].wait()
    wide_count = jnp.concatenate([home_count] * (home_tokens // LANES), axis=1)
    best, sums, mixed = partials(queries, [resident[k] for k in range(SEQS)], wide_count)
    packed, at = message(best, sums, mixed)
    p_recv[pl.ds(groups, 4)] = packed.astype(bf16).reshape(4, 16, LANES)
    remainder = jnp.where((at >= 3) & (at < RANK), 0.0, packed - rounded(packed))
    remainder = jnp.where(at < 3, packed, remainder)
    p_recv[pl.ds(groups + 4, 4)] = remainder.astype(bf16).reshape(4, 16, LANES)

    small[6].wait()
    for h in range(HEADS):
        joined = dot(wv_ref[...], wbuf[pl.ds(h * LANES, LANES), :])
        w_top[core, pl.ds(h * RANK, RANK), :] = joined.astype(bf16)
        w_low[core, pl.ds(h * RANK, RANK), :] = (joined - rounded(joined)).astype(bf16)

    def weight_handover(which, array):
        return pltpu.make_async_remote_copy(
            src_ref=array.at[0],
            dst_ref=array.at[0],
            send_sem=ws_sem.at[which],
            recv_sem=wr_sem.at[which],
            device_id=(me, partner),
            device_id_type=MESH,
        )

    @pl.when(core == 0)
    def _():
        weight_handover(0, w_top).start()
        weight_handover(1, w_low).start()

    pick_keys = ones_where(iota((RANK, LANES), 0) == iota((RANK, LANES), 1))
    for i, batch in enumerate(serve_batches):
        held = len(batch) * ny
        pltpu.make_async_copy(
            ovf_ref.at[pl.ds(0, held)], pages.at[pl.ds(0, held)], page_sem.at[i]
        ).wait()
        for slot in [dz * ny + ya for dz in batch for ya in range(ny)]:
            page_pair = pages[slot]
            turned_keys = dot_last(pick_keys, page_pair).astype(bf16)
            keys[slot, pl.ds(0, RANK), :] = turned_keys[:, 0:PAGE]
            keys[slot, pl.ds(RANK, RANK), :] = turned_keys[:, PAGE : 2 * PAGE]
            values[slot] = jnp.concatenate(
                [page_pair[PAGE : 2 * PAGE, RANK:], page_pair[0:PAGE, RANK:]], axis=1
            )

    wk_twice = jnp.concatenate([wk_ref[...], wk_ref[...]], axis=0)

    def served(query_rows, slots, token_count):
        at, row_at = iota(query_rows.shape, 1), iota(query_rows.shape, 0)
        second = (row_at // HEADS) % SLOTS == 1
        folded = dot_last(query_rows, wk_twice)
        folded = jnp.where((at >= RANK) == second, folded, 0.0)
        top = folded.astype(bf16)
        rest = folded - top.astype(f32)
        middle = rest.astype(bf16)
        low = (rest - middle.astype(f32)).astype(bf16)
        scores = []
        for i, slot in enumerate(slots):
            part = slice(16 * i, 16 * i + 16)
            s = dot(jnp.concatenate([top[part], middle[part], low[part]], axis=0), keys[slot])
            scores.append(s[0:16] + s[16:32] + s[32:48])
        scores = jnp.concatenate(scores, axis=0) * scale
        mask = at.astype(f32) < token_count
        scores = jnp.where(mask, scores, very_low)
        best = jnp.max(scores, axis=1, keepdims=True)
        weights = jnp.where(mask, jnp.exp(scores - best), 0.0)
        sums = jnp.sum(weights, axis=1, keepdims=True)
        top = weights.astype(bf16)
        low = (weights - top.astype(f32)).astype(bf16)
        mixed = []
        for i, slot in enumerate(slots):
            part = slice(16 * i, 16 * i + 16)
            o = dot(jnp.concatenate([top[part], low[part]], axis=0), values[slot])
            mixed.append(o[0:16] + o[16:32])
        mixed = jnp.concatenate(mixed, axis=0)
        return best, sums, jnp.where(second, pltpu.roll(mixed, RANK, 1), mixed)

    chunk = ny * SLOTS * HEADS
    for i, batch in enumerate(serve_batches):
        many(q_send, q_recv, slots_in(batch), qs_sem.at[0], qr_sem.at[i]).wait_recv()
        block = jnp.concatenate(
            [q_recv[pl.ds(dz * ny, ny)].reshape(chunk, LANES) for dz in batch], axis=0
        )
        token_count = jnp.concatenate(
            [counts[pl.ds(dz * chunk, chunk), :] for dz in batch], axis=0
        )
        slots = [dz * ny + ya for dz in batch for ya in range(ny)]
        best, sums, mixed = served(block, slots, token_count)
        packed, _ = message(best, sums, mixed)
        packed = packed.astype(bf16).reshape(len(batch) * ny, SLOTS * HEADS, LANES)
        for n, dz in enumerate(batch):
            p_send[pl.ds(dz * ny, ny)] = packed[n * ny : (n + 1) * ny]
        for dz in batch:
            for ya in others_in_plane(dz):
                part_copy(dz, ya, source_at(dz, ya)).start()
            if dz == 0:
                p_recv[y] = p_send[y]

    many(p_send, p_recv, groups - 1, ps_sem.at[0], pr_sem.at[0]).wait_recv()
    parts = p_recv[...].reshape(rows + 128, LANES)
    peaks = dot_last(ones_where(iota((SEQS, LANES), 1) < 3), parts)
    peaks = jnp.broadcast_to(peaks[0:1], chosen.shape)
    member = chosen[...] > 0.5
    peak = jnp.max(jnp.where(member, peaks, very_low), axis=1, keepdims=True)
    factor = jnp.where(member, jnp.exp(peaks - peak), 0.0)
    factor_top = rounded(factor)
    merged = dot(
        jnp.concatenate([factor_top, factor - factor_top], axis=0).astype(bf16), parts
    )
    merged = merged[0:64] + merged[64:128]
    merged_sum = merged[:, 3:4] + merged[:, 4:5] + merged[:, 5:6]
    latent = merged / merged_sum
    low_lane = iota((SEQS, LANES), 1) < RANK
    for v in range(HEADS // 2):
        even = latent[16 * v : 16 * v + 8]
        odd = latent[16 * v + 8 : 16 * v + 16]
        own_lat[:, pl.ds(v * LANES, LANES)] = jnp.where(
            low_lane, pltpu.roll(even, RANK, 1), odd
        ).astype(bf16)

    def latent_copy(dz, peer):
        return pltpu.make_async_remote_copy(
            src_ref=own_lat,
            dst_ref=all_lat.at[core * groups + me],
            send_sem=as_sem.at[0],
            recv_sem=ar_sem.at[core * nz + dz],
            device_id=(peer, lax.div(mp, 2) * 2 + 1),
            device_id_type=MESH,
        )

    early = [lax.rem(nz + plane - z, nz) for plane in range(min(3, nz))]

    @pl.when(core == 0)
    def _():
        latent_copy(0, me).start()

    for plane, to_plane in enumerate(early):

        @pl.when(z != plane)
        def _():
            for ya in range(ny):
                latent_copy(to_plane, plane * ny + ya).start()

    upward_first = [*range(nz // 2), *range(nz - 1, nz // 2 - 1, -1)]
    for dz in upward_first:
        later = functools.reduce(jnp.logical_and, [to_plane != dz for to_plane in early])

        @pl.when(later | (dz == 0))
        def _():
            for ya in others_in_plane(dz):
                latent_copy(dz, holder_at(dz, ya)).start()

    @pl.when(core == 1)
    def _():
        all_lat[groups + me] = own_lat[...]

    def sum_copy(target):
        place = lax.rem(lax.div(mp, 2) + half - lax.div(target, 2), half)
        return pltpu.make_async_remote_copy(
            src_ref=r_send.at[target],
            dst_ref=r_recv.at[place],
            send_sem=rs_sem.at[0],
            recv_sem=rr_sem.at[0],
            device_id=(me, target),
            device_id_type=MESH,
        )

    def project(batch):
        part = None
        for c in (1, 0):
            for dz in batch:
                landed = slots_in([dz]) if c else ny
                many(
                    all_lat, all_lat, landed, as_sem.at[0], ar_sem.at[c * nz + dz]
                ).wait_recv()
            block = jnp.concatenate(
                [
                    all_lat[
                        pl.ds(c * groups + lax.rem(z + nz - dz, nz) * ny, ny)
                    ].reshape(ny * SEQS, HEADS * RANK)
                    for dz in batch
                ],
                axis=0,
            )
            added = dot(block, w_top[c]) + dot(block, w_low[c])
            part = added if part is None else part + added
        for n, dz in enumerate(batch):
            target = lax.rem(z + nz - dz, nz)
            piece = part[n * ny * SEQS : (n + 1) * ny * SEQS]

            @pl.when(target == mp)
            def _():
                own_part[...] = piece

            @pl.when(target != mp)
            def _():
                r_send[target] = piece.astype(bf16)
                sum_copy(target).start()

    @pl.when(core == 1)
    def _():
        weight_handover(0, w_top).wait_recv()
        weight_handover(1, w_low).wait_recv()
        for batch in project_batches:
            project(batch)
        many(r_send, r_recv, half - 1, rs_sem.at[0], rr_sem.at[0]).wait_recv()

    @pl.when(core == 0)
    def _():
        many(r_send, r_recv, half, rs_sem.at[0], rr_sem.at[0]).wait_recv()
        own_part[...] = r_recv[0].astype(f32)

    summed = own_part[...]
    for place in range(1, half):
        summed = summed + r_recv[place].astype(f32)
    out_ref[...] = summed.astype(bf16)
    many(q_send, q_recv, groups - 1, qs_sem.at[0], qr_sem.at[0]).wait_send()
    many(p_send, p_recv, groups - 1, ps_sem.at[0], pr_sem.at[0]).wait_send()

    @pl.when(core == 0)
    def _():
        weight_handover(0, w_top).wait_send()
        weight_handover(1, w_low).wait_send()
        many(all_lat, all_lat, groups, as_sem.at[0], ar_sem.at[0]).wait_send()

    @pl.when(core == 1)
    def _():
        many(all_lat, all_lat, groups - 1, as_sem.at[0], ar_sem.at[0]).wait_send()
        many(r_send, r_send, nm - 1, rs_sem.at[0], rr_sem.at[0]).wait_send()


def body(
    nz,
    ny,
    queries,
    resident_cache,
    overflow_cache,
    key_up_weight,
    value_up_weight,
    lengths,
    routes,
    out_weight,
):
    nm = lax.axis_size("mp")
    groups = nz * ny
    home_tokens = resident_cache.shape[1]
    out_columns = out_weight.shape[1]
    total = lengths.shape[0]
    tail = routes.shape[1]
    rows = groups * SLOTS * HEADS
    args = (
        queries.reshape(SEQS * HEADS, LANES),
        resident_cache.reshape(SEQS, home_tokens, LANES),
        overflow_cache.reshape(groups, SLOTS * PAGE, LANES),
        key_up_weight.reshape(RANK, LANES),
        value_up_weight.reshape(RANK, LANES),
        lengths.reshape(1, total),
        routes.transpose(1, 2, 0),
        out_weight,
    )
    in_vmem = pl.BlockSpec(memory_space=pltpu.VMEM)
    anywhere = pl.BlockSpec(memory_space=pl.ANY)
    dma = pltpu.SemaphoreType.DMA
    return pl.pallas_call(
        functools.partial(kernel, nz, ny, nm, 1.0 / math.sqrt(LANES)),
        out_shape=pltpu.VMEM((ny * SEQS, out_columns), bf16),
        in_specs=[anywhere] * 8,
        out_specs=in_vmem,
        scratch_shapes=[
            pltpu.VMEM((SEQS * HEADS, LANES), bf16),
            pltpu.VMEM((RANK, LANES), bf16),
            pltpu.VMEM((RANK, LANES), bf16),
            pltpu.VMEM((1, total), i32),
            pltpu.VMEM((tail, 1, total), i32),
            pltpu.VMEM((groups, SLOTS * PAGE, LANES), bf16),
            pltpu.VMEM((SEQS, home_tokens, LANES), bf16),
            pltpu.VMEM((groups, SLOTS * RANK, PAGE), bf16),
            pltpu.VMEM((groups, PAGE, SLOTS * RANK), bf16),
            pltpu.VMEM(out_weight.shape, bf16),
            pltpu.VMEM((2, HEADS * RANK, out_columns), bf16),
            pltpu.VMEM((2, HEADS * RANK, out_columns), bf16),
            pltpu.VMEM((SEQS * HEADS, rows + 128), f32),
            pltpu.VMEM((rows, LANES), f32),
            pltpu.VMEM((groups, SLOTS * HEADS, LANES), bf16),
            pltpu.VMEM((groups, SLOTS * HEADS, LANES), bf16),
            pltpu.VMEM((groups, SLOTS * HEADS, LANES), bf16),
            pltpu.VMEM((groups + 8, SLOTS * HEADS, LANES), bf16),
            pltpu.VMEM((SEQS, HEADS * RANK), bf16),
            pltpu.VMEM((2 * groups, SEQS, HEADS * RANK), bf16),
            pltpu.VMEM((ny * SEQS, out_columns), f32),
            pltpu.VMEM((nm, ny * SEQS, out_columns), bf16),
            pltpu.VMEM((nm // 2, ny * SEQS, out_columns), bf16),
            dma((5,)),
            dma((7,)),
            dma((1,)),
            dma((5,)),
            dma((1,)),
            dma((1,)),
            dma((1,)),
            dma((2 * nz,)),
            dma((1,)),
            dma((1,)),
            dma((2,)),
            dma((2,)),
        ],
        compiler_params=pltpu.CompilerParams(collective_id=0, has_side_effects=True),
        name="spilled_attention",
    )(*args)


def solution(mesh):
    placed = (
        P("dp", "mp", None),
        P("dp", None, "mp", None),
        P("dp", None, None, None, "mp", None),
        P("mp", None, None),
        P("mp", None, None),
        P(),
        P(),
        P("mp", "dp"),
    )
    nz = mesh.shape["mp"]
    ny = mesh.shape["dp"] // nz
    return jax.shard_map(
        functools.partial(body, nz, ny),
        mesh=mesh,
        in_specs=placed,
        out_specs=P("mp", "dp"),
        check_vma=False,
    )
```

```python
import functools
import math

import jax
import jax.numpy as jnp
from jax import lax
from jax.experimental import pallas as pl
from jax.experimental.pallas import tpu as pltpu
from jax.sharding import PartitionSpec as P

MESH = pl.DeviceIdType.MESH
very_low = -1e30
f32, bf16, i32 = jnp.float32, jnp.bfloat16, jnp.int32

SEQS = 8
HEADS = 8
SLOTS = 2
PAGE = 128
LANES = 128
RANK = 64


def iota(shape, dim):
    return lax.broadcasted_iota(i32, shape, dim)


def ones_where(condition, kind=bf16):
    return jnp.where(condition, 1.0, 0.0).astype(kind)


def dot(a, b):
    return jnp.dot(a, b, preferred_element_type=f32)


def dot_last(a, b):
    return lax.dot_general(a, b, (((1,), (1,)), ((), ())), preferred_element_type=f32)


def dot_first(a, b):
    return lax.dot_general(a, b, (((0,), (0,)), ((), ())), preferred_element_type=f32)


def rounded(x):
    return x.astype(bf16).astype(f32)


def three_pieces(x):
    top = rounded(x)
    middle = rounded(x - top)
    return top, middle, (x - top) - middle


def distance_order(nz):
    return sorted(range(nz), key=lambda dz: (min(dz, nz - dz), -dz))


def batches(order, sizes):
    cut, at = [], 0
    for size in sizes:
        if order[at : at + size]:
            cut.append(order[at : at + size])
        at += size
    return cut


def kernel(
    nz,
    ny,
    nm,
    scale,
    q_hbm,
    res_ref,
    ovf_ref,
    wk_hbm,
    wv_hbm,
    len_hbm,
    rt_hbm,
    w_ref,
    out_ref,
    q_ref,
    wk_ref,
    wv_ref,
    len_ref,
    rt_ref,
    pages,
    resident,
    keys,
    values,
    wbuf,
    w_top,
    w_low,
    chosen,
    counts,
    q_send,
    q_recv,
    p_send,
    p_recv,
    own_lat,
    all_lat,
    own_part,
    r_send,
    r_recv,
    page_sem,
    local_sem,
    qs_sem,
    qr_sem,
    ps_sem,
    pr_sem,
    as_sem,
    ar_sem,
    rs_sem,
    rr_sem,
    ws_sem,
    wr_sem,
):
    me, mp = lax.axis_index("dp"), lax.axis_index("mp")
    z, y = lax.div(me, ny), lax.rem(me, ny)
    groups = nz * ny
    core = lax.rem(mp, 2)
    half = nm // 2
    items = groups * SLOTS
    rows = items * HEADS
    tail = rt_ref.shape[0]
    total = groups * SEQS
    home_tokens = resident.shape[1]

    def group_at(dz, dy):
        return lax.rem(z + dz, nz) * ny + lax.rem(y + dy, ny)

    def holder_at(dz, ya):
        return lax.rem(z + dz, nz) * ny + ya

    def source_at(dz, ya):
        return lax.rem(z + nz - dz, nz) * ny + ya

    def others_in_plane(dz):
        return [lax.rem(y + dy, ny) for dy in range(1 if dz == 0 else 0, ny)]

    barrier = pltpu.get_barrier_semaphore()

    near_first = distance_order(nz)
    far_first = near_first[::-1]
    serve_batches = [[0]] + batches([dz for dz in far_first if dz], (4, 3))
    project_batches = batches(near_first, (1, 1, 2, 2, 2))

    def batch_of(dz, cut):
        return next(i for i, batch in enumerate(cut) if dz in batch)

    def slots_in(batch):
        return sum(ny - (dz == 0) for dz in batch)

    for dz in far_first:
        for ya in others_in_plane(dz):
            pl.semaphore_signal(
                barrier, inc=1, device_id=(holder_at(dz, ya), mp), device_id_type=MESH
            )
    for step in range(1, nm):
        pl.semaphore_signal(
            barrier, inc=1, device_id=(me, lax.rem(mp + step, nm)), device_id_type=MESH
        )

    small = [
        pltpu.make_async_copy(source, target, local_sem.at[i])
        for i, (source, target) in enumerate(
            [
                (rt_hbm, rt_ref),
                (len_hbm, len_ref),
                (q_hbm, q_ref),
                (wk_hbm, wk_ref),
                (wv_hbm, wv_ref),
                (res_ref, resident),
                (w_ref, wbuf),
            ]
        )
    ]
    for copy in small:
        copy.start()
    for i, batch in enumerate(serve_batches):
        for dz in batch:
            first = lax.rem(z + nz - dz, nz) * ny
            pltpu.make_async_copy(
                ovf_ref.at[pl.ds(first, ny)], pages.at[pl.ds(dz * ny, ny)], page_sem.at[i]
            ).start()
    for copy in small[:5]:
        copy.wait()

    routes = jnp.concatenate([rt_ref[p] for p in range(tail)], axis=0).astype(f32)
    lens = len_ref[...].astype(f32)

    entry = iota((items, LANES), 0)
    lane = iota((items, LANES), 1)
    entry_dz, entry_y, entry_c = entry // (ny * SLOTS), (entry // SLOTS) % ny, entry % SLOTS
    holder = (((z + entry_dz) % nz) * ny + entry_y).astype(f32)
    own_columns = ones_where(
        iota((total, LANES), 0) == me * SEQS + iota((total, LANES), 1) % SEQS
    )
    own_routes = dot(routes.astype(bf16), own_columns)
    named = [jnp.where(own_routes[p : p + 1] == holder, 1.0, 0.0) for p in range(tail)]
    row_l, column_l = iota((LANES, LANES), 0), iota((LANES, LANES), 1)
    earlier = ones_where(
        (row_l // SEQS == column_l // SEQS) & (row_l % SEQS < column_l % SEQS)
    )
    before = dot(functools.reduce(jnp.add, named).astype(bf16), earlier)
    picked = jnp.zeros((items, LANES), f32)
    wanted = entry_c.astype(f32)
    for match in named:
        picked = picked + jnp.where(before == wanted, match, 0.0)
        before = before + match
    expand = ones_where(iota((rows, items), 0) // HEADS == iota((rows, items), 1))
    row = iota((rows, LANES), 0)
    row_lane = iota((rows, LANES), 1)
    same_head = row_lane // SEQS == row % HEADS
    picks = jnp.where(same_head, dot(expand, picked.astype(bf16)), 0.0).astype(bf16)

    home_row, home_lane = iota((64, LANES), 0), iota((64, LANES), 1)
    turned = ones_where(
        (home_lane // SEQS == home_row % HEADS) & (home_lane % SEQS == home_row // HEADS)
    )
    queries = q_ref[...]
    by_head = dot_first(turned, queries).astype(bf16)
    q_send[...] = dot(picks, by_head).astype(bf16).reshape(groups, SLOTS * HEADS, LANES)

    sequence = iota((total, total), 0)
    later = iota((total, total), 1)
    held_before = ones_where((sequence // SEQS == later // SEQS) & (sequence < later))
    here = jnp.where(routes == me.astype(f32), 1.0, 0.0)
    rank = dot(jnp.sum(here, axis=0, keepdims=True).astype(bf16), held_before)
    room = [jnp.zeros((1, total), f32) for _ in range(SLOTS)]
    for p in range(tail):
        match = here[p : p + 1]
        valid = jnp.clip(lens - (home_tokens + p * PAGE), 0.0, float(PAGE)) * match
        for c in range(SLOTS):
            room[c] = room[c] + jnp.where(rank == float(c), valid, 0.0)
        rank = rank + match
    entry_s = iota((items, total), 0)
    column_s = iota((items, total), 1)
    source = ((z + nz - entry_s // (ny * SLOTS)) % nz) * ny + (entry_s // SLOTS) % ny
    sized = jnp.where(entry_s % SLOTS == 0, room[0], room[1])
    sized = jnp.where(column_s // SEQS == source, sized, 0.0).astype(bf16)
    all_ones = jnp.ones((total, LANES), bf16)
    per_item = dot(sized, all_ones).astype(bf16)
    counts[...] = dot(expand, per_item)

    home_s = iota((64, total), 1) == me * SEQS + iota((64, total), 0) // HEADS
    home_count = dot(
        jnp.where(home_s, jnp.minimum(lens, float(home_tokens)), 0.0).astype(bf16), all_ones
    )

    pl.semaphore_wait(barrier, groups - 1 + nm - 1)

    def query_copy(dz, ya, peer):
        return pltpu.make_async_remote_copy(
            src_ref=q_send.at[dz * ny + ya],
            dst_ref=q_recv.at[dz * ny + y],
            send_sem=qs_sem.at[0],
            recv_sem=qr_sem.at[batch_of(dz, serve_batches)],
            device_id=(peer, mp),
            device_id_type=MESH,
        )

    def part_copy(dz, ya, peer):
        return pltpu.make_async_remote_copy(
            src_ref=p_send.at[dz * ny + ya],
            dst_ref=p_recv.at[dz * ny + y],
            send_sem=ps_sem.at[0],
            recv_sem=pr_sem.at[0],
            device_id=(peer, mp),
            device_id_type=MESH,
        )

    def many(source, target, count, send_sem, recv_sem):
        return pltpu.make_async_remote_copy(
            src_ref=source.at[pl.ds(0, count)],
            dst_ref=target.at[pl.ds(0, count)],
            send_sem=send_sem,
            recv_sem=recv_sem,
            device_id=(me, mp),
            device_id_type=MESH,
        )

    for dz in far_first:
        for ya in others_in_plane(dz):
            query_copy(dz, ya, holder_at(dz, ya)).start()
    q_recv[y] = q_send[y]

    wk_wide = jnp.concatenate([wk_ref[...], jnp.zeros((RANK, LANES), bf16)], axis=0)

    def message(best, sums, mixed):
        at = iota(mixed.shape, 1)
        best_pieces, sum_pieces = three_pieces(best), three_pieces(sums)
        packed = mixed
        for i in range(3):
            packed = jnp.where(at == i, best_pieces[i], packed)
            packed = jnp.where(at == 3 + i, sum_pieces[i], packed)
        return packed, at

    def partials(query_rows, latents, token_count):
        folded = three_pieces(dot_last(query_rows, wk_wide))
        scores = []
        for i, latent in enumerate(latents):
            stacked = jnp.concatenate([f[8 * i : 8 * i + 8] for f in folded], axis=0)
            s = dot_last(stacked.astype(bf16), latent)
            scores.append(s[0:8] + s[8:16] + s[16:24])
        scores = jnp.concatenate(scores, axis=0) * scale
        mask = iota(scores.shape, 1).astype(f32) < token_count
        scores = jnp.where(mask, scores, very_low)
        best = jnp.max(scores, axis=1, keepdims=True)
        weights = jnp.where(mask, jnp.exp(scores - best), 0.0)
        sums = jnp.sum(weights, axis=1, keepdims=True)
        top = rounded(weights)
        low = weights - top
        mixed = []
        for i, latent in enumerate(latents):
            stacked = jnp.concatenate([top[8 * i : 8 * i + 8], low[8 * i : 8 * i + 8]], axis=0)
            o = dot(stacked.astype(bf16), latent)
            mixed.append(o[0:8] + o[8:16])
        return best, sums, jnp.concatenate(mixed, axis=0)

    square = ones_where(home_row == home_lane)
    chosen[:, pl.ds(0, rows)] = dot_last(square, picks)
    turned_back = dot_last(square, turned)
    chosen[:, pl.ds(rows, 128)] = jnp.concatenate([turned_back, turned_back], axis=1)
    small[5].wait()
    wide_count = jnp.concatenate([home_count] * (home_tokens // LANES), axis=1)
    best, sums, mixed = partials(queries, [resident[k] for k in range(SEQS)], wide_count)
    packed, at = message(best, sums, mixed)
    p_recv[pl.ds(groups, 4)] = packed.astype(bf16).reshape(4, 16, LANES)
    remainder = jnp.where((at >= 3) & (at < RANK), 0.0, packed - rounded(packed))
    remainder = jnp.where(at < 3, packed, remainder)
    p_recv[pl.ds(groups + 4, 4)] = remainder.astype(bf16).reshape(4, 16, LANES)

    small[6].wait()
    for h in range(HEADS):
        joined = dot(wv_ref[...], wbuf[pl.ds(h * LANES, LANES), :])
        w_top[core, pl.ds(h * RANK, RANK), :] = joined.astype(bf16)
        w_low[core, pl.ds(h * RANK, RANK), :] = (joined - rounded(joined)).astype(bf16)

    def weight_handover(which, array):
        return pltpu.make_async_remote_copy(
            src_ref=array.at[0],
            dst_ref=array.at[0],
            send_sem=ws_sem.at[which],
            recv_sem=wr_sem.at[which],
            device_id=(me, lax.div(mp, 2) * 2 + 1),
            device_id_type=MESH,
        )

    @pl.when(core == 0)
    def _():
        weight_handover(0, w_top).start()
        weight_handover(1, w_low).start()

    pick_keys = ones_where(iota((RANK, LANES), 0) == iota((RANK, LANES), 1))
    for i, batch in enumerate(serve_batches):
        held = len(batch) * ny
        pltpu.make_async_copy(
            ovf_ref.at[pl.ds(0, held)], pages.at[pl.ds(0, held)], page_sem.at[i]
        ).wait()
        for slot in [dz * ny + ya for dz in batch for ya in range(ny)]:
            page_pair = pages[slot]
            turned_keys = dot_last(pick_keys, page_pair).astype(bf16)
            keys[slot, pl.ds(0, RANK), :] = turned_keys[:, 0:PAGE]
            keys[slot, pl.ds(RANK, RANK), :] = turned_keys[:, PAGE : 2 * PAGE]
            values[slot] = jnp.concatenate(
                [page_pair[PAGE : 2 * PAGE, RANK:], page_pair[0:PAGE, RANK:]], axis=1
            )

    wk_twice = jnp.concatenate([wk_ref[...], wk_ref[...]], axis=0)

    def served(query_rows, slots, token_count):
        at, row_at = iota(query_rows.shape, 1), iota(query_rows.shape, 0)
        second = (row_at // HEADS) % SLOTS == 1
        folded = dot_last(query_rows, wk_twice)
        folded = jnp.where((at >= RANK) == second, folded, 0.0)
        top = folded.astype(bf16)
        rest = folded - top.astype(f32)
        middle = rest.astype(bf16)
        low = (rest - middle.astype(f32)).astype(bf16)
        scores = []
        for i, slot in enumerate(slots):
            part = slice(16 * i, 16 * i + 16)
            s = dot(jnp.concatenate([top[part], middle[part], low[part]], axis=0), keys[slot])
            scores.append(s[0:16] + s[16:32] + s[32:48])
        scores = jnp.concatenate(scores, axis=0) * scale
        mask = at.astype(f32) < token_count
        scores = jnp.where(mask, scores, very_low)
        best = jnp.max(scores, axis=1, keepdims=True)
        weights = jnp.where(mask, jnp.exp(scores - best), 0.0)
        sums = jnp.sum(weights, axis=1, keepdims=True)
        top = weights.astype(bf16)
        low = (weights - top.astype(f32)).astype(bf16)
        mixed = []
        for i, slot in enumerate(slots):
            part = slice(16 * i, 16 * i + 16)
            o = dot(jnp.concatenate([top[part], low[part]], axis=0), values[slot])
            mixed.append(o[0:16] + o[16:32])
        mixed = jnp.concatenate(mixed, axis=0)
        return best, sums, jnp.where(second, pltpu.roll(mixed, RANK, 1), mixed)

    chunk = ny * SLOTS * HEADS
    for i, batch in enumerate(serve_batches):
        many(q_send, q_recv, slots_in(batch), qs_sem.at[0], qr_sem.at[i]).wait_recv()
        block = jnp.concatenate(
            [q_recv[pl.ds(dz * ny, ny)].reshape(chunk, LANES) for dz in batch], axis=0
        )
        token_count = jnp.concatenate(
            [counts[pl.ds(dz * chunk, chunk), :] for dz in batch], axis=0
        )
        slots = [dz * ny + ya for dz in batch for ya in range(ny)]
        best, sums, mixed = served(block, slots, token_count)
        packed, _ = message(best, sums, mixed)
        packed = packed.astype(bf16).reshape(len(batch) * ny, SLOTS * HEADS, LANES)
        for n, dz in enumerate(batch):
            p_send[pl.ds(dz * ny, ny)] = packed[n * ny : (n + 1) * ny]
        for dz in batch:
            for ya in others_in_plane(dz):
                part_copy(dz, ya, source_at(dz, ya)).start()
            if dz == 0:
                p_recv[y] = p_send[y]

    many(p_send, p_recv, groups - 1, ps_sem.at[0], pr_sem.at[0]).wait_recv()
    parts = p_recv[...].reshape(rows + 128, LANES)
    peaks = dot_last(ones_where(iota((SEQS, LANES), 1) < 3), parts)
    peaks = jnp.broadcast_to(peaks[0:1], chosen.shape)
    member = chosen[...] > 0.5
    peak = jnp.max(jnp.where(member, peaks, very_low), axis=1, keepdims=True)
    factor = jnp.where(member, jnp.exp(peaks - peak), 0.0)
    factor_top = rounded(factor)
    merged = dot(
        jnp.concatenate([factor_top, factor - factor_top], axis=0).astype(bf16), parts
    )
    merged = merged[0:64] + merged[64:128]
    merged_sum = merged[:, 3:4] + merged[:, 4:5] + merged[:, 5:6]
    latent = merged / merged_sum
    low_lane = iota((SEQS, LANES), 1) < RANK
    for v in range(HEADS // 2):
        even = latent[16 * v : 16 * v + 8]
        odd = latent[16 * v + 8 : 16 * v + 16]
        own_lat[:, pl.ds(v * LANES, LANES)] = jnp.where(
            low_lane, pltpu.roll(even, RANK, 1), odd
        ).astype(bf16)

    def latent_copy(dz, peer):
        return pltpu.make_async_remote_copy(
            src_ref=own_lat,
            dst_ref=all_lat.at[core * groups + me],
            send_sem=as_sem.at[0],
            recv_sem=ar_sem.at[dz],
            device_id=(peer, lax.div(mp, 2) * 2 + 1),
            device_id_type=MESH,
        )

    early = [lax.rem(nz + plane - z, nz) for plane in range(min(3, nz))]

    @pl.when(core == 0)
    def _():
        latent_copy(0, me).start()

    for plane, to_plane in enumerate(early):

        @pl.when(z != plane)
        def _():
            for ya in range(ny):
                latent_copy(to_plane, plane * ny + ya).start()

    for dz in near_first:
        later = functools.reduce(jnp.logical_and, [to_plane != dz for to_plane in early])

        @pl.when(later | (dz == 0))
        def _():
            for ya in others_in_plane(dz):
                latent_copy(dz, holder_at(dz, ya)).start()

    @pl.when(core == 1)
    def _():
        all_lat[groups + me] = own_lat[...]

    def sum_copy(target):
        place = lax.rem(lax.div(mp, 2) + half - lax.div(target, 2), half)
        return pltpu.make_async_remote_copy(
            src_ref=r_send.at[target],
            dst_ref=r_recv.at[place],
            send_sem=rs_sem.at[0],
            recv_sem=rr_sem.at[0],
            device_id=(me, target),
            device_id_type=MESH,
        )

    def project(batch):
        part = None
        for c in range(2):
            block = jnp.concatenate(
                [
                    all_lat[
                        pl.ds(c * groups + lax.rem(z + nz - dz, nz) * ny, ny)
                    ].reshape(ny * SEQS, HEADS * RANK)
                    for dz in batch
                ],
                axis=0,
            )
            added = dot(block, w_top[c]) + dot(block, w_low[c])
            part = added if part is None else part + added
        for n, dz in enumerate(batch):
            target = lax.rem(z + nz - dz, nz)
            piece = part[n * ny * SEQS : (n + 1) * ny * SEQS]

            @pl.when(target == mp)
            def _():
                own_part[...] = piece

            @pl.when(target != mp)
            def _():
                r_send[target] = piece.astype(bf16)
                sum_copy(target).start()

    @pl.when(core == 1)
    def _():
        weight_handover(0, w_top).wait_recv()
        weight_handover(1, w_low).wait_recv()
        for batch in project_batches:
            for dz in batch:
                landed = slots_in([dz]) + ny
                many(all_lat, all_lat, landed, as_sem.at[0], ar_sem.at[dz]).wait_recv()
            project(batch)
        many(r_send, r_recv, half - 1, rs_sem.at[0], rr_sem.at[0]).wait_recv()

    @pl.when(core == 0)
    def _():
        many(r_send, r_recv, half, rs_sem.at[0], rr_sem.at[0]).wait_recv()
        own_part[...] = r_recv[0].astype(f32)

    summed = own_part[...]
    for place in range(1, half):
        summed = summed + r_recv[place].astype(f32)
    out_ref[...] = summed.astype(bf16)
    many(q_send, q_recv, groups - 1, qs_sem.at[0], qr_sem.at[0]).wait_send()
    many(p_send, p_recv, groups - 1, ps_sem.at[0], pr_sem.at[0]).wait_send()

    @pl.when(core == 0)
    def _():
        weight_handover(0, w_top).wait_send()
        weight_handover(1, w_low).wait_send()
        many(all_lat, all_lat, groups, as_sem.at[0], ar_sem.at[0]).wait_send()

    @pl.when(core == 1)
    def _():
        many(all_lat, all_lat, groups - 1, as_sem.at[0], ar_sem.at[0]).wait_send()
        many(r_send, r_send, nm - 1, rs_sem.at[0], rr_sem.at[0]).wait_send()


def body(
    nz,
    ny,
    queries,
    resident_cache,
    overflow_cache,
    key_up_weight,
    value_up_weight,
    lengths,
    routes,
    out_weight,
):
    nm = lax.axis_size("mp")
    groups = nz * ny
    home_tokens = resident_cache.shape[1]
    out_columns = out_weight.shape[1]
    total = lengths.shape[0]
    tail = routes.shape[1]
    rows = groups * SLOTS * HEADS
    args = (
        queries.reshape(SEQS * HEADS, LANES),
        resident_cache.reshape(SEQS, home_tokens, LANES),
        overflow_cache.reshape(groups, SLOTS * PAGE, LANES),
        key_up_weight.reshape(RANK, LANES),
        value_up_weight.reshape(RANK, LANES),
        lengths.reshape(1, total),
        routes.transpose(1, 2, 0),
        out_weight,
    )
    in_vmem = pl.BlockSpec(memory_space=pltpu.VMEM)
    anywhere = pl.BlockSpec(memory_space=pl.ANY)
    dma = pltpu.SemaphoreType.DMA
    return pl.pallas_call(
        functools.partial(kernel, nz, ny, nm, 1.0 / math.sqrt(LANES)),
        out_shape=pltpu.VMEM((ny * SEQS, out_columns), bf16),
        in_specs=[anywhere] * 8,
        out_specs=in_vmem,
        scratch_shapes=[
            pltpu.VMEM((SEQS * HEADS, LANES), bf16),
            pltpu.VMEM((RANK, LANES), bf16),
            pltpu.VMEM((RANK, LANES), bf16),
            pltpu.VMEM((1, total), i32),
            pltpu.VMEM((tail, 1, total), i32),
            pltpu.VMEM((groups, SLOTS * PAGE, LANES), bf16),
            pltpu.VMEM((SEQS, home_tokens, LANES), bf16),
            pltpu.VMEM((groups, SLOTS * RANK, PAGE), bf16),
            pltpu.VMEM((groups, PAGE, SLOTS * RANK), bf16),
            pltpu.VMEM(out_weight.shape, bf16),
            pltpu.VMEM((2, HEADS * RANK, out_columns), bf16),
            pltpu.VMEM((2, HEADS * RANK, out_columns), bf16),
            pltpu.VMEM((SEQS * HEADS, rows + 128), f32),
            pltpu.VMEM((rows, LANES), f32),
            pltpu.VMEM((groups, SLOTS * HEADS, LANES), bf16),
            pltpu.VMEM((groups, SLOTS * HEADS, LANES), bf16),
            pltpu.VMEM((groups, SLOTS * HEADS, LANES), bf16),
            pltpu.VMEM((groups + 8, SLOTS * HEADS, LANES), bf16),
            pltpu.VMEM((SEQS, HEADS * RANK), bf16),
            pltpu.VMEM((2 * groups, SEQS, HEADS * RANK), bf16),
            pltpu.VMEM((ny * SEQS, out_columns), f32),
            pltpu.VMEM((nm, ny * SEQS, out_columns), bf16),
            pltpu.VMEM((nm // 2, ny * SEQS, out_columns), bf16),
            dma((5,)),
            dma((7,)),
            dma((1,)),
            dma((5,)),
            dma((1,)),
            dma((1,)),
            dma((1,)),
            dma((nz,)),
            dma((1,)),
            dma((1,)),
            dma((2,)),
            dma((2,)),
        ],
        compiler_params=pltpu.CompilerParams(collective_id=0, has_side_effects=True),
        name="spilled_attention",
    )(*args)


def solution(mesh):
    placed = (
        P("dp", "mp", None),
        P("dp", None, "mp", None),
        P("dp", None, None, None, "mp", None),
        P("mp", None, None),
        P("mp", None, None),
        P(),
        P(),
        P("mp", "dp"),
    )
    nz = mesh.shape["mp"]
    ny = mesh.shape["dp"] // nz
    return jax.shard_map(
        functools.partial(body, nz, ny),
        mesh=mesh,
        in_specs=placed,
        out_specs=P("mp", "dp"),
        check_vma=False,
    )
```
